512 devices in a mesh: gx: 8 (over x, core), gy: 8 (over y), gz: 8 (over z).
Axes of the slice: x: 4, y: 8, z: 8, core: 2. Of those that a mesh axis runs over, the one named last changes fastest.
Arguments:
- warped_image: float32 [512, 512, 1024], P('gx', 'gy', 'gz'), may hold values from -6 to 6
- fixed_image: float32 [512, 512, 1024], P('gx', 'gy', 'gz'), may hold values from -6 to 6
- fine_control: float32 [3, 64, 64, 128], P(None, 'gx', 'gy', 'gz'), may hold values from -6 to 6
- coarse_control: float32 [3, 16, 16, 32], replicated, may hold values from -6 to 6
Outputs:
- fine_gradient: float32 [3, 64, 64, 128], P(None, 'gx', 'gy', 'gz')
- coarse_gradient: float32 [3, 16, 16, 32], replicated
The draws below stay inside these ranges and needn't reach their ends.
All inputs are finite; a program needn't handle non-finite values.
Results may differ from the reference program's by a relative error of at most 0.0003.
Values sent between devices are 32-bit elements; how exact they have to be, the bound alone decides.
A program may use at most 64 MiB of HBM per device.

```python
import jax
import jax.numpy as jnp
from jax import lax

SPF = 8
SPC = 32
NX = 512
NY = 512
NZ = 1024
FX = 64
FY = 64
FZ = 128
KX = 16
KY = 16
KZ = 32


def levels(key, shape, shards, low, largest):
    def one(position, shards_of):
        draws = jax.random.uniform(jax.random.fold_in(jax.random.fold_in(key, 6), position), (shards_of,), jnp.float32, low / len(shards), largest / len(shards))
        return jnp.repeat(jnp.exp(draws), shape[position] // shards_of).reshape((-1,) + (1,) * (len(shape) - position - 1))

    gain = one(*shards[0])
    for cut in shards[1:]:
        gain = gain * one(*cut)
    return gain


def scatter_about(rng, extent, deviation, most, cuts=(), kind=jnp.bfloat16):
    entries = deviation * jax.random.normal(rng, extent, jnp.float32)
    if cuts:
        entries = entries * levels(rng, extent, cuts, -0.22, 0.18)
    return jnp.clip(entries, -most, most).astype(kind)


def setup_inputs(seed: int = 0) -> dict:
    arg_keys = jax.random.split(jax.random.key(seed), 5)
    return {
        "warped_image": scatter_about(arg_keys[0], (NX, NY, NZ), 1.0, 6.0, ((0, 8), (1, 8), (2, 8)), jnp.float32),
        "fixed_image": scatter_about(arg_keys[1], (NX, NY, NZ), 1.0, 6.0, ((0, 8), (1, 8), (2, 8)), jnp.float32),
        "fine_control": scatter_about(arg_keys[2], (3, FX, FY, FZ), 1.0, 6.0, ((1, 8), (2, 8), (3, 8)), jnp.float32),
        "coarse_control": scatter_about(arg_keys[3], (3, KX, KY, KZ), 1.0, 6.0, (), jnp.float32),
    }


bend_factor = 0.01
highest = lax.Precision.HIGHEST


def spline(values):
    magnitude = jnp.abs(values)
    inner = 2.0 / 3.0 - magnitude * magnitude + 0.5 * magnitude * magnitude * magnitude
    remain = 2.0 - magnitude
    outer = remain * remain * remain / 6.0
    return jnp.where(magnitude < 1.0, inner, jnp.where(magnitude < 2.0, outer, 0.0 * magnitude))


def basis_matrix(voxels, points, spacing, voxel_start, point_start):
    voxel = (jnp.arange(voxels, dtype=jnp.int32) + voxel_start).astype(jnp.float32) + 0.5
    centre = (jnp.arange(points, dtype=jnp.int32) + point_start).astype(jnp.float32) * spacing + 0.5 * spacing
    return spline((voxel[:, None] - centre[None, :]) / spacing)


def slope(padded, axis):
    rank = padded.ndim
    count = padded.shape[axis] - 4

    def shifted(offset):
        piece = lax.slice_in_dim(padded, offset, offset + count, axis=axis)
        for other in range(rank - 3, rank):
            if other != axis:
                piece = lax.slice_in_dim(piece, 2, piece.shape[other] - 2, axis=other)
        return piece

    return (shifted(0) - 8.0 * shifted(1) + 8.0 * shifted(3) - shifted(4)) / 12.0


def stencil(padded):
    centre = padded[:, 1:-1, 1:-1, 1:-1]
    total = padded[:, 2:, 1:-1, 1:-1] + padded[:, :-2, 1:-1, 1:-1]
    total = total + padded[:, 1:-1, 2:, 1:-1] + padded[:, 1:-1, :-2, 1:-1]
    total = total + padded[:, 1:-1, 1:-1, 2:] + padded[:, 1:-1, 1:-1, :-2]
    return total - 6.0 * centre


def laplace(field):
    return stencil(jnp.pad(field, ((0, 0), (1, 1), (1, 1), (1, 1))))


def project_blocks(force, along_x, along_y, along_z):
    section = jnp.einsum("axyz,zr->axyr", force, along_z, precision=highest)
    section = jnp.einsum("axyr,yq->axqr", section, along_y, precision=highest)
    return jnp.einsum("axqr,xp->apqr", section, along_x, precision=highest)


def reference(warped_image, fixed_image, fine_control, coarse_control):
    summed = jnp.pad(warped_image + fixed_image, 2)
    difference = warped_image - fixed_image
    fine_x = basis_matrix(NX, FX, SPF, 0, 0)
    fine_y = basis_matrix(NY, FY, SPF, 0, 0)
    fine_z = basis_matrix(NZ, FZ, SPF, 0, 0)
    coarse_x = basis_matrix(NX, KX, SPC, 0, 0)
    coarse_y = basis_matrix(NY, KY, SPC, 0, 0)
    coarse_z = basis_matrix(NZ, KZ, SPC, 0, 0)
    block_rows = 16

    def block(carry, start):
        fine_sum, coarse_sum = carry
        slab = lax.dynamic_slice_in_dim(summed, start, block_rows + 4, 0)
        slopes = jnp.stack([slope(slab, 0), slope(slab, 1), slope(slab, 2)]) * 0.5
        local = lax.dynamic_slice_in_dim(difference, start, block_rows, 0)
        force = slopes * local[None]
        fine_rows = lax.dynamic_slice_in_dim(fine_x, start, block_rows, 0)
        coarse_rows = lax.dynamic_slice_in_dim(coarse_x, start, block_rows, 0)
        fine_sum = fine_sum + project_blocks(force, fine_rows, fine_y, fine_z)
        coarse_sum = coarse_sum + project_blocks(force, coarse_rows, coarse_y, coarse_z)
        return (fine_sum, coarse_sum), None

    starts = jnp.arange(NX // block_rows, dtype=jnp.int32) * block_rows
    initial = (jnp.zeros((3, FX, FY, FZ), jnp.float32), jnp.zeros((3, KX, KY, KZ), jnp.float32))
    (fine_sum, coarse_sum), _ = lax.scan(block, initial, starts)
    fine_gradient = fine_sum * (SPF ** -1.5) + bend_factor * laplace(laplace(fine_control))
    coarse_gradient = coarse_sum * (SPC ** -1.5) + bend_factor * laplace(laplace(coarse_control))
    return fine_gradient, coarse_gradient
```

```python
import functools

import jax
import jax.numpy as jnp
from jax import lax
from jax.experimental import pallas as pl
from jax.experimental.pallas import tpu as pltpu
from jax.sharding import PartitionSpec as P

SPF = 8
SPC = 32
BEND = 0.01
HI = lax.Precision.HIGHEST
MESH = pl.DeviceIdType.MESH
f32 = jnp.float32
bf16 = jnp.bfloat16


def nn(a, b):
    return lax.dot_general(
        a, b, (((1,), (0,)), ((), ())), precision=HI, preferred_element_type=f32
    )


def nt(a, b):
    return lax.dot_general(
        a, b, (((1,), (1,)), ((), ())), precision=HI, preferred_element_type=f32
    )


def spline(t):
    m = jnp.abs(t)
    inner = 2.0 / 3.0 - m * m + 0.5 * m * m * m
    r = 2.0 - m
    outer = r * r * r * (1.0 / 6.0)
    return jnp.where(m < 1.0, inner, jnp.where(m < 2.0, outer, 0.0))


def weight(voxel, point, spacing):
    scaled = (2 * voxel + 1 - spacing * (2 * point + 1)).astype(f32)
    return spline(scaled * (0.5 / spacing))


def iota(shape, axis):
    return lax.broadcasted_iota(jnp.int32, shape, axis)


def diff1(out, inp):
    d = jnp.abs(out - inp)
    return jnp.where(d == 0, -2.0, jnp.where(d == 1, 1.0, 0.0)).astype(f32)


def diff2(out, inp, count):
    d = jnp.abs(out - inp)
    edge = (inp == 0) | (inp == count - 1)
    centre = jnp.where(edge, 5.0, 6.0)
    return jnp.where(
        d == 0, centre, jnp.where(d == 1, -4.0, jnp.where(d == 2, 1.0, 0.0))
    ).astype(f32)


def same(out, inp):
    return jnp.where(out == inp, 1.0, 0.0).astype(f32)


def bend_planes(px, py, qx, qy, cx, cy):
    jx, jy = same(px, qx), same(py, qy)
    tx, ty = diff1(px, qx), diff1(py, qy)
    m0 = diff2(px, qx, cx) * jy + jx * diff2(py, qy, cy) + 2.0 * tx * ty
    m1 = 2.0 * (tx * jy + jx * ty)
    return m0 * BEND, m1 * BEND, jx * jy * BEND


def kernel(sizes, w_hbm, f_hbm, fc_hbm, cc_hbm, fo_ref, co_ref,
           w_v, f_v, fc_ref, cc_ref, s_v, ysend, yrecv, zsend, zrecv, zcorr,
           wf_v, wc_v, fh_v, fl_v,
           accf, accc, tz_v, bend_v, clane, cbend, zmsg, zgot, a_v, agot, b_v, bgot,
           cmsg, crecv, zrow, xrow, load_sem, small_sem, hs_sem, hr_sem, ys_sem, yr_sem,
           ms_sem, mr_sem, ns_sem, nr_sem, cs_sem, cr_sem):
    nx, ny, nz = sizes
    axes = ("gx", "gy", "gz")
    counts = sizes
    me = [lax.axis_index(a) for a in axes]
    SX, SY, SZ = w_v.shape
    PX, PY, PZ = SX // SPF, SY // SPF, SZ // SPF
    KX, KY, KZ = cc_ref.shape[1:]
    EX, QE = PX + 4, 2 * PY
    CR = accc.shape[0]
    cells = SX // SPF
    lanes = 3 * SZ

    loads = []
    for c in range(cells):
        part = pl.ds(c * SPF, SPF)
        loads.append((
            pltpu.make_async_copy(w_hbm.at[part], w_v.at[part], load_sem.at[0, c]),
            pltpu.make_async_copy(f_hbm.at[part], f_v.at[part], load_sem.at[1, c]),
        ))
    small = (pltpu.make_async_copy(fc_hbm, fc_ref, small_sem.at[0]),
             pltpu.make_async_copy(cc_hbm, cc_ref, small_sem.at[1]))
    order = [0, cells - 1] + list(range(1, cells - 1))
    for c in order:
        loads[c][0].start()
        loads[c][1].start()
    for copy in small:
        copy.start()

    has = [(me[k] > 0, me[k] < counts[k] - 1) for k in range(3)]
    sides = [(d, e, f) for f in range(3) for d in range(3) for e in range(3)]

    def toward(step):
        ok = None
        for k in range(3):
            if step[k] != 1:
                here = has[k][0] if step[k] == 0 else has[k][1]
                ok = here if ok is None else ok & here
        return ok, {axes[k]: me[k] + (step[k] - 1) for k in range(3) if step[k] != 1}

    zero_plane = jnp.zeros((2, SY, SZ), f32)
    s_v[0:2, 8:8 + SY, :] = zero_plane
    s_v[SX + 2:SX + 4, 8:8 + SY, :] = zero_plane
    yrecv[...] = jnp.zeros(yrecv.shape, f32)
    zrecv[...] = jnp.zeros(zrecv.shape, f32)
    zgot[...] = jnp.zeros(zgot.shape, f32)
    agot[...] = jnp.zeros(agot.shape, f32)
    bgot[...] = jnp.zeros(bgot.shape, f32)
    crecv[...] = jnp.zeros(crecv.shape, f32)

    barrier = pltpu.get_barrier_semaphore()
    total = 0
    for k, a in enumerate(axes):
        for d in range(1, counts[k]):
            pl.semaphore_signal(
                barrier, inc=1, device_id={a: lax.rem(me[k] + d, counts[k])}, device_id_type=MESH
            )
            total += 1
    for step in sides:
        if sum(n != 1 for n in step) >= 2:
            ok, there = toward(step)

            @pl.when(ok)
            def _(there=there):
                pl.semaphore_signal(barrier, inc=1, device_id=there, device_id_type=MESH)
    near = [low.astype(jnp.int32) + high.astype(jnp.int32) for low, high in has]
    total = total + (near[0] + 1) * (near[1] + 1) * (near[2] + 1) - 1 - near[0] - near[1] - near[2]

    def split_store(ref, index, value):
        high = value.astype(bf16)
        ref[index + (0,)] = high
        ref[index + (1,)] = (value - high.astype(f32)).astype(bf16)

    KC = SPF * SY

    def ext_q(q):
        return jnp.where(q < PY, q, jnp.where(q < PY + 2, q - PY - 2, q - 2))

    rows, cols = iota((5 * QE, KC), 0), iota((5 * QE, KC), 1)
    split_store(wf_v, (), weight(cols // SY, rows // QE - 2, SPF)
                * weight(cols % SY, ext_q(rows % QE), SPF))
    rows, cols = iota((CR, KC), 0), iota((CR, KC), 1)
    side, inner = rows // 4, rows % 4
    along_y = weight(cols % SY, 2 * (side % 3) + inner % 2 - 2, SPC)
    for c in range(cells):
        split_store(wc_v, (c,),
                    weight(cols // SY + c * SPF, 2 * (side // 3) + inner // 2 - 2, SPC) * along_y)

    pl.semaphore_wait(barrier, total)

    pieces = ys_sem.shape[1]
    each = SX // pieces

    def halo(k, side, piece=0):
        if k == 1:
            part = pl.ds(piece * each, each)
            return neighbour_copy(
                k, side, ysend.at[side, part], yrecv.at[1 - side, part],
                ys_sem.at[side, piece], yr_sem.at[1 - side, piece])
        if k == 0:
            src = s_v.at[pl.ds(2 if side == 0 else SX, 2), pl.ds(8, SY), :]
            dst = s_v.at[pl.ds(SX + 2 if side == 0 else 0, 2), pl.ds(8, SY), :]
        else:
            src, dst = zsend.at[side], zrecv.at[1 - side]
        return neighbour_copy(k, side, src, dst, hs_sem.at[k, side], hr_sem.at[k, 1 - side])

    def neighbour_copy(k, side, src, dst, send, recv):
        other = me[k] - 1 if side == 0 else me[k] + 1
        return pltpu.make_async_remote_copy(
            src_ref=src, dst_ref=dst, send_sem=send, recv_sem=recv,
            device_id={axes[k]: other}, device_id_type=MESH,
        )

    def start_halo(k, side, piece=0):
        @pl.when(has[k][side])
        def _():
            halo(k, side, piece).start()

    lane = iota((SY, SZ), 1)

    def one_slab(x, carry):
        low, high = carry
        s = w_v[x] + f_v[x]
        s_v[x + 2, 8:8 + SY, :] = s
        ysend[0, x] = s[0:2]
        ysend[1, x] = s[SY - 2:SY]
        here = lane // 2 == x
        low = jnp.where(here, pltpu.roll(s, 2 * x, 1), low)
        high = jnp.where(here, pltpu.roll(s, lax.rem(2 * x + 2, SZ), 1), high)
        return low, high

    carry = (jnp.zeros((SY, SZ), f32), jnp.zeros((SY, SZ), f32))
    done = set()
    sent = set()
    for c in order:
        for copy in loads[c]:
            copy.wait()
        carry = lax.fori_loop(c * SPF, (c + 1) * SPF, one_slab, carry)
        done.add(c)
        for piece in range(pieces):
            inside = range(piece * each // SPF, (piece + 1) * each // SPF)
            if piece not in sent and all(n in done for n in inside):
                sent.add(piece)
                start_halo(1, 0, piece)
                start_halo(1, 1, piece)
        if c == 0:
            start_halo(0, 0)
        if c == cells - 1:
            start_halo(0, 1)
    zsend[0] = carry[0]
    zsend[1] = carry[1]
    start_halo(2, 0)
    start_halo(2, 1)

    accf[...] = jnp.zeros(accf.shape, f32)
    accc[...] = jnp.zeros(accc.shape, f32)

    for k in (0, 1, 2):
        for side in range(2):
            for piece in range(pieces if k == 1 else 1):
                @pl.when(has[k][1 - side])
                def _(k=k, side=side, piece=piece):
                    halo(k, side, piece).wait_recv()

    even = lane % 2 == 0
    dl = zrecv[0] - zsend[1]
    dh = zrecv[1] - zsend[0]
    zcorr[0] = jnp.where(even, dl - 8.0 * pltpu.roll(dl, SZ - 1, 1), dl)
    zcorr[1] = jnp.where(even, -dh, 8.0 * pltpu.roll(dh, 1, 1) - dh)

    def forces(i):
        slot = i % 2
        for xx in range(SPF):
            x = i * SPF + xx
            s_v[x + 2, 6:8, :] = yrecv[0, x]
            s_v[x + 2, 8 + SY:10 + SY, :] = yrecv[1, x]
            d = w_v[x] - f_v[x]
            s = s_v[x + 2, 8:8 + SY, :]
            gx = (s_v[x, 8:8 + SY, :] - s_v[x + 4, 8:8 + SY, :]
                  + 8.0 * (s_v[x + 3, 8:8 + SY, :] - s_v[x + 1, 8:8 + SY, :]))
            gy = (s_v[x + 2, 6:6 + SY, :] - s_v[x + 2, 10:10 + SY, :]
                  + 8.0 * (s_v[x + 2, 9:9 + SY, :] - s_v[x + 2, 7:7 + SY, :]))
            gz = (pltpu.roll(s, 2, 1) - pltpu.roll(s, SZ - 2, 1)
                  + 8.0 * (pltpu.roll(s, SZ - 1, 1) - pltpu.roll(s, 1, 1)))
            corr = jnp.where(lane < 2, pltpu.roll(zcorr[0], (SZ - 2 * x) % SZ, 1), 0.0)
            corr = jnp.where(lane >= SZ - 2,
                             pltpu.roll(zcorr[1], (2 * SZ - 2 - 2 * x) % SZ, 1), corr)
            gz = gz + corr
            for a, g in enumerate((gx, gy, gz)):
                force = g * d
                high = force.astype(bf16)
                fh_v[slot, xx * SY:(xx + 1) * SY, a * SZ:(a + 1) * SZ] = high
                fl_v[slot, xx * SY:(xx + 1) * SY, a * SZ:(a + 1) * SZ] = (
                    force - high.astype(f32)).astype(bf16)

    def gather(i):
        slot = i % 2
        many = 5 * QE + CR
        weights = jnp.concatenate([wf_v[0], wc_v[i, 0], wf_v[1], wc_v[i, 1]], axis=0)
        both = jnp.dot(weights, fh_v[slot], preferred_element_type=f32)
        out = both[:many] + both[many:] + jnp.dot(
            weights[:many], fl_v[slot], preferred_element_type=f32)
        fine = out[:5 * QE].reshape(5, 2, PY, lanes)
        accf[0, i:i + 5] += fine[:, 0]
        accf[1, i:i + 5] += fine[:, 1]
        accc[...] += out[5 * QE:]

    forces(0)
    for i in range(cells):
        if i + 1 < cells:
            forces(i + 1)
        gather(i)

    rows, cols = iota((SZ, 128), 0), iota((SZ, 128), 1)
    bzc = weight(rows, cols % 4 + 4 * (cols // 16 - 1), SPC) * (SPC ** -1.5 / 24.0)
    stack = jnp.concatenate([accc[:, a * SZ:(a + 1) * SZ] for a in range(3)], axis=0)
    shares = nn(stack, bzc)
    rows, cols = iota((CR, 128), 0), iota((CR, 128), 1)
    keep = (rows % 4 == (cols // 4) % 4) & (cols < 48)
    for f in range(3):
        value = shares[0:CR]
        value = value if f == 0 else pltpu.roll(value, 128 - 16 * f, 1)
        for a in (1, 2):
            moved = shares[a * CR:(a + 1) * CR]
            moved = moved if a == f else pltpu.roll(moved, (128 + 16 * (a - f)) % 128, 1)
            value = jnp.where(cols // 16 == a, moved, value)
        value = jnp.where(keep, value, 0.0).reshape(CR // 8, 8, 128)
        value = value + pltpu.roll(value, 7, 1)
        value = value + pltpu.roll(value, 6, 1)
        for s in range(9):
            row = 4 * (s % 2)
            cmsg[f * 9 + s] = value[s // 2, row:row + 1, :]

    def share_copy(n):
        there = toward(sides[n])[1]
        return pltpu.make_async_remote_copy(
            src_ref=cmsg.at[n], dst_ref=crecv.at[26 - n],
            send_sem=ns_sem.at[n], recv_sem=nr_sem.at[26 - n],
            device_id=there, device_id_type=MESH,
        )

    far = sorted((n for n in range(27) if n != 13),
                 key=lambda n: -sum(v != 1 for v in sides[n]))
    for n in far:
        @pl.when(toward(sides[n])[0])
        def _(n=n):
            share_copy(n).start()

    for copy in small:
        copy.wait()
    shape = (EX * QE, PX * PY)
    rows, cols = iota(shape, 0), iota(shape, 1)
    ox, oy = me[0] * PX, me[1] * PY
    outer, inner = rows // (EX * PY), rows % (EX * PY)
    planes = bend_planes(inner // PY - 2 + ox, ext_q(inner % PY + PY * outer) + oy,
                         cols // PY + ox, cols % PY + oy, PX * nx, PY * ny)
    RZ = tz_v.shape[2]

    def ext_point(row):
        return jnp.where(row < PZ, row, jnp.where(row < PZ + 2, row - PZ - 2, row - 2))

    oz = me[2] * PZ
    zr, zc = ext_point(iota((RZ, PZ), 0)) + oz, iota((RZ, PZ), 1) + oz
    along = (same(zr, zc), diff1(zr, zc), diff2(zr, zc, PZ * nz))
    for a in range(3):
        block = fc_ref[a].reshape(PX * PY, PZ)
        factors = [nn(plane, block) for plane in planes]
        for half in range(2):
            part = slice(half * EX * PY, (half + 1) * EX * PY)
            bend_v[half, a] = (nt(along[0], factors[0][part]) + nt(along[1], factors[1][part])
                               + nt(along[2], factors[2][part]))

    rows, cols = iota((RZ, SZ), 0), iota((RZ, SZ), 1)
    bz = weight(cols, ext_point(rows), SPF) * (SPF ** -1.5 / 24.0)
    for a in range(3):
        for half in range(2):
            block = accf[half, :, :, a * SZ:(a + 1) * SZ].reshape(EX * PY, SZ)
            tz_v[half, a] = nt(bz, block) + bend_v[half, a]
            for side in range(2):
                zmsg[side, half, 2 * a:2 * a + 2, :] = tz_v[
                    half, a, PZ + 2 * side:PZ + 2 * side + 2, :]

    def fine_copy(k, side):
        source, got = ((b_v, bgot), (a_v.at[1], agot), (zmsg.at[side], zgot))[k]
        return neighbour_copy(k, side, source, got.at[1 - side],
                              ms_sem.at[k, side], mr_sem.at[k, 1 - side])

    def fine_start(k):
        for side in range(2):
            @pl.when(has[k][side])
            def _(side=side):
                fine_copy(k, side).start()

    def fine_wait(k):
        for side in range(2):
            @pl.when(has[k][1 - side])
            def _(side=side):
                fine_copy(k, side).wait_recv()

    hz = nz // 2
    slots = (xrow.at[me[0]], xrow.at[me[0], me[1]], zrow.at[me[2]])

    def coarse_copy(k, d):
        return pltpu.make_async_remote_copy(
            src_ref=slots[k], dst_ref=slots[k],
            send_sem=cs_sem.at[k, d], recv_sem=cr_sem.at[k, d],
            device_id={axes[k]: lax.rem(me[k] + d, counts[k])}, device_id_type=MESH,
        )

    def coarse_from(k, d):
        other = lax.rem(me[k] + counts[k] - d, counts[k])
        slot = (xrow.at[other], xrow.at[me[0], other], zrow.at[other])[k]
        return pltpu.make_async_remote_copy(
            src_ref=slot, dst_ref=slot, send_sem=cs_sem.at[k, d], recv_sem=cr_sem.at[k, d],
            device_id={axes[k]: other}, device_id_type=MESH,
        )

    def coarse_start(k):
        n = counts[k]
        for d in sorted(range(1, n), key=lambda d: -min(d, n - d)):
            coarse_copy(k, d).start()

    def coarse_wait(k):
        for d in range(1, counts[k]):
            coarse_from(k, d).wait_recv()

    fine_start(2)

    for n in range(27):
        if n != 13:
            @pl.when(toward(sides[n])[0])
            def _(n=n):
                share_copy(26 - n).wait_recv()
    own = cmsg[13]
    for n in range(27):
        if n != 13:
            own = own + crecv[n]
    zrow[me[2]] = own
    coarse_start(2)

    fine_wait(2)
    for half in range(2):
        for a in range(3):
            tz_v[half, a, 0:2, :] = tz_v[half, a, 0:2, :] + zgot[0, half, 2 * a:2 * a + 2, :]
            tz_v[half, a, PZ - 2:PZ, :] = (
                tz_v[half, a, PZ - 2:PZ, :] + zgot[1, half, 2 * a:2 * a + 2, :])
            a_v[half, a * PZ:(a + 1) * PZ, :] = tz_v[half, a, 0:PZ, :]
    fine_start(1)

    q_at, r_at = iota((KX, KY, 128), 1), iota((KX, KY, 128), 2)

    def laplace(c):
        zero = jnp.zeros((1, KY, 128), f32)
        total = (jnp.concatenate([c[1:], zero], axis=0) + jnp.concatenate([zero, c[:-1]], axis=0)
                 + jnp.where(q_at < KY - 1, pltpu.roll(c, KY - 1, 1), 0.0)
                 + jnp.where(q_at > 0, pltpu.roll(c, 1, 1), 0.0)
                 + pltpu.roll(c, 127, 2) + pltpu.roll(c, 1, 2))
        return jnp.where(r_at < KZ, total - 6.0 * c, 0.0)

    clane[...] = jnp.zeros(clane.shape, f32)
    for a in range(3):
        clane[:, :, 0:KZ] = cc_ref[a]
        cbend[a] = BEND * laplace(laplace(clane[...]))

    coarse_wait(2)
    for kk in range(hz):
        xrow[me[0], me[1], kk] = zrow[kk] + pltpu.roll(zrow[kk + hz], 64, 1)
    coarse_start(1)

    fine_wait(1)
    shape = (EX * PY, EX * PY)
    rows, cols = iota(shape, 0), iota(shape, 1)
    p_same = rows // PY == cols // PY
    q, r = rows % PY, cols % PY
    low = jnp.where(p_same & (q == r + 2) & (r < 2), 1.0, 0.0)
    high = jnp.where(p_same & (q == r - (PY - 2)) & (r >= PY - 2), 1.0, 0.0)
    b_v[...] = a_v[0] + nn(agot[0], low) + nn(agot[1], high)
    fine_start(0)

    coarse_wait(1)
    coarse_start(0)

    fine_wait(0)
    shape = (PX * PY, EX * PY)
    rows, cols = iota(shape, 0), iota(shape, 1)
    own = jnp.where(cols == rows + 2 * PY, 1.0, 0.0)
    low = jnp.where((cols == rows + (PX + 2) * PY) & (rows < 2 * PY), 1.0, 0.0)
    high = jnp.where((cols == rows - (PX - 2) * PY) & (rows >= (PX - 2) * PY), 1.0, 0.0)
    for a in range(3):
        part = slice(a * PZ, (a + 1) * PZ)
        out = nt(own, b_v[part]) + nt(low, bgot[0, part]) + nt(high, bgot[1, part])
        fo_ref[a] = out.reshape(PX, PY, PZ)

    coarse_wait(0)
    sub, at = iota((ny, 128), 0), iota((ny, 128), 1)
    for i in range(nx):
        pages = []
        for kk in range(hz):
            page = jnp.broadcast_to(xrow[i, 0, kk], (ny, 128))
            for j in range(1, ny):
                page = jnp.where(sub == j, jnp.broadcast_to(xrow[i, j, kk], (ny, 128)), page)
            pages.append(page)
        for a in range(3):
            for g in range(4):
                c = 4 * a + g
                value = None
                for kk in range(hz):
                    shift = (128 + 4 * kk - 4 * c) % 128
                    moved = pages[kk] if shift == 0 else pltpu.roll(pages[kk], shift, 1)
                    value = moved if kk == 0 else jnp.where(
                        (at % 64) // 4 == kk, moved, value)
                value = jnp.where(at < 4 * hz, value, pltpu.roll(value, 64 + 4 * hz, 1))
                p = 2 * i + g // 2
                part = pl.ds(g % 2, ny, stride=2)
                co_ref[a, p, part, :] = (value + cbend[a, p, part, :])[:, 0:KZ]

    for n in range(27):
        if n != 13:
            @pl.when(toward(sides[n])[0])
            def _(n=n):
                share_copy(n).wait_send()
    for k in range(3):
        for side in range(2):
            @pl.when(has[k][side])
            def _(k=k, side=side):
                for piece in range(pieces if k == 1 else 1):
                    halo(k, side, piece).wait_send()
                fine_copy(k, side).wait_send()
        for d in range(1, counts[k]):
            coarse_copy(k, d).wait_send()


def solution(mesh):
    sizes = tuple(mesh.shape[a] for a in ("gx", "gy", "gz"))

    def step(warped, fixed, fine, coarse):
        SX, SY, SZ = warped.shape
        PX, PY, PZ = SX // SPF, SY // SPF, SZ // SPF
        KX, KY, KZ = coarse.shape[1:]
        EX, QE, RZ = PX + 4, 2 * PY, PZ + 8
        CR = 48
        KC = SPF * SY
        most = max(sizes)
        vmem = pl.BlockSpec(memory_space=pltpu.VMEM)
        hbm = pl.BlockSpec(memory_space=pltpu.HBM)
        V = pltpu.VMEM
        D = pltpu.SemaphoreType.DMA
        return pl.pallas_call(
            functools.partial(kernel, sizes),
            out_shape=(jax.ShapeDtypeStruct(fine.shape, f32),
                       jax.ShapeDtypeStruct(coarse.shape, f32)),
            in_specs=[hbm] * 4,
            out_specs=(vmem, vmem),
            scratch_shapes=[
                V((SX, SY, SZ), f32), V((SX, SY, SZ), f32),
                V((3, PX, PY, PZ), f32), V(coarse.shape, f32),
                V((SX + 4, SY + 16, SZ), f32),
                V((2, SX, 2, SZ), f32), V((2, SX, 2, SZ), f32),
                V((2, SY, SZ), f32), V((2, SY, SZ), f32), V((2, SY, SZ), f32),
                V((2, 5 * QE, KC), bf16), V((SX // SPF, 2, CR, KC), bf16),
                V((2, KC, 3 * SZ), bf16), V((2, KC, 3 * SZ), bf16),
                V((2, EX, PY, 3 * SZ), f32), V((CR, 3 * SZ), f32),
                V((2, 3, RZ, EX * PY), f32), V((2, 3, RZ, EX * PY), f32),
                V((KX, KY, 128), f32), V((3, KX, KY, 128), f32),
                V((2, 2, 8, EX * PY), f32), V((2, 2, 8, EX * PY), f32),
                V((2, 3 * PZ, EX * PY), f32), V((2, 3 * PZ, EX * PY), f32),
                V((3 * PZ, EX * PY), f32), V((2, 3 * PZ, EX * PY), f32),
                V((27, 1, 128), f32), V((27, 1, 128), f32),
                V((sizes[2], 1, 128), f32),
                V((sizes[0], sizes[1], sizes[2] // 2, 1, 128), f32),
                D((2, SX // SPF)), D((2,)), D((3, 2)), D((3, 2)), D((2, 4)), D((2, 4)),
                D((3, 2)), D((3, 2)), D((27,)), D((27,)), D((3, most)), D((3, most)),
            ],
            compiler_params=pltpu.CompilerParams(
                collective_id=0, has_side_effects=True, vmem_limit_bytes=66000000
            ),
        )(warped, fixed, fine, coarse)

    in_specs = (P("gx", "gy", "gz"), P("gx", "gy", "gz"), P(None, "gx", "gy", "gz"), P())
    out_specs = (P(None, "gx", "gy", "gz"), P())
    return jax.shard_map(
        step, mesh=mesh, in_specs=in_specs, out_specs=out_specs, check_vma=False
    )
```

```python
import functools

import jax
import jax.numpy as jnp
from jax import lax
from jax.experimental import pallas as pl
from jax.experimental.pallas import tpu as pltpu
from jax.sharding import PartitionSpec as P

SPF = 8
SPC = 32
BEND = 0.01
HI = lax.Precision.HIGHEST
MESH = pl.DeviceIdType.MESH
f32 = jnp.float32
bf16 = jnp.bfloat16


def nn(a, b):
    return lax.dot_general(
        a, b, (((1,), (0,)), ((), ())), precision=HI, preferred_element_type=f32
    )


def nt(a, b):
    return lax.dot_general(
        a, b, (((1,), (1,)), ((), ())), precision=HI, preferred_element_type=f32
    )


def spline(t):
    m = jnp.abs(t)
    inner = 2.0 / 3.0 - m * m + 0.5 * m * m * m
    r = 2.0 - m
    outer = r * r * r * (1.0 / 6.0)
    return jnp.where(m < 1.0, inner, jnp.where(m < 2.0, outer, 0.0))


def weight(voxel, point, spacing):
    scaled = (2 * voxel + 1 - spacing * (2 * point + 1)).astype(f32)
    return spline(scaled * (0.5 / spacing))


def iota(shape, axis):
    return lax.broadcasted_iota(jnp.int32, shape, axis)


def diff1(out, inp):
    d = jnp.abs(out - inp)
    return jnp.where(d == 0, -2.0, jnp.where(d == 1, 1.0, 0.0)).astype(f32)


def diff2(out, inp, count):
    d = jnp.abs(out - inp)
    edge = (inp == 0) | (inp == count - 1)
    centre = jnp.where(edge, 5.0, 6.0)
    return jnp.where(
        d == 0, centre, jnp.where(d == 1, -4.0, jnp.where(d == 2, 1.0, 0.0))
    ).astype(f32)


def same(out, inp):
    return jnp.where(out == inp, 1.0, 0.0).astype(f32)


def bend_planes(px, py, qx, qy, cx, cy):
    jx, jy = same(px, qx), same(py, qy)
    tx, ty = diff1(px, qx), diff1(py, qy)
    m0 = diff2(px, qx, cx) * jy + jx * diff2(py, qy, cy) + 2.0 * tx * ty
    m1 = 2.0 * (tx * jy + jx * ty)
    return m0 * BEND, m1 * BEND, jx * jy * BEND


def kernel(sizes, w_hbm, f_hbm, fc_hbm, cc_hbm, fo_ref, co_ref,
           w_v, f_v, fc_ref, cc_ref, s_v, ysend, yrecv, zsend, zrecv, zcorr,
           wf_v, wc_v, fh_v, fl_v,
           accf, accc, tz_v, bend_v, clane, cbend, zmsg, zgot, a_v, agot, b_v, bgot,
           cmsg, crecv, zrow, xrow, load_sem, small_sem, hs_sem, hr_sem, ys_sem, yr_sem,
           ms_sem, mr_sem, ns_sem, nr_sem, cs_sem, cr_sem):
    nx, ny, nz = sizes
    axes = ("gx", "gy", "gz")
    counts = sizes
    me = [lax.axis_index(a) for a in axes]
    SX, SY, SZ = w_v.shape
    PX, PY, PZ = SX // SPF, SY // SPF, SZ // SPF
    KX, KY, KZ = cc_ref.shape[1:]
    EX, QE = PX + 4, 2 * PY
    CR = accc.shape[0]
    cells = SX // SPF
    lanes = 3 * SZ

    loads = []
    for c in range(cells):
        part = pl.ds(c * SPF, SPF)
        loads.append((
            pltpu.make_async_copy(w_hbm.at[part], w_v.at[part], load_sem.at[0, c]),
            pltpu.make_async_copy(f_hbm.at[part], f_v.at[part], load_sem.at[1, c]),
        ))
    small = (pltpu.make_async_copy(fc_hbm, fc_ref, small_sem.at[0]),
             pltpu.make_async_copy(cc_hbm, cc_ref, small_sem.at[1]))
    order = [0, cells - 1] + list(range(1, cells - 1))
    for c in order:
        loads[c][0].start()
        loads[c][1].start()
    for copy in small:
        copy.start()

    has = [(me[k] > 0, me[k] < counts[k] - 1) for k in range(3)]
    sides = [(d, e, f) for f in range(3) for d in range(3) for e in range(3)]

    def toward(step):
        ok = None
        for k in range(3):
            if step[k] != 1:
                here = has[k][0] if step[k] == 0 else has[k][1]
                ok = here if ok is None else ok & here
        return ok, {axes[k]: me[k] + (step[k] - 1) for k in range(3) if step[k] != 1}

    zero_plane = jnp.zeros((2, SY, SZ), f32)
    s_v[0:2, 8:8 + SY, :] = zero_plane
    s_v[SX + 2:SX + 4, 8:8 + SY, :] = zero_plane
    yrecv[...] = jnp.zeros(yrecv.shape, f32)
    zrecv[...] = jnp.zeros(zrecv.shape, f32)
    zgot[...] = jnp.zeros(zgot.shape, f32)
    agot[...] = jnp.zeros(agot.shape, f32)
    bgot[...] = jnp.zeros(bgot.shape, f32)
    crecv[...] = jnp.zeros(crecv.shape, f32)

    barrier = pltpu.get_barrier_semaphore()
    total = 0
    for k, a in enumerate(axes):
        for d in range(1, counts[k]):
            pl.semaphore_signal(
                barrier, inc=1, device_id={a: lax.rem(me[k] + d, counts[k])}, device_id_type=MESH
            )
            total += 1
    for step in sides:
        if sum(n != 1 for n in step) >= 2:
            ok, there = toward(step)

            @pl.when(ok)
            def _(there=there):
                pl.semaphore_signal(barrier, inc=1, device_id=there, device_id_type=MESH)
    near = [low.astype(jnp.int32) + high.astype(jnp.int32) for low, high in has]
    total = total + (near[0] + 1) * (near[1] + 1) * (near[2] + 1) - 1 - near[0] - near[1] - near[2]

    def split_store(ref, index, value):
        high = value.astype(bf16)
        ref[index + (0,)] = high
        ref[index + (1,)] = (value - high.astype(f32)).astype(bf16)

    KC = SPF * SY

    def ext_q(q):
        return jnp.where(q < PY, q, jnp.where(q < PY + 2, q - PY - 2, q - 2))

    rows, cols = iota((5 * QE, KC), 0), iota((5 * QE, KC), 1)
    split_store(wf_v, (), weight(cols // SY, rows // QE - 2, SPF)
                * weight(cols % SY, ext_q(rows % QE), SPF))
    rows, cols = iota((CR, KC), 0), iota((CR, KC), 1)
    side, inner = rows // 4, rows % 4
    along_y = weight(cols % SY, 2 * (side % 3) + inner % 2 - 2, SPC)
    for c in range(cells):
        split_store(wc_v, (c,),
                    weight(cols // SY + c * SPF, 2 * (side // 3) + inner // 2 - 2, SPC) * along_y)

    pl.semaphore_wait(barrier, total)

    pieces = ys_sem.shape[1]
    each = SX // pieces

    def halo(k, side, piece=0):
        if k == 1:
            part = pl.ds(piece * each, each)
            return neighbour_copy(
                k, side, ysend.at[side, part], yrecv.at[1 - side, part],
                ys_sem.at[side, piece], yr_sem.at[1 - side, piece])
        if k == 0:
            src = s_v.at[pl.ds(2 if side == 0 else SX, 2), pl.ds(8, SY), :]
            dst = s_v.at[pl.ds(SX + 2 if side == 0 else 0, 2), pl.ds(8, SY), :]
        else:
            src, dst = zsend.at[side], zrecv.at[1 - side]
        return neighbour_copy(k, side, src, dst, hs_sem.at[k, side], hr_sem.at[k, 1 - side])

    def neighbour_copy(k, side, src, dst, send, recv):
        other = me[k] - 1 if side == 0 else me[k] + 1
        return pltpu.make_async_remote_copy(
            src_ref=src, dst_ref=dst, send_sem=send, recv_sem=recv,
            device_id={axes[k]: other}, device_id_type=MESH,
        )

    def start_halo(k, side, piece=0):
        @pl.when(has[k][side])
        def _():
            halo(k, side, piece).start()

    lane = iota((SY, SZ), 1)

    def one_slab(x, carry):
        low, high = carry
        s = w_v[x] + f_v[x]
        s_v[x + 2, 8:8 + SY, :] = s
        ysend[0, x] = s[0:2]
        ysend[1, x] = s[SY - 2:SY]
        here = lane // 2 == x
        low = jnp.where(here, pltpu.roll(s, 2 * x, 1) if x else s, low)
        shift = (2 * x + 2) % SZ
        high = jnp.where(here, pltpu.roll(s, shift, 1) if shift else s, high)
        return low, high

    carry = (jnp.zeros((SY, SZ), f32), jnp.zeros((SY, SZ), f32))
    done = set()
    sent = set()
    for c in order:
        for copy in loads[c]:
            copy.wait()
        for x in range(c * SPF, (c + 1) * SPF):
            carry = one_slab(x, carry)
        done.add(c)
        for piece in range(pieces):
            inside = range(piece * each // SPF, (piece + 1) * each // SPF)
            if piece not in sent and all(n in done for n in inside):
                sent.add(piece)
                start_halo(1, 0, piece)
                start_halo(1, 1, piece)
        if c == 0:
            start_halo(0, 0)
        if c == cells - 1:
            start_halo(0, 1)
    zsend[0] = carry[0]
    zsend[1] = carry[1]
    start_halo(2, 0)
    start_halo(2, 1)

    accf[...] = jnp.zeros(accf.shape, f32)
    accc[...] = jnp.zeros(accc.shape, f32)

    for copy in small:
        copy.wait()
    shape = (EX * QE, PX * PY)
    rows, cols = iota(shape, 0), iota(shape, 1)
    ox, oy = me[0] * PX, me[1] * PY
    outer, inner = rows // (EX * PY), rows % (EX * PY)
    planes = bend_planes(inner // PY - 2 + ox, ext_q(inner % PY + PY * outer) + oy,
                         cols // PY + ox, cols % PY + oy, PX * nx, PY * ny)
    RZ = tz_v.shape[2]

    def ext_point(row):
        return jnp.where(row < PZ, row, jnp.where(row < PZ + 2, row - PZ - 2, row - 2))

    oz = me[2] * PZ
    zr, zc = ext_point(iota((RZ, PZ), 0)) + oz, iota((RZ, PZ), 1) + oz
    along = (same(zr, zc), diff1(zr, zc), diff2(zr, zc, PZ * nz))
    for a in range(3):
        block = fc_ref[a].reshape(PX * PY, PZ)
        factors = [nn(plane, block) for plane in planes]
        for half in range(2):
            part = slice(half * EX * PY, (half + 1) * EX * PY)
            bend_v[half, a] = (nt(along[0], factors[0][part]) + nt(along[1], factors[1][part])
                               + nt(along[2], factors[2][part]))

    for k in (0, 1, 2):
        for side in range(2):
            for piece in range(pieces if k == 1 else 1):
                @pl.when(has[k][1 - side])
                def _(k=k, side=side, piece=piece):
                    halo(k, side, piece).wait_recv()

    even = lane % 2 == 0
    dl = zrecv[0] - zsend[1]
    dh = zrecv[1] - zsend[0]
    zcorr[0] = jnp.where(even, dl - 8.0 * pltpu.roll(dl, SZ - 1, 1), dl)
    zcorr[1] = jnp.where(even, -dh, 8.0 * pltpu.roll(dh, 1, 1) - dh)

    def forces(i):
        slot = i % 2
        for xx in range(SPF):
            x = i * SPF + xx
            s_v[x + 2, 6:8, :] = yrecv[0, x]
            s_v[x + 2, 8 + SY:10 + SY, :] = yrecv[1, x]
            d = w_v[x] - f_v[x]
            s = s_v[x + 2, 8:8 + SY, :]
            gx = (s_v[x, 8:8 + SY, :] - s_v[x + 4, 8:8 + SY, :]
                  + 8.0 * (s_v[x + 3, 8:8 + SY, :] - s_v[x + 1, 8:8 + SY, :]))
            gy = (s_v[x + 2, 6:6 + SY, :] - s_v[x + 2, 10:10 + SY, :]
                  + 8.0 * (s_v[x + 2, 9:9 + SY, :] - s_v[x + 2, 7:7 + SY, :]))
            gz = (pltpu.roll(s, 2, 1) - pltpu.roll(s, SZ - 2, 1)
                  + 8.0 * (pltpu.roll(s, SZ - 1, 1) - pltpu.roll(s, 1, 1)))
            corr = jnp.where(lane < 2, pltpu.roll(zcorr[0], (SZ - 2 * x) % SZ, 1), 0.0)
            corr = jnp.where(lane >= SZ - 2,
                             pltpu.roll(zcorr[1], (2 * SZ - 2 - 2 * x) % SZ, 1), corr)
            gz = gz + corr
            for a, g in enumerate((gx, gy, gz)):
                force = g * d
                high = force.astype(bf16)
                fh_v[slot, xx * SY:(xx + 1) * SY, a * SZ:(a + 1) * SZ] = high
                fl_v[slot, xx * SY:(xx + 1) * SY, a * SZ:(a + 1) * SZ] = (
                    force - high.astype(f32)).astype(bf16)

    def gather(i):
        slot = i % 2
        many = 5 * QE + CR
        weights = jnp.concatenate([wf_v[0], wc_v[i, 0], wf_v[1], wc_v[i, 1]], axis=0)
        both = jnp.dot(weights, fh_v[slot], preferred_element_type=f32)
        out = both[:many] + both[many:] + jnp.dot(
            weights[:many], fl_v[slot], preferred_element_type=f32)
        fine = out[:5 * QE].reshape(5, 2, PY, lanes)
        accf[0, i:i + 5] += fine[:, 0]
        accf[1, i:i + 5] += fine[:, 1]
        accc[...] += out[5 * QE:]

    forces(0)
    for i in range(cells):
        if i + 1 < cells:
            forces(i + 1)
        gather(i)

    rows, cols = iota((SZ, 128), 0), iota((SZ, 128), 1)
    bzc = weight(rows, cols % 4 + 4 * (cols // 16 - 1), SPC) * (SPC ** -1.5 / 24.0)
    stack = jnp.concatenate([accc[:, a * SZ:(a + 1) * SZ] for a in range(3)], axis=0)
    shares = nn(stack, bzc)
    rows, cols = iota((CR, 128), 0), iota((CR, 128), 1)
    keep = (rows % 4 == (cols // 4) % 4) & (cols < 48)
    for f in range(3):
        value = shares[0:CR]
        value = value if f == 0 else pltpu.roll(value, 128 - 16 * f, 1)
        for a in (1, 2):
            moved = shares[a * CR:(a + 1) * CR]
            moved = moved if a == f else pltpu.roll(moved, (128 + 16 * (a - f)) % 128, 1)
            value = jnp.where(cols // 16 == a, moved, value)
        value = jnp.where(keep, value, 0.0).reshape(CR // 8, 8, 128)
        value = value + pltpu.roll(value, 7, 1)
        value = value + pltpu.roll(value, 6, 1)
        for s in range(9):
            row = 4 * (s % 2)
            cmsg[f * 9 + s] = value[s // 2, row:row + 1, :]

    def share_copy(n):
        there = toward(sides[n])[1]
        return pltpu.make_async_remote_copy(
            src_ref=cmsg.at[n], dst_ref=crecv.at[26 - n],
            send_sem=ns_sem.at[n], recv_sem=nr_sem.at[26 - n],
            device_id=there, device_id_type=MESH,
        )

    far = sorted((n for n in range(27) if n != 13),
                 key=lambda n: -sum(v != 1 for v in sides[n]))
    for n in far:
        @pl.when(toward(sides[n])[0])
        def _(n=n):
            share_copy(n).start()

    rows, cols = iota((RZ, SZ), 0), iota((RZ, SZ), 1)
    bz = weight(cols, ext_point(rows), SPF) * (SPF ** -1.5 / 24.0)
    for a in range(3):
        for half in range(2):
            block = accf[half, :, :, a * SZ:(a + 1) * SZ].reshape(EX * PY, SZ)
            tz_v[half, a] = nt(bz, block) + bend_v[half, a]
            for side in range(2):
                zmsg[side, half, 2 * a:2 * a + 2, :] = tz_v[
                    half, a, PZ + 2 * side:PZ + 2 * side + 2, :]

    def fine_copy(k, side):
        source, got = ((b_v, bgot), (a_v.at[1], agot), (zmsg.at[side], zgot))[k]
        return neighbour_copy(k, side, source, got.at[1 - side],
                              ms_sem.at[k, side], mr_sem.at[k, 1 - side])

    def fine_start(k):
        for side in range(2):
            @pl.when(has[k][side])
            def _(side=side):
                fine_copy(k, side).start()

    def fine_wait(k):
        for side in range(2):
            @pl.when(has[k][1 - side])
            def _(side=side):
                fine_copy(k, side).wait_recv()

    def coarse_slot(k, n):
        if k == 0:
            return xrow.at[n]
        if k == 1:
            return xrow.at[me[0], :, pl.ds(n, 1), :]
        return zrow.at[:, pl.ds(n, 1), :]

    def coarse_copy(k, d):
        return pltpu.make_async_remote_copy(
            src_ref=coarse_slot(k, me[k]), dst_ref=coarse_slot(k, me[k]),
            send_sem=cs_sem.at[k, d], recv_sem=cr_sem.at[k, d],
            device_id={axes[k]: lax.rem(me[k] + d, counts[k])}, device_id_type=MESH,
        )

    def coarse_from(k, d):
        other = lax.rem(me[k] + counts[k] - d, counts[k])
        return pltpu.make_async_remote_copy(
            src_ref=coarse_slot(k, other), dst_ref=coarse_slot(k, other),
            send_sem=cs_sem.at[k, d], recv_sem=cr_sem.at[k, d],
            device_id={axes[k]: other}, device_id_type=MESH,
        )

    def coarse_start(k):
        n = counts[k]
        for d in sorted(range(1, n), key=lambda d: -min(d, n - d)):
            coarse_copy(k, d).start()

    def coarse_wait(k):
        for d in range(1, counts[k]):
            coarse_from(k, d).wait_recv()

    fine_start(2)

    for n in range(27):
        if n != 13:
            @pl.when(toward(sides[n])[0])
            def _(n=n):
                share_copy(26 - n).wait_recv()
    own = cmsg[13]
    for n in range(27):
        if n != 13:
            own = own + crecv[n]
    at = iota((1, 128), 1)
    own = pltpu.roll(own, 4 * me[2], 1)
    for a in range(3):
        value = own if a == 0 else pltpu.roll(own, 128 - 16 * a, 1)
        for g in range(1, 4):
            value = jnp.where(at // 32 == g, pltpu.roll(own, (128 + 28 * g - 16 * a) % 128, 1), value)
        zrow[a, pl.ds(me[2], 1), :] = jnp.where((at % 32) // 4 == me[2], value, 0.0)
    coarse_start(2)

    fine_wait(2)
    for half in range(2):
        for a in range(3):
            tz_v[half, a, 0:2, :] = tz_v[half, a, 0:2, :] + zgot[0, half, 2 * a:2 * a + 2, :]
            tz_v[half, a, PZ - 2:PZ, :] = (
                tz_v[half, a, PZ - 2:PZ, :] + zgot[1, half, 2 * a:2 * a + 2, :])
            a_v[half, a * PZ:(a + 1) * PZ, :] = tz_v[half, a, 0:PZ, :]
    fine_start(1)

    q_at, r_at = iota((KX, KY, 128), 1), iota((KX, KY, 128), 2)

    def laplace(c):
        zero = jnp.zeros((1, KY, 128), f32)
        total = (jnp.concatenate([c[1:], zero], axis=0) + jnp.concatenate([zero, c[:-1]], axis=0)
                 + jnp.where(q_at < KY - 1, pltpu.roll(c, KY - 1, 1), 0.0)
                 + jnp.where(q_at > 0, pltpu.roll(c, 1, 1), 0.0)
                 + pltpu.roll(c, 127, 2) + pltpu.roll(c, 1, 2))
        return jnp.where(r_at < KZ, total - 6.0 * c, 0.0)

    clane[...] = jnp.zeros(clane.shape, f32)
    for a in range(3):
        clane[:, :, 0:KZ] = cc_ref[a]
        cbend[a] = BEND * laplace(laplace(clane[...]))

    coarse_wait(2)
    for a in range(3):
        xrow[me[0], a, pl.ds(me[1], 1), :] = jnp.sum(zrow[a], axis=0, keepdims=True)
    coarse_start(1)

    fine_wait(1)
    shape = (EX * PY, EX * PY)
    rows, cols = iota(shape, 0), iota(shape, 1)
    p_same = rows // PY == cols // PY
    q, r = rows % PY, cols % PY
    low = jnp.where(p_same & (q == r + 2) & (r < 2), 1.0, 0.0)
    high = jnp.where(p_same & (q == r - (PY - 2)) & (r >= PY - 2), 1.0, 0.0)
    b_v[...] = a_v[0] + nn(agot[0], low) + nn(agot[1], high)
    fine_start(0)

    coarse_wait(1)
    coarse_start(0)

    fine_wait(0)
    shape = (PX * PY, EX * PY)
    rows, cols = iota(shape, 0), iota(shape, 1)
    own = jnp.where(cols == rows + 2 * PY, 1.0, 0.0)
    low = jnp.where((cols == rows + (PX + 2) * PY) & (rows < 2 * PY), 1.0, 0.0)
    high = jnp.where((cols == rows - (PX - 2) * PY) & (rows >= (PX - 2) * PY), 1.0, 0.0)
    for a in range(3):
        part = slice(a * PZ, (a + 1) * PZ)
        out = nt(own, b_v[part]) + nt(low, bgot[0, part]) + nt(high, bgot[1, part])
        fo_ref[a] = out.reshape(PX, PY, PZ)

    coarse_wait(0)
    for i in range(nx):
        for a in range(3):
            block = xrow[i, a]
            for g in range(4):
                value = block if g == 0 else pltpu.roll(block, 128 - 32 * g, 1)
                p = 2 * i + g // 2
                part = pl.ds(g % 2, ny, stride=2)
                co_ref[a, p, part, :] = (value + cbend[a, p, part, :])[:, 0:KZ]

    for n in range(27):
        if n != 13:
            @pl.when(toward(sides[n])[0])
            def _(n=n):
                share_copy(n).wait_send()
    for k in range(3):
        for side in range(2):
            @pl.when(has[k][side])
            def _(k=k, side=side):
                for piece in range(pieces if k == 1 else 1):
                    halo(k, side, piece).wait_send()
                fine_copy(k, side).wait_send()
        for d in range(1, counts[k]):
            coarse_copy(k, d).wait_send()


def solution(mesh):
    sizes = tuple(mesh.shape[a] for a in ("gx", "gy", "gz"))

    def step(warped, fixed, fine, coarse):
        SX, SY, SZ = warped.shape
        PX, PY, PZ = SX // SPF, SY // SPF, SZ // SPF
        KX, KY, KZ = coarse.shape[1:]
        EX, QE, RZ = PX + 4, 2 * PY, PZ + 8
        CR = 48
        KC = SPF * SY
        most = max(sizes)
        vmem = pl.BlockSpec(memory_space=pltpu.VMEM)
        hbm = pl.BlockSpec(memory_space=pltpu.HBM)
        V = pltpu.VMEM
        D = pltpu.SemaphoreType.DMA
        return pl.pallas_call(
            functools.partial(kernel, sizes),
            out_shape=(V(fine.shape, f32), V(coarse.shape, f32)),
            in_specs=[hbm] * 4,
            out_specs=(vmem, vmem),
            scratch_shapes=[
                V((SX, SY, SZ), f32), V((SX, SY, SZ), f32),
                V((3, PX, PY, PZ), f32), V(coarse.shape, f32),
                V((SX + 4, SY + 16, SZ), f32),
                V((2, SX, 2, SZ), f32), V((2, SX, 2, SZ), f32),
                V((2, SY, SZ), f32), V((2, SY, SZ), f32), V((2, SY, SZ), f32),
                V((2, 5 * QE, KC), bf16), V((SX // SPF, 2, CR, KC), bf16),
                V((2, KC, 3 * SZ), bf16), V((2, KC, 3 * SZ), bf16),
                V((2, EX, PY, 3 * SZ), f32), V((CR, 3 * SZ), f32),
                V((2, 3, RZ, EX * PY), f32), V((2, 3, RZ, EX * PY), f32),
                V((KX, KY, 128), f32), V((3, KX, KY, 128), f32),
                V((2, 2, 8, EX * PY), f32), V((2, 2, 8, EX * PY), f32),
                V((2, 3 * PZ, EX * PY), f32), V((2, 3 * PZ, EX * PY), f32),
                V((3 * PZ, EX * PY), f32), V((2, 3 * PZ, EX * PY), f32),
                V((27, 1, 128), f32), V((27, 1, 128), f32),
                V((3, sizes[2], 128), f32), V((sizes[0], 3, sizes[1], 128), f32),
                D((2, SX // SPF)), D((2,)), D((3, 2)), D((3, 2)), D((2, 4)), D((2, 4)),
                D((3, 2)), D((3, 2)), D((27,)), D((27,)), D((3, most)), D((3, most)),
            ],
            compiler_params=pltpu.CompilerParams(
                collective_id=0, has_side_effects=True, vmem_limit_bytes=66000000
            ),
        )(warped, fixed, fine, coarse)

    in_specs = (P("gx", "gy", "gz"), P("gx", "gy", "gz"), P(None, "gx", "gy", "gz"), P())
    out_specs = (P(None, "gx", "gy", "gz"), P())
    return jax.shard_map(
        step, mesh=mesh, in_specs=in_specs, out_specs=out_specs, check_vma=False
    )
```

```python
import functools

import jax
import jax.numpy as jnp
from jax import lax
from jax.experimental import pallas as pl
from jax.experimental.pallas import tpu as pltpu
from jax.sharding import PartitionSpec as P

SPF = 8
SPC = 32
BEND = 0.01
HI = lax.Precision.HIGHEST
MESH = pl.DeviceIdType.MESH
f32 = jnp.float32
bf16 = jnp.bfloat16


def nn(a, b):
    return lax.dot_general(
        a, b, (((1,), (0,)), ((), ())), precision=HI, preferred_element_type=f32
    )


def nt(a, b):
    return lax.dot_general(
        a, b, (((1,), (1,)), ((), ())), precision=HI, preferred_element_type=f32
    )


def spline(t):
    m = jnp.abs(t)
    inner = 2.0 / 3.0 - m * m + 0.5 * m * m * m
    r = 2.0 - m
    outer = r * r * r * (1.0 / 6.0)
    return jnp.where(m < 1.0, inner, jnp.where(m < 2.0, outer, 0.0))


def weight(voxel, point, spacing):
    scaled = (2 * voxel + 1 - spacing * (2 * point + 1)).astype(f32)
    return spline(scaled * (0.5 / spacing))


def iota(shape, axis):
    return lax.broadcasted_iota(jnp.int32, shape, axis)


def diff1(out, inp):
    d = jnp.abs(out - inp)
    return jnp.where(d == 0, -2.0, jnp.where(d == 1, 1.0, 0.0)).astype(f32)


def diff2(out, inp, count):
    d = jnp.abs(out - inp)
    edge = (inp == 0) | (inp == count - 1)
    centre = jnp.where(edge, 5.0, 6.0)
    return jnp.where(
        d == 0, centre, jnp.where(d == 1, -4.0, jnp.where(d == 2, 1.0, 0.0))
    ).astype(f32)


def same(out, inp):
    return jnp.where(out == inp, 1.0, 0.0).astype(f32)


def bend_planes(px, py, qx, qy, cx, cy):
    jx, jy = same(px, qx), same(py, qy)
    tx, ty = diff1(px, qx), diff1(py, qy)
    m0 = diff2(px, qx, cx) * jy + jx * diff2(py, qy, cy) + 2.0 * tx * ty
    m1 = 2.0 * (tx * jy + jx * ty)
    return m0 * BEND, m1 * BEND, jx * jy * BEND


def kernel(sizes, w_hbm, f_hbm, fc_hbm, cc_hbm, fo_ref, co_ref,
           w_v, f_v, fc_ref, cc_ref, s_v, xrecv, ysend, yrecv, yd, zsend, zrecv, zd,
           wf_v, wc_v, wy_v, wxe_v, fh_v, fl_v,
           accf, accc, tz_v, clane, cbend, zmsg, zgot, a_v, agot, b_v, bgot,
           cmsg, crecv, zrow, xrow, load_sem, small_sem, hs_sem, hr_sem,
           ms_sem, mr_sem, n_sem, cs_sem, cr_sem):
    nx, ny, nz = sizes
    axes = ("gx", "gy", "gz")
    counts = sizes
    me = [lax.axis_index(a) for a in axes]
    SX, SY, SZ = w_v.shape
    PX, PY, PZ = SX // SPF, SY // SPF, SZ // SPF
    KX, KY, KZ = cc_ref.shape[1:]
    EX, QE = PX + 4, 2 * PY
    CR = accc.shape[0]
    CQ, CX = 8, CR // 8
    RZ = tz_v.shape[2]
    KC = SPF * SY
    cells = SX // SPF
    lanes = 3 * SZ

    for c in range(cells):
        part = pl.ds(c * SPF, SPF)
        pltpu.make_async_copy(w_hbm.at[part], w_v.at[part], load_sem.at[c]).start()
        pltpu.make_async_copy(f_hbm.at[part], f_v.at[part], load_sem.at[c]).start()
    small = (pltpu.make_async_copy(fc_hbm, fc_ref, small_sem.at[0]),
             pltpu.make_async_copy(cc_hbm, cc_ref, small_sem.at[1]))
    for copy in small:
        copy.start()

    def load_wait(c):
        both = pl.ds(0, 2 * SPF)
        pltpu.make_async_copy(w_hbm.at[both], w_v.at[both], load_sem.at[c]).wait()

    has = [(me[k] > 0, me[k] < counts[k] - 1) for k in range(3)]
    sides = [(d, e, f) for f in range(3) for d in range(3) for e in range(3)]

    def toward(step):
        return {axes[k]: lax.rem(me[k] + (counts[k] + step[k] - 1), counts[k])
                for k in range(3) if step[k] != 1}

    def inside(step):
        ok = None
        for k in range(3):
            if step[k] != 1:
                here = has[k][0] if step[k] == 0 else has[k][1]
                ok = here if ok is None else ok & here
        return ok

    def far_first(n):
        return sorted(range(1, n), key=lambda d: -min(d, n - d))

    barrier = pltpu.get_barrier_semaphore()
    total = 0
    for k, a in enumerate(axes):
        for d in far_first(counts[k]):
            pl.semaphore_signal(
                barrier, inc=1, device_id={a: lax.rem(me[k] + d, counts[k])}, device_id_type=MESH
            )
            total += 1
    for step in sides:
        if sum(n != 1 for n in step) >= 2:
            pl.semaphore_signal(barrier, inc=1, device_id=toward(step), device_id_type=MESH)
            total += 1

    zero_plane = jnp.zeros((2, SY, SZ), f32)
    s_v[0:2, 8:8 + SY, :] = zero_plane
    s_v[SX + 2:SX + 4, 8:8 + SY, :] = zero_plane
    zero_rows = jnp.zeros((SX, 2, SZ), f32)
    s_v[2:SX + 2, 6:8, :] = zero_rows
    s_v[2:SX + 2, 8 + SY:10 + SY, :] = zero_rows

    def split_store(ref, index, value):
        high = value.astype(bf16)
        ref[index + (0,)] = high
        ref[index + (1,)] = (value - high.astype(f32)).astype(bf16)

    def ext_q(q):
        return jnp.where(q < PY, q, jnp.where(q < PY + 2, q - PY - 2, q - 2))

    def outer(along_x, along_y):
        return jnp.concatenate([along_x[p:p + 1] * along_y for p in range(along_x.shape[0])], axis=0)

    col = iota((8, KC), 1)
    col2 = iota((QE, KC), 1)
    split_store(wf_v, (), outer(weight(col // SY, iota((8, KC), 0) - 2, SPF)[0:5],
                                weight(col2 % SY, ext_q(iota((QE, KC), 0)), SPF)))
    along_y = weight(col % SY, iota((8, KC), 0) - 2, SPC)
    for c in range(cells):
        split_store(wc_v, (c,), outer(
            weight(col // SY + c * SPF, iota((8, KC), 0) - 2, SPC)[0:CX], along_y))
    col, row = iota((QE, 4 * SX), 1), iota((QE, 4 * SX), 0)
    face_x, face_y = (col % (2 * SX)) // 2, col % 2 + (SY - 2) * (col // (2 * SX))
    along_x = weight(face_x, row - 2, SPF)[0:EX]
    along_y = weight(face_y, ext_q(row), SPF)
    split_store(wy_v, (), jnp.concatenate([
        outer(along_x, along_y[0:PY]), outer(along_x, along_y[PY:QE]),
        outer(weight(face_x, row - 2, SPC)[0:CX], weight(face_y, row - 2, SPC)[0:CQ])], axis=0))
    row, col = iota((4 * SX, 128), 0), iota((4 * SX, 128), 1)
    face_x = (row % (2 * SX)) // 2
    place = row % 2 + 2 - 2 * (row // (2 * SX))
    wxe_v[...] = jnp.where(col % 4 == place, jnp.where(
        col < 64, weight(face_x, col // 4 - 2, SPF), weight(face_x, col // 4 - 18, SPC)), 0.0)
    accf[...] = jnp.zeros(accf.shape, f32)
    accc[...] = jnp.zeros(accc.shape, f32)

    lane = iota((SY, SZ), 1)
    packs = [jnp.zeros((SY, SZ), f32) for _ in range(4)]
    for c in range(cells):
        load_wait(c)
        for x in range(c * SPF, (c + 1) * SPF):
            w, f = w_v[x], f_v[x]
            s, d = w + f, w - f
            s_v[x + 2, 8:8 + SY, :] = s
            for side, part in ((0, slice(0, 2)), (1, slice(SY - 2, SY))):
                ysend[side, 2 * x:2 * x + 2, :] = s[part]
                yd[side, 2 * x:2 * x + 2, :] = d[part]
            here = lane // 2 == x
            for n, value in enumerate((s, s, d, d)):
                shift = (2 * x + 2 * (n % 2)) % SZ
                moved = pltpu.roll(value, shift, 1) if shift else value
                packs[n] = jnp.where(here, moved, packs[n])
    for side in range(2):
        zsend[side] = packs[side]
        zd[side] = packs[2 + side]

    pl.semaphore_wait(barrier, total)

    def neighbour_copy(k, side, src, dst, send, recv):
        step = [1, 1, 1]
        step[k] = 2 * side
        return pltpu.make_async_remote_copy(
            src_ref=src, dst_ref=dst, send_sem=send, recv_sem=recv,
            device_id=toward(step), device_id_type=MESH,
        )

    def halo(k, side):
        if k == 0:
            src = s_v.at[pl.ds(2 if side == 0 else SX, 2), pl.ds(8, SY), :]
        else:
            src = (ysend if k == 1 else zsend).at[side]
        return neighbour_copy(k, side, src, (xrecv, yrecv, zrecv)[k].at[1 - side],
                              hs_sem.at[k], hr_sem.at[k])

    def whole(k, ref, send, recv):
        return neighbour_copy(k, 0, ref, ref, send, recv)

    for k in (1, 2, 0):
        for side in range(2):
            halo(k, side).start()

    def forces(i):
        slot = i % 2
        T = 16
        for xx in range(SPF):
            x = i * SPF + xx
            for r in range(0, SY, T):
                at = 8 + r
                d = w_v[x, r:r + T, :] - f_v[x, r:r + T, :]
                s = s_v[x + 2, at:at + T, :]
                gx = (s_v[x, at:at + T, :] - s_v[x + 4, at:at + T, :]
                      + 8.0 * (s_v[x + 3, at:at + T, :] - s_v[x + 1, at:at + T, :]))
                gy = (s_v[x + 2, at - 2:at - 2 + T, :] - s_v[x + 2, at + 2:at + 2 + T, :]
                      + 8.0 * (s_v[x + 2, at + 1:at + 1 + T, :] - s_v[x + 2, at - 1:at - 1 + T, :]))
                gz = (pltpu.roll(s, 2, 1) - pltpu.roll(s, SZ - 2, 1)
                      + 8.0 * (pltpu.roll(s, SZ - 1, 1) - pltpu.roll(s, 1, 1)))
                row = xx * SY + r
                for a, g in enumerate((gx, gy, gz)):
                    force = g * d
                    high = force.astype(bf16)
                    fh_v[slot, row:row + T, a * SZ:(a + 1) * SZ] = high
                    fl_v[slot, row:row + T, a * SZ:(a + 1) * SZ] = (
                        force - high.astype(f32)).astype(bf16)

    def cell_weights(i):
        return jnp.concatenate([wf_v[0], wc_v[i, 0], wf_v[1], wc_v[i, 1]], axis=0)

    def project(weights, high, low):
        many = weights.shape[0] // 2
        both = jnp.dot(weights, high, preferred_element_type=f32)
        return both[:many] + both[many:] + jnp.dot(
            weights[:many], low, preferred_element_type=f32)

    def collect(i, out, part):
        fine = out[:5 * QE].reshape(5, 2, PY, out.shape[1])
        accf[0, i:i + 5, :, part] += fine[:, 0]
        accf[1, i:i + 5, :, part] += fine[:, 1]
        accc[:, part] += out[5 * QE:]

    def gather(i):
        slot = i % 2
        collect(i, project(cell_weights(i), fh_v[slot], fl_v[slot]), slice(0, lanes))

    forces(0)
    for i in range(cells):
        if i + 1 < cells:
            forces(i + 1)
        gather(i)

    for k, got in enumerate((xrecv, yrecv, zrecv)):
        whole(k, got, hs_sem.at[k], hr_sem.at[k]).wait_recv()

    gate = [[jnp.where(h, 1.0, 0.0) for h in pair] for pair in has]

    def split(value):
        high = value.astype(bf16)
        return high, (value - high.astype(f32)).astype(bf16)

    def diff(x):
        return w_v[x] - f_v[x]

    for side, i in ((0, 0), (1, cells - 1)):
        r0, r1 = xrecv[side, 0] * gate[0][side], xrecv[side, 1] * gate[0][side]
        if side == 0:
            face = jnp.concatenate([(r0 - 8.0 * r1) * diff(0), r1 * diff(1)], axis=0)
            part = slice(0, 2 * SY)
        else:
            face = jnp.concatenate([-r0 * diff(SX - 2), (8.0 * r0 - r1) * diff(SX - 1)], axis=0)
            part = slice(KC - 2 * SY, KC)
        collect(i, project(cell_weights(i)[:, part], *split(face)), slice(0, SZ))

    rows = iota((SX // 4, 8, SZ), 1) % 2 == 0
    r = (yrecv[0] * gate[1][0]).reshape(SX // 4, 8, SZ)
    low = jnp.where(rows, r - 8.0 * pltpu.roll(r, 7, 1), r).reshape(2 * SX, SZ) * yd[0]
    r = (yrecv[1] * gate[1][1]).reshape(SX // 4, 8, SZ)
    high = jnp.where(rows, -r, 8.0 * pltpu.roll(r, 1, 1) - r).reshape(2 * SX, SZ) * yd[1]
    out = project(jnp.concatenate([wy_v[0], wy_v[1]], axis=0),
                  *split(jnp.concatenate([low, high], axis=0)))
    for half in range(2):
        accf[half, :, :, SZ:2 * SZ] += out[half * EX * PY:(half + 1) * EX * PY].reshape(EX, PY, SZ)
    accc[:, SZ:2 * SZ] += out[2 * EX * PY:]

    even = lane % 2 == 0
    dl = zrecv[0] * gate[2][0] - zsend[1]
    dh = zrecv[1] * gate[2][1] - zsend[0]
    low = jnp.where(even, dl - 8.0 * pltpu.roll(dl, SZ - 1, 1), dl) * zd[0]
    high = jnp.where(even, -dh, 8.0 * pltpu.roll(dh, 1, 1) - dh) * zd[1]
    row, col = iota((QE + CQ, SY), 0), iota((QE + CQ, SY), 1)
    along_y = jnp.where(row < QE, weight(col, ext_q(row), SPF), weight(col, row - QE - 2, SPC))
    out = nn(nn(along_y, jnp.concatenate([low, high], axis=1)), wxe_v[...])
    at = iota((PY, SZ), 1)
    edge = (at < 2) | (at >= SZ - 2)

    def spread(half, shift):
        return jnp.where(edge, pltpu.roll(out[half * PY:(half + 1) * PY], shift % 128, 1), 0.0)

    for p in range(EX):
        for half in range(2):
            accf[half, p, :, 2 * SZ:3 * SZ] += spread(half, 254 - 4 * p)
    for p in range(CX):
        accc[p * CQ:(p + 1) * CQ, 2 * SZ:3 * SZ] += spread(2, 254 - 64 - 4 * p)

    rows, cols = iota((SZ, 128), 0), iota((SZ, 128), 1)
    bzc = weight(rows, cols % 4 + 4 * (cols // 16 - 1), SPC) * (SPC ** -1.5 / 24.0)
    stack = jnp.concatenate([accc[:, a * SZ:(a + 1) * SZ] for a in range(3)], axis=0)
    shares = nn(stack, bzc)
    rows, cols = iota((CR, 128), 0), iota((CR, 128), 1)
    keep = ((cols // 4) % 4 == 2 * ((rows // CQ) % 2) + rows % 2) & (cols < 48)
    for f in range(3):
        value = shares[0:CR]
        value = value if f == 0 else pltpu.roll(value, 128 - 16 * f, 1)
        for a in (1, 2):
            moved = shares[a * CR:(a + 1) * CR]
            moved = moved if a == f else pltpu.roll(moved, (128 + 16 * (a - f)) % 128, 1)
            value = jnp.where(cols // 16 == a, moved, value)
        value = jnp.where(keep, value, 0.0).reshape(3, 2, CQ, 128)
        value = value[:, 0] + value[:, 1]
        value = value + pltpu.roll(value, 7, 1)
        for d in range(3):
            for e in range(3):
                cmsg[f * 9 + d * 3 + e] = value[d, 2 * e:2 * e + 1, :]

    others = [n for n in range(27) if n != 13]
    for n in sorted(others, key=lambda n: -sum(v != 1 for v in sides[n])):
        pltpu.make_async_remote_copy(
            src_ref=cmsg.at[n], dst_ref=crecv.at[others.index(26 - n)],
            send_sem=n_sem.at[0], recv_sem=n_sem.at[1],
            device_id=toward(sides[n]), device_id_type=MESH,
        ).start()

    rows, cols = iota((RZ, SZ), 0), iota((RZ, SZ), 1)

    def ext_point(row):
        return jnp.where(row < PZ, row, jnp.where(row < PZ + 2, row - PZ - 2, row - 2))

    bz = weight(cols, ext_point(rows), SPF) * (SPF ** -1.5 / 24.0)
    for a in range(3):
        for half in range(2):
            block = accf[half, :, :, a * SZ:(a + 1) * SZ].reshape(EX * PY, SZ)
            tz_v[half, a] = nt(bz, block)

    for copy in small:
        copy.wait()
    shape = (PX * PY, EX * QE)
    rows, cols = iota(shape, 0), iota(shape, 1)
    ox, oy, oz = me[0] * PX, me[1] * PY, me[2] * PZ
    wide, inner = cols // (EX * PY), cols % (EX * PY)
    planes = bend_planes(inner // PY - 2 + ox, ext_q(inner % PY + PY * wide) + oy,
                         rows // PY + ox, rows % PY + oy, PX * nx, PY * ny)
    zr, zc = ext_point(iota((RZ, PZ), 0)) + oz, iota((RZ, PZ), 1) + oz
    along = jnp.concatenate([same(zr, zc), diff1(zr, zc), diff2(zr, zc, PZ * nz)], axis=0)
    turned = nt(along, fc_ref[...].reshape(3 * PX * PY, PZ))
    turned = jnp.concatenate([jnp.concatenate([
        turned[k * RZ:(k + 1) * RZ, a * PX * PY:(a + 1) * PX * PY] for k in range(3)], axis=1)
        for a in range(3)], axis=0)
    bent = nn(turned, jnp.concatenate(planes, axis=0))
    for a in range(3):
        for half in range(2):
            tz_v[half, a] += bent[a * RZ:(a + 1) * RZ, half * EX * PY:(half + 1) * EX * PY]
            for side in range(2):
                zmsg[side, half, 2 * a:2 * a + 2, :] = tz_v[
                    half, a, PZ + 2 * side:PZ + 2 * side + 2, :]

    def fine_start(k):
        for side in range(2):
            source = (b_v, a_v.at[1], zmsg.at[side])[k]
            neighbour_copy(k, side, source, (bgot, agot, zgot)[k].at[1 - side],
                           ms_sem.at[k], mr_sem.at[k]).start()

    def fine_whole(k):
        return whole(k, (bgot, agot, zgot)[k], ms_sem.at[k], mr_sem.at[k])

    def coarse_slot(k, n):
        if k == 0:
            return xrow.at[n]
        if k == 1:
            return xrow.at[me[0], :, pl.ds(n, 1), :]
        return zrow.at[:, pl.ds(n, 1), :]

    def coarse_start(k):
        for d in far_first(counts[k]):
            pltpu.make_async_remote_copy(
                src_ref=coarse_slot(k, me[k]), dst_ref=coarse_slot(k, me[k]),
                send_sem=cs_sem.at[k], recv_sem=cr_sem.at[k],
                device_id={axes[k]: lax.rem(me[k] + d, counts[k])}, device_id_type=MESH,
            ).start()

    def coarse_whole(k):
        part = pl.ds(0, counts[k] - 1)
        ref = (xrow.at[part], xrow.at[me[0], :, part, :], zrow.at[:, part, :])[k]
        return whole(k, ref, cs_sem.at[k], cr_sem.at[k])

    fine_start(2)

    whole(0, crecv, n_sem.at[0], n_sem.at[1]).wait_recv()
    own = cmsg[13]
    for n in others:
        own = own + jnp.where(inside(sides[n]), crecv[others.index(n)], 0.0)
    at = iota((1, 128), 1)
    own = pltpu.roll(own, 4 * me[2], 1)
    for a in range(3):
        value = own if a == 0 else pltpu.roll(own, 128 - 16 * a, 1)
        for g in range(1, 4):
            value = jnp.where(at // 32 == g, pltpu.roll(own, (128 + 28 * g - 16 * a) % 128, 1), value)
        zrow[a, pl.ds(me[2], 1), :] = jnp.where((at % 32) // 4 == me[2], value, 0.0)
    coarse_start(2)

    q_at, r_at = iota((KX, KY, 128), 1), iota((KX, KY, 128), 2)

    def laplace(c):
        zero = jnp.zeros((1, KY, 128), f32)
        total = (jnp.concatenate([c[1:], zero], axis=0) + jnp.concatenate([zero, c[:-1]], axis=0)
                 + jnp.where(q_at < KY - 1, pltpu.roll(c, KY - 1, 1), 0.0)
                 + jnp.where(q_at > 0, pltpu.roll(c, 1, 1), 0.0)
                 + pltpu.roll(c, 127, 2) + pltpu.roll(c, 1, 2))
        return jnp.where(r_at < KZ, total - 6.0 * c, 0.0)

    clane[...] = jnp.zeros(clane.shape, f32)
    for a in range(3):
        clane[:, :, 0:KZ] = cc_ref[a]
        cbend[a] = BEND * laplace(laplace(clane[...]))

    coarse_whole(2).wait_recv()
    for a in range(3):
        xrow[me[0], a, pl.ds(me[1], 1), :] = jnp.sum(zrow[a], axis=0, keepdims=True)
    coarse_start(1)

    fine_whole(2).wait_recv()
    for half in range(2):
        for a in range(3):
            part = slice(2 * a, 2 * a + 2)
            tz_v[half, a, 0:2, :] = tz_v[half, a, 0:2, :] + zgot[0, half, part, :] * gate[2][0]
            tz_v[half, a, PZ - 2:PZ, :] = (
                tz_v[half, a, PZ - 2:PZ, :] + zgot[1, half, part, :] * gate[2][1])
            a_v[half, a * PZ:(a + 1) * PZ, :] = tz_v[half, a, 0:PZ, :]
    fine_start(1)

    coarse_whole(1).wait_recv()
    coarse_start(0)

    fine_whole(1).wait_recv()
    shape = (EX * PY, EX * PY)
    rows, cols = iota(shape, 0), iota(shape, 1)
    p_same = rows // PY == cols // PY
    q, r = rows % PY, cols % PY
    low = jnp.where(p_same & (q == r + 2) & (r < 2), 1.0, 0.0)
    high = jnp.where(p_same & (q == r - (PY - 2)) & (r >= PY - 2), 1.0, 0.0)
    b_v[...] = (a_v[0] + nn(agot[0] * gate[1][0], low) + nn(agot[1] * gate[1][1], high))
    fine_start(0)

    fine_whole(0).wait_recv()
    shape = (PX * PY, EX * PY)
    rows, cols = iota(shape, 0), iota(shape, 1)
    own = jnp.where(cols == rows + 2 * PY, 1.0, 0.0)
    low = jnp.where((cols == rows + (PX + 2) * PY) & (rows < 2 * PY), gate[0][0], 0.0)
    high = jnp.where((cols == rows - (PX - 2) * PY) & (rows >= (PX - 2) * PY), gate[0][1], 0.0)
    for a in range(3):
        part = slice(a * PZ, (a + 1) * PZ)
        out = nt(own, b_v[part]) + nt(low, bgot[0, part]) + nt(high, bgot[1, part])
        fo_ref[a] = out.reshape(PX, PY, PZ)

    for k, got in enumerate((xrecv, yrecv, zrecv)):
        whole(k, got, hs_sem.at[k], hr_sem.at[k]).wait_send()
        fine_whole(k).wait_send()
        coarse_whole(k).wait_send()
    whole(0, crecv, n_sem.at[0], n_sem.at[1]).wait_send()

    coarse_whole(0).wait_recv()
    for i in range(nx):
        for a in range(3):
            block = xrow[i, a]
            for g in range(4):
                value = block if g == 0 else pltpu.roll(block, 128 - 32 * g, 1)
                p = 2 * i + g // 2
                part = pl.ds(g % 2, ny, stride=2)
                co_ref[a, p, part, :] = (value + cbend[a, p, part, :])[:, 0:KZ]


def solution(mesh):
    sizes = tuple(mesh.shape[a] for a in ("gx", "gy", "gz"))

    def step(warped, fixed, fine, coarse):
        SX, SY, SZ = warped.shape
        PX, PY, PZ = SX // SPF, SY // SPF, SZ // SPF
        KX, KY, KZ = coarse.shape[1:]
        EX, QE, RZ = PX + 4, 2 * PY, PZ + 8
        CR = 48
        KC = SPF * SY
        vmem = pl.BlockSpec(memory_space=pltpu.VMEM)
        hbm = pl.BlockSpec(memory_space=pltpu.HBM)
        V = pltpu.VMEM
        D = pltpu.SemaphoreType.DMA
        return pl.pallas_call(
            functools.partial(kernel, sizes),
            out_shape=(V(fine.shape, f32), V(coarse.shape, f32)),
            in_specs=[hbm] * 4,
            out_specs=(vmem, vmem),
            scratch_shapes=[
                V((SX, SY, SZ), f32), V((SX, SY, SZ), f32),
                V((3, PX, PY, PZ), f32), V(coarse.shape, f32),
                V((SX + 4, SY + 16, SZ), f32), V((2, 2, SY, SZ), f32),
                V((2, 2 * SX, SZ), f32), V((2, 2 * SX, SZ), f32), V((2, 2 * SX, SZ), f32),
                V((2, SY, SZ), f32), V((2, SY, SZ), f32), V((2, SY, SZ), f32),
                V((2, 5 * QE, KC), bf16), V((SX // SPF, 2, CR, KC), bf16),
                V((2, EX * QE + CR, 4 * SX), bf16), V((4 * SX, 128), f32),
                V((2, KC, 3 * SZ), bf16), V((2, KC, 3 * SZ), bf16),
                V((2, EX, PY, 3 * SZ), f32), V((CR, 3 * SZ), f32),
                V((2, 3, RZ, EX * PY), f32),
                V((KX, KY, 128), f32), V((3, KX, KY, 128), f32),
                V((2, 2, 8, EX * PY), f32), V((2, 2, 8, EX * PY), f32),
                V((2, 3 * PZ, EX * PY), f32), V((2, 3 * PZ, EX * PY), f32),
                V((3 * PZ, EX * PY), f32), V((2, 3 * PZ, EX * PY), f32),
                V((27, 1, 128), f32), V((26, 1, 128), f32),
                V((3, sizes[2], 128), f32), V((sizes[0], 3, sizes[1], 128), f32),
                D((SX // SPF,)), D((2,)), D((3,)), D((3,)),
                D((3,)), D((3,)), D((2,)), D((3,)), D((3,)),
            ],
            compiler_params=pltpu.CompilerParams(
                collective_id=0, has_side_effects=True, vmem_limit_bytes=66000000
            ),
        )(warped, fixed, fine, coarse)

    in_specs = (P("gx", "gy", "gz"), P("gx", "gy", "gz"), P(None, "gx", "gy", "gz"), P())
    out_specs = (P(None, "gx", "gy", "gz"), P())
    return jax.shard_map(
        step, mesh=mesh, in_specs=in_specs, out_specs=out_specs, check_vma=False
    )
```

```python
import functools

import jax
import jax.numpy as jnp
from jax import lax
from jax.experimental import pallas as pl
from jax.experimental.pallas import tpu as pltpu
from jax.sharding import PartitionSpec as P

SPF = 8
SPC = 32
BEND = 0.01
HI = lax.Precision.HIGHEST
MESH = pl.DeviceIdType.MESH
f32 = jnp.float32
bf16 = jnp.bfloat16


def nn(a, b):
    return lax.dot_general(
        a, b, (((1,), (0,)), ((), ())), precision=HI, preferred_element_type=f32
    )


def nt(a, b):
    return lax.dot_general(
        a, b, (((1,), (1,)), ((), ())), precision=HI, preferred_element_type=f32
    )


def spline(t):
    m = jnp.abs(t)
    inner = 2.0 / 3.0 - m * m + 0.5 * m * m * m
    r = 2.0 - m
    outer = r * r * r * (1.0 / 6.0)
    return jnp.where(m < 1.0, inner, jnp.where(m < 2.0, outer, 0.0))


def weight(voxel, point, spacing):
    scaled = (2 * voxel + 1 - spacing * (2 * point + 1)).astype(f32)
    return spline(scaled * (0.5 / spacing))


def iota(shape, axis):
    return lax.broadcasted_iota(jnp.int32, shape, axis)


def diff1(out, inp):
    d = jnp.abs(out - inp)
    return jnp.where(d == 0, -2.0, jnp.where(d == 1, 1.0, 0.0)).astype(f32)


def diff2(out, inp, count):
    d = jnp.abs(out - inp)
    edge = (inp == 0) | (inp == count - 1)
    centre = jnp.where(edge, 5.0, 6.0)
    return jnp.where(
        d == 0, centre, jnp.where(d == 1, -4.0, jnp.where(d == 2, 1.0, 0.0))
    ).astype(f32)


def same(out, inp):
    return jnp.where(out == inp, 1.0, 0.0).astype(f32)


def bend_planes(px, py, qx, qy, cx, cy):
    jx, jy = same(px, qx), same(py, qy)
    tx, ty = diff1(px, qx), diff1(py, qy)
    m0 = diff2(px, qx, cx) * jy + jx * diff2(py, qy, cy) + 2.0 * tx * ty
    m1 = 2.0 * (tx * jy + jx * ty)
    return m0 * BEND, m1 * BEND, jx * jy * BEND


def kernel(sizes, w_hbm, f_hbm, fc_hbm, cc_hbm, fo_ref, co_ref,
           w_v, f_v, fc_ref, cc_ref, s_v, xrecv, ysend, yrecv, yd, zsend, zrecv, zd,
           wf_v, wc_v, wy_v, wxe_v, bzc_v, pz_v, gz_v, zp_v,
           accf, accc, tz_v, clane, cbend, zmsg, zgot, a_v, agot, b_v, bgot,
           cmsg, crecv, zrow, xrow, load_sem, small_sem, hs_sem, hr_sem,
           ms_sem, mr_sem, n_sem, cs_sem, cr_sem):
    nx, ny, nz = sizes
    axes = ("gx", "gy", "gz")
    counts = sizes
    me = [lax.axis_index(a) for a in axes]
    SX, SY, SZ = w_v.shape
    PX, PY, PZ = SX // SPF, SY // SPF, SZ // SPF
    KX, KY, KZ = cc_ref.shape[1:]
    EX, QE = PX + 4, 2 * PY
    CR = accc.shape[0]
    CQ, CX = 8, CR // 8
    RZ = tz_v.shape[2]
    KC = SPF * SY
    cells = SX // SPF
    lanes = 3 * SZ

    for c in range(cells):
        part = pl.ds(c * SPF, SPF)
        pltpu.make_async_copy(w_hbm.at[part], w_v.at[part], load_sem.at[c]).start()
        pltpu.make_async_copy(f_hbm.at[part], f_v.at[part], load_sem.at[c]).start()
    small = (pltpu.make_async_copy(fc_hbm, fc_ref, small_sem.at[0]),
             pltpu.make_async_copy(cc_hbm, cc_ref, small_sem.at[1]))
    for copy in small:
        copy.start()

    def load_wait(c):
        both = pl.ds(0, 2 * SPF)
        pltpu.make_async_copy(w_hbm.at[both], w_v.at[both], load_sem.at[c]).wait()

    has = [(me[k] > 0, me[k] < counts[k] - 1) for k in range(3)]
    sides = [(d, e, f) for f in range(3) for d in range(3) for e in range(3)]

    def toward(step):
        return {axes[k]: lax.rem(me[k] + (counts[k] + step[k] - 1), counts[k])
                for k in range(3) if step[k] != 1}

    def inside(step):
        ok = None
        for k in range(3):
            if step[k] != 1:
                here = has[k][0] if step[k] == 0 else has[k][1]
                ok = here if ok is None else ok & here
        return ok

    def far_first(n):
        return sorted(range(1, n), key=lambda d: -min(d, n - d))

    barrier = pltpu.get_barrier_semaphore()
    total = 0
    for k, a in enumerate(axes):
        for d in far_first(counts[k]):
            pl.semaphore_signal(
                barrier, inc=1, device_id={a: lax.rem(me[k] + d, counts[k])}, device_id_type=MESH
            )
            total += 1
    for step in sides:
        if sum(n != 1 for n in step) >= 2:
            pl.semaphore_signal(barrier, inc=1, device_id=toward(step), device_id_type=MESH)
            total += 1

    zero_plane = jnp.zeros((2, SY, SZ), f32)
    s_v[0:2, 8:8 + SY, :] = zero_plane
    s_v[SX + 2:SX + 4, 8:8 + SY, :] = zero_plane
    zero_rows = jnp.zeros((SX, 2, SZ), f32)
    s_v[2:SX + 2, 6:8, :] = zero_rows
    s_v[2:SX + 2, 8 + SY:10 + SY, :] = zero_rows

    def split_store(ref, index, value):
        high = value.astype(bf16)
        ref[index + (0,)] = high
        ref[index + (1,)] = (value - high.astype(f32)).astype(bf16)

    def ext_q(q):
        return jnp.where(q < PY, q, jnp.where(q < PY + 2, q - PY - 2, q - 2))

    def outer(along_x, along_y):
        return jnp.concatenate([along_x[p:p + 1] * along_y for p in range(along_x.shape[0])], axis=0)

    col = iota((8, KC), 1)
    col2 = iota((QE, KC), 1)
    split_store(wf_v, (), outer(weight(col // SY, iota((8, KC), 0) - 2, SPF)[0:5],
                                weight(col2 % SY, ext_q(iota((QE, KC), 0)), SPF)))
    along_y = weight(col % SY, iota((8, KC), 0) - 2, SPC)
    for c in range(cells):
        split_store(wc_v, (c,), outer(
            weight(col // SY + c * SPF, iota((8, KC), 0) - 2, SPC)[0:CX], along_y))
    col, row = iota((QE, 4 * SX), 1), iota((QE, 4 * SX), 0)
    face_x, face_y = (col % (2 * SX)) // 2, col % 2 + (SY - 2) * (col // (2 * SX))
    along_x = weight(face_x, row - 2, SPF)[0:EX]
    along_y = weight(face_y, ext_q(row), SPF)
    split_store(wy_v, (), jnp.concatenate([
        outer(along_x, along_y[0:PY]), outer(along_x, along_y[PY:QE]),
        outer(weight(face_x, row - 2, SPC)[0:CX], weight(face_y, row - 2, SPC)[0:CQ])], axis=0))
    row, col = iota((4 * SX, 128), 0), iota((4 * SX, 128), 1)
    face_x = (row % (2 * SX)) // 4 + jnp.where(row % 4 < 2, SX // 2, 0)
    place = row % 2 + 2 - 2 * (row // (2 * SX))
    wxe_v[...] = jnp.where(col % 4 == place, jnp.where(
        col < 64, weight(face_x, col // 4 - 2, SPF), weight(face_x, col // 4 - 18, SPC)), 0.0)
    row, col = iota((2 * SZ, 2 * SZ), 0) % SZ, iota((2 * SZ, 2 * SZ), 1)
    away = row - col
    slope = jnp.where(away == 1, 8.0, jnp.where(away == -1, -8.0, jnp.where(
        away == -2, 1.0, jnp.where(away == 2, -1.0, 0.0))))
    pick = jnp.where(row == (col % 4 + SZ - 2) % SZ, 1.0, 0.0)
    pz_v[...] = jnp.where(col < SZ, slope, pick).astype(bf16)
    rows, cols = iota((SZ, 128), 0), iota((SZ, 128), 1)
    bzc_v[...] = weight(rows, cols % 4 + 4 * (cols // 16 - 1), SPC) * (SPC ** -1.5 / 24.0)
    accf[...] = jnp.zeros(accf.shape, f32)
    accc[...] = jnp.zeros(accc.shape, f32)

    lane = iota((SY, SZ), 1)
    half_x = SX // 2

    def split(value):
        high = value.astype(bf16)
        return high, (value - high.astype(f32)).astype(bf16)

    for c in range(cells):
        load_wait(c)
        wide = ([], [])
        for x in range(c * SPF, (c + 1) * SPF):
            w, f = w_v[x], f_v[x]
            s, d = w + f, w - f
            s_v[x + 2, 8:8 + SY, :] = s
            w_v[x] = d
            for side, part in ((0, slice(0, 2)), (1, slice(SY - 2, SY))):
                ysend[side, 2 * x:2 * x + 2, :] = s[part]
                yd[side, 2 * x:2 * x + 2, :] = d[part]
            for n, value in enumerate((s, d)):
                wide[n].append(jnp.concatenate(split(value), axis=1))
        out = jnp.dot(jnp.concatenate(wide[0], axis=0), pz_v[...], preferred_element_type=f32)
        gz_v[c] = out[:, 0:SZ]
        picked = (out[:, SZ:2 * SZ],
                  jnp.dot(jnp.concatenate(wide[1], axis=0), pz_v[:, SZ:2 * SZ], preferred_element_type=f32))
        tile = c * SPF // half_x
        for n in range(2):
            pack = None if c * SPF % half_x == 0 else zp_v[n, tile]
            for xx in range(SPF):
                value = picked[n][xx * SY:(xx + 1) * SY]
                here = lane // 4 == (c * SPF + xx) % half_x
                pack = value if pack is None else jnp.where(here, value, pack)
            zp_v[n, tile] = pack
    upper = lane % 4 >= 2
    for n, ref in enumerate((zsend, zd)):
        ref[0] = jnp.where(upper, zp_v[n, 0], pltpu.roll(zp_v[n, 1], SZ - 2, 1))
        ref[1] = jnp.where(upper, pltpu.roll(zp_v[n, 0], 2, 1), zp_v[n, 1])

    pl.semaphore_wait(barrier, total)

    def neighbour_copy(k, side, src, dst, send, recv):
        step = [1, 1, 1]
        step[k] = 2 * side
        return pltpu.make_async_remote_copy(
            src_ref=src, dst_ref=dst, send_sem=send, recv_sem=recv,
            device_id=toward(step), device_id_type=MESH,
        )

    def halo(k, side):
        if k == 0:
            src = s_v.at[pl.ds(2 if side == 0 else SX, 2), pl.ds(8, SY), :]
        else:
            src = (ysend if k == 1 else zsend).at[side]
        return neighbour_copy(k, side, src, (xrecv, yrecv, zrecv)[k].at[1 - side],
                              hs_sem.at[k], hr_sem.at[k])

    def whole(k, ref, send, recv):
        return neighbour_copy(k, 0, ref, ref, send, recv)

    for k in (1, 2, 0):
        for side in range(2):
            halo(k, side).start()

    def forces(i):
        T = 16
        tiles = {}
        for r in range(0, SY, T):
            at = 8 + r
            near = [s_v[i * SPF + n, at:at + T, :] for n in range(4)]
            for xx in range(SPF):
                x = i * SPF + xx
                near.append(s_v[x + 4, at:at + T, :])
                d = w_v[x, r:r + T, :]
                gx = near[0] - near[4] + 8.0 * (near[3] - near[1])
                near.pop(0)
                gy = (s_v[x + 2, at - 2:at - 2 + T, :] - s_v[x + 2, at + 2:at + 2 + T, :]
                      + 8.0 * (s_v[x + 2, at + 1:at + 1 + T, :] - s_v[x + 2, at - 1:at - 1 + T, :]))
                row = xx * SY + r
                gz = gz_v[i, row:row + T, :]
                tiles[row] = [split(g * d) for g in (gx, gy, gz)]
        return [jnp.concatenate([
            jnp.concatenate([tiles[row][a][n] for row in sorted(tiles)], axis=0)
            for a in range(3)], axis=1) for n in range(2)]

    def cell_weights(i):
        return jnp.concatenate([wf_v[0], wc_v[i, 0], wf_v[1], wc_v[i, 1]], axis=0)

    def project(weights, high, low):
        many = weights.shape[0] // 2
        both = jnp.dot(weights, high, preferred_element_type=f32)
        return both[:many] + both[many:] + jnp.dot(
            weights[:many], low, preferred_element_type=f32)

    def collect(i, out, part):
        fine = out[:5 * QE].reshape(5, 2, PY, out.shape[1])
        accf[0, i:i + 5, :, part] += fine[:, 0]
        accf[1, i:i + 5, :, part] += fine[:, 1]
        accc[:, part] += out[5 * QE:]

    for i in range(cells):
        collect(i, project(cell_weights(i), *forces(i)), slice(0, lanes))

    for k, got in enumerate((xrecv, yrecv, zrecv)):
        whole(k, got, hs_sem.at[k], hr_sem.at[k]).wait_recv()

    gate = [[jnp.where(h, 1.0, 0.0) for h in pair] for pair in has]

    def diff(x):
        return w_v[x]

    for side, i in ((0, 0), (1, cells - 1)):
        r0, r1 = xrecv[side, 0] * gate[0][side], xrecv[side, 1] * gate[0][side]
        if side == 0:
            face = jnp.concatenate([(r0 - 8.0 * r1) * diff(0), r1 * diff(1)], axis=0)
            part = slice(0, 2 * SY)
        else:
            face = jnp.concatenate([-r0 * diff(SX - 2), (8.0 * r0 - r1) * diff(SX - 1)], axis=0)
            part = slice(KC - 2 * SY, KC)
        collect(i, project(cell_weights(i)[:, part], *split(face)), slice(0, SZ))

    rows = iota((SX // 4, 8, SZ), 1) % 2 == 0
    r = (yrecv[0] * gate[1][0]).reshape(SX // 4, 8, SZ)
    low = jnp.where(rows, r - 8.0 * pltpu.roll(r, 7, 1), r).reshape(2 * SX, SZ) * yd[0]
    r = (yrecv[1] * gate[1][1]).reshape(SX // 4, 8, SZ)
    high = jnp.where(rows, -r, 8.0 * pltpu.roll(r, 1, 1) - r).reshape(2 * SX, SZ) * yd[1]
    out = project(jnp.concatenate([wy_v[0], wy_v[1]], axis=0),
                  *split(jnp.concatenate([low, high], axis=0)))
    for half in range(2):
        accf[half, :, :, SZ:2 * SZ] += out[half * EX * PY:(half + 1) * EX * PY].reshape(EX, PY, SZ)
    accc[:, SZ:2 * SZ] += out[2 * EX * PY:]

    even = lane % 2 == 0
    dl = zrecv[0] * gate[2][0]
    dh = zrecv[1] * gate[2][1]
    low = jnp.where(even, dl - 8.0 * pltpu.roll(dl, SZ - 1, 1), dl) * zd[0]
    high = jnp.where(even, -dh, 8.0 * pltpu.roll(dh, 1, 1) - dh) * zd[1]
    row, col = iota((QE + CQ, SY), 0), iota((QE + CQ, SY), 1)
    along_y = jnp.where(row < QE, weight(col, ext_q(row), SPF), weight(col, row - QE - 2, SPC))
    out = nn(nn(along_y, jnp.concatenate([low, high], axis=1)), wxe_v[...])
    at = iota((PY, SZ), 1)
    edge = (at < 2) | (at >= SZ - 2)

    def spread(half, shift):
        return jnp.where(edge, pltpu.roll(out[half * PY:(half + 1) * PY], shift % 128, 1), 0.0)

    for p in range(EX):
        for half in range(2):
            accf[half, p, :, 2 * SZ:3 * SZ] += spread(half, 254 - 4 * p)
    for p in range(CX):
        accc[p * CQ:(p + 1) * CQ, 2 * SZ:3 * SZ] += spread(2, 254 - 64 - 4 * p)

    stack = jnp.concatenate([accc[:, a * SZ:(a + 1) * SZ] for a in range(3)], axis=0)
    shares = nn(stack, bzc_v[...])
    rows, cols = iota((CR, 128), 0), iota((CR, 128), 1)
    keep = ((cols // 4) % 4 == 2 * ((rows // CQ) % 2) + rows % 2) & (cols < 48)
    for f in range(3):
        value = shares[0:CR]
        value = value if f == 0 else pltpu.roll(value, 128 - 16 * f, 1)
        for a in (1, 2):
            moved = shares[a * CR:(a + 1) * CR]
            moved = moved if a == f else pltpu.roll(moved, (128 + 16 * (a - f)) % 128, 1)
            value = jnp.where(cols // 16 == a, moved, value)
        value = jnp.where(keep, value, 0.0).reshape(3, 2, CQ, 128)
        value = value[:, 0] + value[:, 1]
        value = value + pltpu.roll(value, 7, 1)
        for d in range(3):
            for e in range(3):
                cmsg[f * 9 + d * 3 + e] = value[d, 2 * e:2 * e + 1, :]

    others = [n for n in range(27) if n != 13]
    for n in sorted(others, key=lambda n: -sum(v != 1 for v in sides[n])):
        pltpu.make_async_remote_copy(
            src_ref=cmsg.at[n], dst_ref=crecv.at[others.index(26 - n)],
            send_sem=n_sem.at[0], recv_sem=n_sem.at[1],
            device_id=toward(sides[n]), device_id_type=MESH,
        ).start()

    rows, cols = iota((RZ, SZ), 0), iota((RZ, SZ), 1)

    def ext_point(row):
        return jnp.where(row < PZ, row, jnp.where(row < PZ + 2, row - PZ - 2, row - 2))

    bz = weight(cols, ext_point(rows), SPF) * (SPF ** -1.5 / 24.0)
    for a in range(3):
        for half in range(2):
            block = accf[half, :, :, a * SZ:(a + 1) * SZ].reshape(EX * PY, SZ)
            tz_v[half, a] = nt(bz, block)

    for copy in small:
        copy.wait()
    shape = (PX * PY, EX * QE)
    rows, cols = iota(shape, 0), iota(shape, 1)
    ox, oy, oz = me[0] * PX, me[1] * PY, me[2] * PZ
    wide, inner = cols // (EX * PY), cols % (EX * PY)
    planes = bend_planes(inner // PY - 2 + ox, ext_q(inner % PY + PY * wide) + oy,
                         rows // PY + ox, rows % PY + oy, PX * nx, PY * ny)
    zr, zc = ext_point(iota((RZ, PZ), 0)) + oz, iota((RZ, PZ), 1) + oz
    along = jnp.concatenate([same(zr, zc), diff1(zr, zc), diff2(zr, zc, PZ * nz)], axis=0)
    turned = nt(along, fc_ref[...].reshape(3 * PX * PY, PZ))
    turned = jnp.concatenate([jnp.concatenate([
        turned[k * RZ:(k + 1) * RZ, a * PX * PY:(a + 1) * PX * PY] for k in range(3)], axis=1)
        for a in range(3)], axis=0)
    bent = nn(turned, jnp.concatenate(planes, axis=0))
    for a in range(3):
        for half in range(2):
            tz_v[half, a] += bent[a * RZ:(a + 1) * RZ, half * EX * PY:(half + 1) * EX * PY]
            for side in range(2):
                zmsg[side, half, 2 * a:2 * a + 2, :] = tz_v[
                    half, a, PZ + 2 * side:PZ + 2 * side + 2, :]

    def fine_start(k):
        for side in range(2):
            source = (b_v, a_v.at[1], zmsg.at[side])[k]
            neighbour_copy(k, side, source, (bgot, agot, zgot)[k].at[1 - side],
                           ms_sem.at[k], mr_sem.at[k]).start()

    def fine_whole(k):
        return whole(k, (bgot, agot, zgot)[k], ms_sem.at[k], mr_sem.at[k])

    def coarse_slot(k, n):
        if k == 0:
            return xrow.at[n]
        if k == 1:
            return xrow.at[me[0], :, pl.ds(n, 1), :]
        return zrow.at[:, pl.ds(n, 1), :]

    def coarse_start(k):
        for d in far_first(counts[k]):
            pltpu.make_async_remote_copy(
                src_ref=coarse_slot(k, me[k]), dst_ref=coarse_slot(k, me[k]),
                send_sem=cs_sem.at[k], recv_sem=cr_sem.at[k],
                device_id={axes[k]: lax.rem(me[k] + d, counts[k])}, device_id_type=MESH,
            ).start()

    def coarse_whole(k):
        part = pl.ds(0, counts[k] - 1)
        ref = (xrow.at[part], xrow.at[me[0], :, part, :], zrow.at[:, part, :])[k]
        return whole(k, ref, cs_sem.at[k], cr_sem.at[k])

    fine_start(2)

    whole(0, crecv, n_sem.at[0], n_sem.at[1]).wait_recv()
    own = cmsg[13]
    for n in others:
        own = own + jnp.where(inside(sides[n]), crecv[others.index(n)], 0.0)
    at = iota((1, 128), 1)
    own = pltpu.roll(own, 4 * me[2], 1)
    for a in range(3):
        value = own if a == 0 else pltpu.roll(own, 128 - 16 * a, 1)
        for g in range(1, 4):
            value = jnp.where(at // 32 == g, pltpu.roll(own, (128 + 28 * g - 16 * a) % 128, 1), value)
        zrow[a, pl.ds(me[2], 1), :] = jnp.where((at % 32) // 4 == me[2], value, 0.0)
    coarse_start(2)

    q_at, r_at = iota((KX, KY, 128), 1), iota((KX, KY, 128), 2)

    def laplace(c):
        zero = jnp.zeros((1, KY, 128), f32)
        total = (jnp.concatenate([c[1:], zero], axis=0) + jnp.concatenate([zero, c[:-1]], axis=0)
                 + jnp.where(q_at < KY - 1, pltpu.roll(c, KY - 1, 1), 0.0)
                 + jnp.where(q_at > 0, pltpu.roll(c, 1, 1), 0.0)
                 + pltpu.roll(c, 127, 2) + pltpu.roll(c, 1, 2))
        return jnp.where(r_at < KZ, total - 6.0 * c, 0.0)

    clane[...] = jnp.zeros(clane.shape, f32)
    for a in range(3):
        clane[:, :, 0:KZ] = cc_ref[a]
        cbend[a] = BEND * laplace(laplace(clane[...]))

    coarse_whole(2).wait_recv()
    for a in range(3):
        xrow[me[0], a, pl.ds(me[1], 1), :] = jnp.sum(zrow[a], axis=0, keepdims=True)
    coarse_start(1)

    fine_whole(2).wait_recv()
    for half in range(2):
        for a in range(3):
            part = slice(2 * a, 2 * a + 2)
            tz_v[half, a, 0:2, :] = tz_v[half, a, 0:2, :] + zgot[0, half, part, :] * gate[2][0]
            tz_v[half, a, PZ - 2:PZ, :] = (
                tz_v[half, a, PZ - 2:PZ, :] + zgot[1, half, part, :] * gate[2][1])
            a_v[half, a * PZ:(a + 1) * PZ, :] = tz_v[half, a, 0:PZ, :]
    fine_start(1)

    coarse_whole(1).wait_recv()
    coarse_start(0)

    fine_whole(1).wait_recv()
    shape = (EX * PY, EX * PY)
    rows, cols = iota(shape, 0), iota(shape, 1)
    p_same = rows // PY == cols // PY
    q, r = rows % PY, cols % PY
    low = jnp.where(p_same & (q == r + 2) & (r < 2), 1.0, 0.0)
    high = jnp.where(p_same & (q == r - (PY - 2)) & (r >= PY - 2), 1.0, 0.0)
    b_v[...] = (a_v[0] + nn(agot[0] * gate[1][0], low) + nn(agot[1] * gate[1][1], high))
    fine_start(0)

    fine_whole(0).wait_recv()
    shape = (PX * PY, EX * PY)
    rows, cols = iota(shape, 0), iota(shape, 1)
    own = jnp.where(cols == rows + 2 * PY, 1.0, 0.0)
    low = jnp.where((cols == rows + (PX + 2) * PY) & (rows < 2 * PY), gate[0][0], 0.0)
    high = jnp.where((cols == rows - (PX - 2) * PY) & (rows >= (PX - 2) * PY), gate[0][1], 0.0)
    for a in range(3):
        part = slice(a * PZ, (a + 1) * PZ)
        out = nt(own, b_v[part]) + nt(low, bgot[0, part]) + nt(high, bgot[1, part])
        fo_ref[a] = out.reshape(PX, PY, PZ)

    for k, got in enumerate((xrecv, yrecv, zrecv)):
        whole(k, got, hs_sem.at[k], hr_sem.at[k]).wait_send()
        fine_whole(k).wait_send()
        coarse_whole(k).wait_send()
    whole(0, crecv, n_sem.at[0], n_sem.at[1]).wait_send()

    coarse_whole(0).wait_recv()
    for i in range(nx):
        for a in range(3):
            block = xrow[i, a]
            for g in range(4):
                value = block if g == 0 else pltpu.roll(block, 128 - 32 * g, 1)
                p = 2 * i + g // 2
                part = pl.ds(g % 2, ny, stride=2)
                co_ref[a, p, part, :] = (value + cbend[a, p, part, :])[:, 0:KZ]


def solution(mesh):
    sizes = tuple(mesh.shape[a] for a in ("gx", "gy", "gz"))

    def step(warped, fixed, fine, coarse):
        SX, SY, SZ = warped.shape
        PX, PY, PZ = SX // SPF, SY // SPF, SZ // SPF
        KX, KY, KZ = coarse.shape[1:]
        EX, QE, RZ = PX + 4, 2 * PY, PZ + 8
        CR = 48
        KC = SPF * SY
        vmem = pl.BlockSpec(memory_space=pltpu.VMEM)
        hbm = pl.BlockSpec(memory_space=pltpu.HBM)
        V = pltpu.VMEM
        D = pltpu.SemaphoreType.DMA
        return pl.pallas_call(
            functools.partial(kernel, sizes),
            out_shape=(V(fine.shape, f32), V(coarse.shape, f32)),
            in_specs=[hbm] * 4,
            out_specs=(vmem, vmem),
            scratch_shapes=[
                V((SX, SY, SZ), f32), V((SX, SY, SZ), f32),
                V((3, PX, PY, PZ), f32), V(coarse.shape, f32),
                V((SX + 4, SY + 16, SZ), f32), V((2, 2, SY, SZ), f32),
                V((2, 2 * SX, SZ), f32), V((2, 2 * SX, SZ), f32), V((2, 2 * SX, SZ), f32),
                V((2, SY, SZ), f32), V((2, SY, SZ), f32), V((2, SY, SZ), f32),
                V((2, 5 * QE, KC), bf16), V((SX // SPF, 2, CR, KC), bf16),
                V((2, EX * QE + CR, 4 * SX), bf16), V((4 * SX, 128), f32), V((SZ, 128), f32),
                V((2 * SZ, 2 * SZ), bf16),
                V((SX // SPF, KC, SZ), f32), V((2, 2, SY, SZ), f32),
                V((2, EX, PY, 3 * SZ), f32), V((CR, 3 * SZ), f32),
                V((2, 3, RZ, EX * PY), f32),
                V((KX, KY, 128), f32), V((3, KX, KY, 128), f32),
                V((2, 2, 8, EX * PY), f32), V((2, 2, 8, EX * PY), f32),
                V((2, 3 * PZ, EX * PY), f32), V((2, 3 * PZ, EX * PY), f32),
                V((3 * PZ, EX * PY), f32), V((2, 3 * PZ, EX * PY), f32),
                V((27, 1, 128), f32), V((26, 1, 128), f32),
                V((3, sizes[2], 128), f32), V((sizes[0], 3, sizes[1], 128), f32),
                D((SX // SPF,)), D((2,)), D((3,)), D((3,)),
                D((3,)), D((3,)), D((2,)), D((3,)), D((3,)),
            ],
            compiler_params=pltpu.CompilerParams(
                collective_id=0, has_side_effects=True, vmem_limit_bytes=66000000
            ),
        )(warped, fixed, fine, coarse)

    in_specs = (P("gx", "gy", "gz"), P("gx", "gy", "gz"), P(None, "gx", "gy", "gz"), P())
    out_specs = (P(None, "gx", "gy", "gz"), P())
    return jax.shard_map(
        step, mesh=mesh, in_specs=in_specs, out_specs=out_specs, check_vma=False
    )
```

```python
import functools

import jax
import jax.numpy as jnp
from jax import lax
from jax.experimental import pallas as pl
from jax.experimental.pallas import tpu as pltpu
from jax.sharding import PartitionSpec as P

SPF = 8
SPC = 32
BEND = 0.01
HI = lax.Precision.HIGHEST
MESH = pl.DeviceIdType.MESH
f32 = jnp.float32
bf16 = jnp.bfloat16


def nn(a, b):
    return lax.dot_general(
        a, b, (((1,), (0,)), ((), ())), precision=HI, preferred_element_type=f32
    )


def nt(a, b):
    return lax.dot_general(
        a, b, (((1,), (1,)), ((), ())), precision=HI, preferred_element_type=f32
    )


def spline(t):
    m = jnp.abs(t)
    inner = 2.0 / 3.0 - m * m + 0.5 * m * m * m
    r = 2.0 - m
    outer = r * r * r * (1.0 / 6.0)
    return jnp.where(m < 1.0, inner, jnp.where(m < 2.0, outer, 0.0))


def weight(voxel, point, spacing):
    scaled = (2 * voxel + 1 - spacing * (2 * point + 1)).astype(f32)
    return spline(scaled * (0.5 / spacing))


def iota(shape, axis):
    return lax.broadcasted_iota(jnp.int32, shape, axis)


def diff1(out, inp):
    d = jnp.abs(out - inp)
    return jnp.where(d == 0, -2.0, jnp.where(d == 1, 1.0, 0.0)).astype(f32)


def diff2(out, inp, count):
    d = jnp.abs(out - inp)
    edge = (inp == 0) | (inp == count - 1)
    centre = jnp.where(edge, 5.0, 6.0)
    return jnp.where(
        d == 0, centre, jnp.where(d == 1, -4.0, jnp.where(d == 2, 1.0, 0.0))
    ).astype(f32)


def same(out, inp):
    return jnp.where(out == inp, 1.0, 0.0).astype(f32)


def bend_planes(px, py, qx, qy, cx, cy):
    jx, jy = same(px, qx), same(py, qy)
    tx, ty = diff1(px, qx), diff1(py, qy)
    m0 = diff2(px, qx, cx) * jy + jx * diff2(py, qy, cy) + 2.0 * tx * ty
    m1 = 2.0 * (tx * jy + jx * ty)
    return m0 * BEND, m1 * BEND, jx * jy * BEND


def kernel(sizes, w_hbm, f_hbm, fc_hbm, cc_hbm, fo_ref, co_ref,
           w_v, f_v, fc_ref, cc_ref, s_v, xrecv, ysend, yrecv, yd, zsend, zrecv, zd,
           wf_v, wc_v, wy_v, wxe_v, bzc_v, pz_v, gz_v, zp_v,
           accf, accc, tz_v, clane, cbend, zmsg, zgot, a_v, agot, b_v, bgot,
           cmsg, crecv, crest, xrow, load_sem, small_sem, hs_sem, hr_sem,
           ms_sem, mr_sem, n_sem, cs_sem, cr_sem):
    nx, ny, nz = sizes
    axes = ("gx", "gy", "gz")
    counts = sizes
    me = [lax.axis_index(a) for a in axes]
    SX, SY, SZ = w_v.shape
    PX, PY, PZ = SX // SPF, SY // SPF, SZ // SPF
    KX, KY, KZ = cc_ref.shape[1:]
    EX, QE = PX + 4, 2 * PY
    CR = accc.shape[0]
    CQ, CX = 8, CR // 8
    RZ = tz_v.shape[2]
    KC = SPF * SY
    cells = SX // SPF
    lanes = 3 * SZ

    for c in range(cells):
        part = pl.ds(c * SPF, SPF)
        pltpu.make_async_copy(w_hbm.at[part], w_v.at[part], load_sem.at[c]).start()
        pltpu.make_async_copy(f_hbm.at[part], f_v.at[part], load_sem.at[c]).start()
    small = (pltpu.make_async_copy(fc_hbm, fc_ref, small_sem.at[0]),
             pltpu.make_async_copy(cc_hbm, cc_ref, small_sem.at[1]))
    for copy in small:
        copy.start()

    def load_wait(c):
        both = pl.ds(0, 2 * SPF)
        pltpu.make_async_copy(w_hbm.at[both], w_v.at[both], load_sem.at[c]).wait()

    has = [(me[k] > 0, me[k] < counts[k] - 1) for k in range(3)]

    def toward(step):
        return {axes[k]: lax.rem(me[k] + (counts[k] + step[k] - 1), counts[k])
                for k in range(3) if step[k] != 1}

    def inside(step):
        ok = None
        for k in range(3):
            if step[k] != 1:
                here = has[k][0] if step[k] == 0 else has[k][1]
                ok = here if ok is None else ok & here
        return ok

    def far_first(n):
        return sorted(range(1, n), key=lambda d: -min(d, n - d))

    columns = [(d, e) for d in range(3) for e in range(3)]
    reach = [(n, dz) for dz in far_first(nz) + [0] for n in range(9) if (n, dz) != (4, 0)]

    def column(n, dz):
        there = toward(columns[n] + (1,))
        if dz:
            there[axes[2]] = lax.rem(me[2] + dz, nz)
        return there

    barrier = pltpu.get_barrier_semaphore()
    for n, dz in reach:
        pl.semaphore_signal(barrier, inc=1, device_id=column(n, dz), device_id_type=MESH)
    total = len(reach)
    for k in range(2):
        for d in range(2, counts[k] - 1):
            pl.semaphore_signal(
                barrier, inc=1, device_id={axes[k]: lax.rem(me[k] + d, counts[k])},
                device_id_type=MESH
            )
            total += 1

    zero_plane = jnp.zeros((2, SY, SZ), f32)
    s_v[0:2, 8:8 + SY, :] = zero_plane
    s_v[SX + 2:SX + 4, 8:8 + SY, :] = zero_plane
    zero_rows = jnp.zeros((SX, 2, SZ), f32)
    s_v[2:SX + 2, 6:8, :] = zero_rows
    s_v[2:SX + 2, 8 + SY:10 + SY, :] = zero_rows

    def split_store(ref, index, value):
        high = value.astype(bf16)
        ref[index + (0,)] = high
        ref[index + (1,)] = (value - high.astype(f32)).astype(bf16)

    def ext_q(q):
        return jnp.where(q < PY, q, jnp.where(q < PY + 2, q - PY - 2, q - 2))

    def outer(along_x, along_y):
        return jnp.concatenate([along_x[p:p + 1] * along_y for p in range(along_x.shape[0])], axis=0)

    col = iota((8, KC), 1)
    col2 = iota((QE, KC), 1)
    split_store(wf_v, (), outer(weight(col // SY, iota((8, KC), 0) - 2, SPF)[0:5],
                                weight(col2 % SY, ext_q(iota((QE, KC), 0)), SPF)))
    along_y = weight(col % SY, iota((8, KC), 0) - 2, SPC)
    for c in range(cells):
        split_store(wc_v, (c,), outer(
            weight(col // SY + c * SPF, iota((8, KC), 0) - 2, SPC)[0:CX], along_y))
    col, row = iota((QE, 4 * SX), 1), iota((QE, 4 * SX), 0)
    face_x, face_y = (col % (2 * SX)) // 2, col % 2 + (SY - 2) * (col // (2 * SX))
    along_x = weight(face_x, row - 2, SPF)[0:EX]
    along_y = weight(face_y, ext_q(row), SPF)
    split_store(wy_v, (), jnp.concatenate([
        outer(along_x, along_y[0:PY]), outer(along_x, along_y[PY:QE]),
        outer(weight(face_x, row - 2, SPC)[0:CX], weight(face_y, row - 2, SPC)[0:CQ])], axis=0))
    row, col = iota((4 * SX, 128), 0), iota((4 * SX, 128), 1)
    face_x = (row % (2 * SX)) // 4 + jnp.where(row % 4 < 2, SX // 2, 0)
    place = row % 2 + 2 - 2 * (row // (2 * SX))
    wxe_v[...] = jnp.where(col % 4 == place, jnp.where(
        col < 64, weight(face_x, col // 4 - 2, SPF), weight(face_x, col // 4 - 18, SPC)), 0.0)
    row, col = iota((2 * SZ, 2 * SZ), 0) % SZ, iota((2 * SZ, 2 * SZ), 1)
    away = row - col
    slope = jnp.where(away == 1, 8.0, jnp.where(away == -1, -8.0, jnp.where(
        away == -2, 1.0, jnp.where(away == 2, -1.0, 0.0))))
    pick = jnp.where(row == (col % 4 + SZ - 2) % SZ, 1.0, 0.0)
    pz_v[...] = jnp.where(col < SZ, slope, pick).astype(bf16)
    rows, cols = iota((SZ, 128), 0), iota((SZ, 128), 1)
    bzc_v[...] = weight(rows, cols % 8 - 2, SPC) * (SPC ** -1.5 / 24.0)
    accf[...] = jnp.zeros(accf.shape, f32)
    accc[...] = jnp.zeros(accc.shape, f32)

    lane = iota((SY, SZ), 1)
    half_x = SX // 2

    def split(value):
        high = value.astype(bf16)
        return high, (value - high.astype(f32)).astype(bf16)

    for c in range(cells):
        load_wait(c)
        wide = ([], [])
        for x in range(c * SPF, (c + 1) * SPF):
            w, f = w_v[x], f_v[x]
            s, d = w + f, w - f
            s_v[x + 2, 8:8 + SY, :] = s
            w_v[x] = d
            for side, part in ((0, slice(0, 2)), (1, slice(SY - 2, SY))):
                ysend[side, 2 * x:2 * x + 2, :] = s[part]
                yd[side, 2 * x:2 * x + 2, :] = d[part]
            for n, value in enumerate((s, d)):
                wide[n].append(jnp.concatenate(split(value), axis=1))
        out = jnp.dot(jnp.concatenate(wide[0], axis=0), pz_v[...], preferred_element_type=f32)
        gz_v[c] = out[:, 0:SZ]
        picked = (out[:, SZ:2 * SZ],
                  jnp.dot(jnp.concatenate(wide[1], axis=0), pz_v[:, SZ:2 * SZ], preferred_element_type=f32))
        tile = c * SPF // half_x
        for n in range(2):
            pack = None if c * SPF % half_x == 0 else zp_v[n, tile]
            for xx in range(SPF):
                value = picked[n][xx * SY:(xx + 1) * SY]
                here = lane // 4 == (c * SPF + xx) % half_x
                pack = value if pack is None else jnp.where(here, value, pack)
            zp_v[n, tile] = pack
    upper = lane % 4 >= 2
    for n, ref in enumerate((zsend, zd)):
        ref[0] = jnp.where(upper, zp_v[n, 0], pltpu.roll(zp_v[n, 1], SZ - 2, 1))
        ref[1] = jnp.where(upper, pltpu.roll(zp_v[n, 0], 2, 1), zp_v[n, 1])

    pl.semaphore_wait(barrier, total)

    def neighbour_copy(k, side, src, dst, send, recv):
        step = [1, 1, 1]
        step[k] = 2 * side
        return pltpu.make_async_remote_copy(
            src_ref=src, dst_ref=dst, send_sem=send, recv_sem=recv,
            device_id=toward(step), device_id_type=MESH,
        )

    def halo(k, side):
        if k == 0:
            src = s_v.at[pl.ds(2 if side == 0 else SX, 2), pl.ds(8, SY), :]
        else:
            src = (ysend if k == 1 else zsend).at[side]
        return neighbour_copy(k, side, src, (xrecv, yrecv, zrecv)[k].at[1 - side],
                              hs_sem.at[k], hr_sem.at[k])

    def whole(k, ref, send, recv):
        return neighbour_copy(k, 0, ref, ref, send, recv)

    for k in (1, 2, 0):
        for side in range(2):
            halo(k, side).start()

    def forces(i):
        T = 16
        tiles = {}
        for r in range(0, SY, T):
            at = 8 + r
            near = [s_v[i * SPF + n, at:at + T, :] for n in range(4)]
            for xx in range(SPF):
                x = i * SPF + xx
                near.append(s_v[x + 4, at:at + T, :])
                d = w_v[x, r:r + T, :]
                gx = near[0] - near[4] + 8.0 * (near[3] - near[1])
                near.pop(0)
                gy = (s_v[x + 2, at - 2:at - 2 + T, :] - s_v[x + 2, at + 2:at + 2 + T, :]
                      + 8.0 * (s_v[x + 2, at + 1:at + 1 + T, :] - s_v[x + 2, at - 1:at - 1 + T, :]))
                row = xx * SY + r
                gz = gz_v[i, row:row + T, :]
                tiles[row] = [split(g * d) for g in (gx, gy, gz)]
        return [jnp.concatenate([
            jnp.concatenate([tiles[row][a][n] for row in sorted(tiles)], axis=0)
            for a in range(3)], axis=1) for n in range(2)]

    def cell_weights(i):
        return jnp.concatenate([wf_v[0], wc_v[i, 0], wf_v[1], wc_v[i, 1]], axis=0)

    def project(weights, high, low):
        many = weights.shape[0] // 2
        both = jnp.dot(weights, high, preferred_element_type=f32)
        return both[:many] + both[many:] + jnp.dot(
            weights[:many], low, preferred_element_type=f32)

    def collect(i, out, part):
        fine = out[:5 * QE].reshape(5, 2, PY, out.shape[1])
        accf[0, i:i + 5, :, part] += fine[:, 0]
        accf[1, i:i + 5, :, part] += fine[:, 1]
        accc[:, part] += out[5 * QE:]

    for i in range(cells):
        collect(i, project(cell_weights(i), *forces(i)), slice(0, lanes))

    for k, got in enumerate((xrecv, yrecv, zrecv)):
        whole(k, got, hs_sem.at[k], hr_sem.at[k]).wait_recv()

    gate = [[jnp.where(h, 1.0, 0.0) for h in pair] for pair in has]

    def diff(x):
        return w_v[x]

    for side, i in ((0, 0), (1, cells - 1)):
        r0, r1 = xrecv[side, 0] * gate[0][side], xrecv[side, 1] * gate[0][side]
        if side == 0:
            face = jnp.concatenate([(r0 - 8.0 * r1) * diff(0), r1 * diff(1)], axis=0)
            part = slice(0, 2 * SY)
        else:
            face = jnp.concatenate([-r0 * diff(SX - 2), (8.0 * r0 - r1) * diff(SX - 1)], axis=0)
            part = slice(KC - 2 * SY, KC)
        collect(i, project(cell_weights(i)[:, part], *split(face)), slice(0, SZ))

    rows = iota((SX // 4, 8, SZ), 1) % 2 == 0
    r = (yrecv[0] * gate[1][0]).reshape(SX // 4, 8, SZ)
    low = jnp.where(rows, r - 8.0 * pltpu.roll(r, 7, 1), r).reshape(2 * SX, SZ) * yd[0]
    r = (yrecv[1] * gate[1][1]).reshape(SX // 4, 8, SZ)
    high = jnp.where(rows, -r, 8.0 * pltpu.roll(r, 1, 1) - r).reshape(2 * SX, SZ) * yd[1]
    out = project(jnp.concatenate([wy_v[0], wy_v[1]], axis=0),
                  *split(jnp.concatenate([low, high], axis=0)))
    for half in range(2):
        accf[half, :, :, SZ:2 * SZ] += out[half * EX * PY:(half + 1) * EX * PY].reshape(EX, PY, SZ)
    accc[:, SZ:2 * SZ] += out[2 * EX * PY:]

    even = lane % 2 == 0
    dl = zrecv[0] * gate[2][0]
    dh = zrecv[1] * gate[2][1]
    low = jnp.where(even, dl - 8.0 * pltpu.roll(dl, SZ - 1, 1), dl) * zd[0]
    high = jnp.where(even, -dh, 8.0 * pltpu.roll(dh, 1, 1) - dh) * zd[1]
    row, col = iota((QE + CQ, SY), 0), iota((QE + CQ, SY), 1)
    along_y = jnp.where(row < QE, weight(col, ext_q(row), SPF), weight(col, row - QE - 2, SPC))
    out = nn(nn(along_y, jnp.concatenate([low, high], axis=1)), wxe_v[...])
    at = iota((PY, SZ), 1)
    edge = (at < 2) | (at >= SZ - 2)

    def spread(half, shift):
        return jnp.where(edge, pltpu.roll(out[half * PY:(half + 1) * PY], shift % 128, 1), 0.0)

    for p in range(EX):
        for half in range(2):
            accf[half, p, :, 2 * SZ:3 * SZ] += spread(half, 254 - 4 * p)
    for p in range(CX):
        accc[p * CQ:(p + 1) * CQ, 2 * SZ:3 * SZ] += spread(2, 254 - 64 - 4 * p)

    stack = jnp.concatenate([accc[:, a * SZ:(a + 1) * SZ] for a in range(3)], axis=0)
    shares = nn(stack, bzc_v[...])
    rows, cols = iota((CR, 128), 0), iota((CR, 128), 1)
    keep = (cols // 32 == 2 * ((rows // CQ) % 2) + rows % 2) & (cols % 32 < 24)
    value = jnp.where(cols % 32 < 8, shares[0:CR],
                      jnp.where(cols % 32 < 16, shares[CR:2 * CR], shares[2 * CR:3 * CR]))
    value = jnp.where(keep, value, 0.0).reshape(3, 2, CQ, 128)
    value = value[:, 0] + value[:, 1]
    value = value + pltpu.roll(value, 7, 1)
    for n, (d, e) in enumerate(columns):
        cmsg[n] = value[d, 2 * e:2 * e + 1, :]
    mine = pl.ds(me[2], 1)
    crecv[4, mine, :] = value[1, 2:3, :]
    for n, dz in reach:
        pltpu.make_async_remote_copy(
            src_ref=cmsg.at[n], dst_ref=crecv.at[8 - n, mine, :],
            send_sem=n_sem.at[0], recv_sem=n_sem.at[1],
            device_id=column(n, dz), device_id_type=MESH,
        ).start()

    rows, cols = iota((RZ, SZ), 0), iota((RZ, SZ), 1)

    def ext_point(row):
        return jnp.where(row < PZ, row, jnp.where(row < PZ + 2, row - PZ - 2, row - 2))

    bz = weight(cols, ext_point(rows), SPF) * (SPF ** -1.5 / 24.0)
    for a in range(3):
        for half in range(2):
            block = accf[half, :, :, a * SZ:(a + 1) * SZ].reshape(EX * PY, SZ)
            tz_v[half, a] = nt(bz, block)

    for copy in small:
        copy.wait()
    shape = (PX * PY, EX * QE)
    rows, cols = iota(shape, 0), iota(shape, 1)
    ox, oy, oz = me[0] * PX, me[1] * PY, me[2] * PZ
    wide, inner = cols // (EX * PY), cols % (EX * PY)
    planes = bend_planes(inner // PY - 2 + ox, ext_q(inner % PY + PY * wide) + oy,
                         rows // PY + ox, rows % PY + oy, PX * nx, PY * ny)
    zr, zc = ext_point(iota((RZ, PZ), 0)) + oz, iota((RZ, PZ), 1) + oz
    along = jnp.concatenate([same(zr, zc), diff1(zr, zc), diff2(zr, zc, PZ * nz)], axis=0)
    turned = nt(along, fc_ref[...].reshape(3 * PX * PY, PZ))
    turned = jnp.concatenate([jnp.concatenate([
        turned[k * RZ:(k + 1) * RZ, a * PX * PY:(a + 1) * PX * PY] for k in range(3)], axis=1)
        for a in range(3)], axis=0)
    bent = nn(turned, jnp.concatenate(planes, axis=0))
    for a in range(3):
        for half in range(2):
            tz_v[half, a] += bent[a * RZ:(a + 1) * RZ, half * EX * PY:(half + 1) * EX * PY]
            for side in range(2):
                zmsg[side, half, 2 * a:2 * a + 2, :] = tz_v[
                    half, a, PZ + 2 * side:PZ + 2 * side + 2, :]

    def fine_start(k):
        for side in range(2):
            source = (b_v, a_v.at[1], zmsg.at[side])[k]
            neighbour_copy(k, side, source, (bgot, agot, zgot)[k].at[1 - side],
                           ms_sem.at[k], mr_sem.at[k]).start()

    def fine_whole(k):
        return whole(k, (bgot, agot, zgot)[k], ms_sem.at[k], mr_sem.at[k])

    def coarse_slot(k, n):
        if k == 0:
            return xrow.at[n]
        return xrow.at[me[0], :, pl.ds(n, 1), :]

    def coarse_start(k):
        for d in far_first(counts[k]):
            pltpu.make_async_remote_copy(
                src_ref=coarse_slot(k, me[k]), dst_ref=coarse_slot(k, me[k]),
                send_sem=cs_sem.at[k], recv_sem=cr_sem.at[k],
                device_id={axes[k]: lax.rem(me[k] + d, counts[k])}, device_id_type=MESH,
            ).start()

    def coarse_whole(k):
        part = pl.ds(0, counts[k] - 1)
        ref = (xrow.at[part], xrow.at[me[0], :, part, :])[k]
        return whole(k, ref, cs_sem.at[k], cr_sem.at[k])

    fine_start(2)

    q_at, r_at = iota((KX, KY, 128), 1), iota((KX, KY, 128), 2)

    def laplace(c):
        zero = jnp.zeros((1, KY, 128), f32)
        total = (jnp.concatenate([c[1:], zero], axis=0) + jnp.concatenate([zero, c[:-1]], axis=0)
                 + jnp.where(q_at < KY - 1, pltpu.roll(c, KY - 1, 1), 0.0)
                 + jnp.where(q_at > 0, pltpu.roll(c, 1, 1), 0.0)
                 + pltpu.roll(c, 127, 2) + pltpu.roll(c, 1, 2))
        return jnp.where(r_at < KZ, total - 6.0 * c, 0.0)

    clane[...] = jnp.zeros(clane.shape, f32)
    for a in range(3):
        clane[:, :, 0:KZ] = cc_ref[a]
        cbend[a] = BEND * laplace(laplace(clane[...]))

    all_shares = crest.at[pl.ds(0, len(reach))]
    whole(0, all_shares, n_sem.at[0], n_sem.at[1]).wait_recv()
    total = crecv[4]
    for n, (d, e) in enumerate(columns):
        if n != 4:
            total = total + jnp.where(inside((d, e, 1)), crecv[n], 0.0)
    sub, at = iota((nz, 128), 0), iota((nz, 128), 1) % 32
    keep = (at >= 4 * sub - 2) & (at < 4 * sub + 6) & (at < KZ)
    for a in range(3):
        value = None
        for n in range(nz):
            shift = (4 * n - 2 - 8 * a) % 128
            moved = pltpu.roll(total, shift, 1) if shift else total
            value = moved if n == 0 else jnp.where(sub == n, moved, value)
        xrow[me[0], a, pl.ds(me[1], 1), :] = jnp.sum(
            jnp.where(keep, value, 0.0), axis=0, keepdims=True)
    coarse_start(1)

    fine_whole(2).wait_recv()
    for half in range(2):
        for a in range(3):
            part = slice(2 * a, 2 * a + 2)
            tz_v[half, a, 0:2, :] = tz_v[half, a, 0:2, :] + zgot[0, half, part, :] * gate[2][0]
            tz_v[half, a, PZ - 2:PZ, :] = (
                tz_v[half, a, PZ - 2:PZ, :] + zgot[1, half, part, :] * gate[2][1])
            a_v[half, a * PZ:(a + 1) * PZ, :] = tz_v[half, a, 0:PZ, :]
    fine_start(1)

    coarse_whole(1).wait_recv()
    coarse_start(0)

    fine_whole(1).wait_recv()
    shape = (EX * PY, EX * PY)
    rows, cols = iota(shape, 0), iota(shape, 1)
    p_same = rows // PY == cols // PY
    q, r = rows % PY, cols % PY
    low = jnp.where(p_same & (q == r + 2) & (r < 2), 1.0, 0.0)
    high = jnp.where(p_same & (q == r - (PY - 2)) & (r >= PY - 2), 1.0, 0.0)
    b_v[...] = (a_v[0] + nn(agot[0] * gate[1][0], low) + nn(agot[1] * gate[1][1], high))
    fine_start(0)

    fine_whole(0).wait_recv()
    shape = (PX * PY, EX * PY)
    rows, cols = iota(shape, 0), iota(shape, 1)
    own = jnp.where(cols == rows + 2 * PY, 1.0, 0.0)
    low = jnp.where((cols == rows + (PX + 2) * PY) & (rows < 2 * PY), gate[0][0], 0.0)
    high = jnp.where((cols == rows - (PX - 2) * PY) & (rows >= (PX - 2) * PY), gate[0][1], 0.0)
    for a in range(3):
        part = slice(a * PZ, (a + 1) * PZ)
        out = nt(own, b_v[part]) + nt(low, bgot[0, part]) + nt(high, bgot[1, part])
        fo_ref[a] = out.reshape(PX, PY, PZ)

    for k, got in enumerate((xrecv, yrecv, zrecv)):
        whole(k, got, hs_sem.at[k], hr_sem.at[k]).wait_send()
        fine_whole(k).wait_send()
        if k < 2:
            coarse_whole(k).wait_send()
    whole(0, all_shares, n_sem.at[0], n_sem.at[1]).wait_send()

    coarse_whole(0).wait_recv()
    for i in range(nx):
        for a in range(3):
            block = xrow[i, a]
            for g in range(4):
                value = block if g == 0 else pltpu.roll(block, 128 - 32 * g, 1)
                p = 2 * i + g // 2
                part = pl.ds(g % 2, ny, stride=2)
                co_ref[a, p, part, :] = (value + cbend[a, p, part, :])[:, 0:KZ]


def solution(mesh):
    sizes = tuple(mesh.shape[a] for a in ("gx", "gy", "gz"))

    def step(warped, fixed, fine, coarse):
        SX, SY, SZ = warped.shape
        PX, PY, PZ = SX // SPF, SY // SPF, SZ // SPF
        KX, KY, KZ = coarse.shape[1:]
        EX, QE, RZ = PX + 4, 2 * PY, PZ + 8
        CR = 48
        KC = SPF * SY
        vmem = pl.BlockSpec(memory_space=pltpu.VMEM)
        hbm = pl.BlockSpec(memory_space=pltpu.HBM)
        V = pltpu.VMEM
        D = pltpu.SemaphoreType.DMA
        return pl.pallas_call(
            functools.partial(kernel, sizes),
            out_shape=(V(fine.shape, f32), V(coarse.shape, f32)),
            in_specs=[hbm] * 4,
            out_specs=(vmem, vmem),
            scratch_shapes=[
                V((SX, SY, SZ), f32), V((SX, SY, SZ), f32),
                V((3, PX, PY, PZ), f32), V(coarse.shape, f32),
                V((SX + 4, SY + 16, SZ), f32), V((2, 2, SY, SZ), f32),
                V((2, 2 * SX, SZ), f32), V((2, 2 * SX, SZ), f32), V((2, 2 * SX, SZ), f32),
                V((2, SY, SZ), f32), V((2, SY, SZ), f32), V((2, SY, SZ), f32),
                V((2, 5 * QE, KC), bf16), V((SX // SPF, 2, CR, KC), bf16),
                V((2, EX * QE + CR, 4 * SX), bf16), V((4 * SX, 128), f32), V((SZ, 128), f32),
                V((2 * SZ, 2 * SZ), bf16),
                V((SX // SPF, KC, SZ), f32), V((2, 2, SY, SZ), f32),
                V((2, EX, PY, 3 * SZ), f32), V((CR, 3 * SZ), f32),
                V((2, 3, RZ, EX * PY), f32),
                V((KX, KY, 128), f32), V((3, KX, KY, 128), f32),
                V((2, 2, 8, EX * PY), f32), V((2, 2, 8, EX * PY), f32),
                V((2, 3 * PZ, EX * PY), f32), V((2, 3 * PZ, EX * PY), f32),
                V((3 * PZ, EX * PY), f32), V((2, 3 * PZ, EX * PY), f32),
                V((9, 1, 128), f32), V((9, sizes[2], 128), f32),
                V((9 * sizes[2], 128), f32), V((sizes[0], 3, sizes[1], 128), f32),
                D((SX // SPF,)), D((2,)), D((3,)), D((3,)),
                D((3,)), D((3,)), D((2,)), D((2,)), D((2,)),
            ],
            compiler_params=pltpu.CompilerParams(
                collective_id=0, has_side_effects=True, vmem_limit_bytes=66000000
            ),
        )(warped, fixed, fine, coarse)

    in_specs = (P("gx", "gy", "gz"), P("gx", "gy", "gz"), P(None, "gx", "gy", "gz"), P())
    out_specs = (P(None, "gx", "gy", "gz"), P())
    return jax.shard_map(
        step, mesh=mesh, in_specs=in_specs, out_specs=out_specs, check_vma=False
    )
```

```python
import functools

import jax
import jax.numpy as jnp
from jax import lax
from jax.experimental import pallas as pl
from jax.experimental.pallas import tpu as pltpu
from jax.sharding import PartitionSpec as P

SPF = 8
SPC = 32
BEND = 0.01
HI = lax.Precision.HIGHEST
MESH = pl.DeviceIdType.MESH
f32 = jnp.float32
bf16 = jnp.bfloat16


def nn(a, b):
    return lax.dot_general(
        a, b, (((1,), (0,)), ((), ())), precision=HI, preferred_element_type=f32
    )


def nt(a, b):
    return lax.dot_general(
        a, b, (((1,), (1,)), ((), ())), precision=HI, preferred_element_type=f32
    )


def spline(t):
    m = jnp.abs(t)
    inner = 2.0 / 3.0 - m * m + 0.5 * m * m * m
    r = 2.0 - m
    outer = r * r * r * (1.0 / 6.0)
    return jnp.where(m < 1.0, inner, jnp.where(m < 2.0, outer, 0.0))


def weight(voxel, point, spacing):
    scaled = (2 * voxel + 1 - spacing * (2 * point + 1)).astype(f32)
    return spline(scaled * (0.5 / spacing))


def iota(shape, axis):
    return lax.broadcasted_iota(jnp.int32, shape, axis)


def diff1(out, inp):
    d = jnp.abs(out - inp)
    return jnp.where(d == 0, -2.0, jnp.where(d == 1, 1.0, 0.0)).astype(f32)


def diff2(out, inp, count):
    d = jnp.abs(out - inp)
    edge = (inp == 0) | (inp == count - 1)
    centre = jnp.where(edge, 5.0, 6.0)
    return jnp.where(
        d == 0, centre, jnp.where(d == 1, -4.0, jnp.where(d == 2, 1.0, 0.0))
    ).astype(f32)


def same(out, inp):
    return jnp.where(out == inp, 1.0, 0.0).astype(f32)


def bend_planes(px, py, qx, qy, cx, cy):
    jx, jy = same(px, qx), same(py, qy)
    tx, ty = diff1(px, qx), diff1(py, qy)
    m0 = diff2(px, qx, cx) * jy + jx * diff2(py, qy, cy) + 2.0 * tx * ty
    m1 = 2.0 * (tx * jy + jx * ty)
    return m0 * BEND, m1 * BEND, jx * jy * BEND


def kernel(sizes, w_hbm, f_hbm, fc_hbm, cc_hbm, fo_ref, co_ref,
           w_v, f_v, fc_ref, cc_ref, s_v, xrecv, ysend, yrecv, yd, zsend, zrecv, zd,
           wf_v, wc_v, wy_v, wxe_v, bzc_v, pz_v, gz_v, zp_v,
           accf, accc, tz_v, clane, cbend, zmsg, zgot, a_v, agot, b_v, bgot,
           cmsg, crecv, crest, xrow, load_sem, small_sem, hs_sem, hr_sem,
           ms_sem, mr_sem, n_sem, cs_sem, cr_sem, ready):
    nx, ny, nz = sizes
    axes = ("gx", "gy", "gz")
    counts = sizes
    me = [lax.axis_index(a) for a in axes]
    SX, SY, SZ = w_v.shape
    PX, PY, PZ = SX // SPF, SY // SPF, SZ // SPF
    KX, KY, KZ = cc_ref.shape[1:]
    EX, QE = PX + 4, 2 * PY
    CR = accc.shape[0]
    CQ, CX = 8, CR // 8
    RZ = tz_v.shape[2]
    KC = SPF * SY
    cells = SX // SPF
    lanes = 3 * SZ

    for c in range(cells):
        part = pl.ds(c * SPF, SPF)
        pltpu.make_async_copy(w_hbm.at[part], w_v.at[part], load_sem.at[c]).start()
        pltpu.make_async_copy(f_hbm.at[part], f_v.at[part], load_sem.at[c]).start()
    small = (pltpu.make_async_copy(fc_hbm, fc_ref, small_sem.at[0]),
             pltpu.make_async_copy(cc_hbm, cc_ref, small_sem.at[1]))
    for copy in small:
        copy.start()

    def load_wait(c):
        both = pl.ds(0, 2 * SPF)
        pltpu.make_async_copy(w_hbm.at[both], w_v.at[both], load_sem.at[c]).wait()

    has = [(me[k] > 0, me[k] < counts[k] - 1) for k in range(3)]

    def toward(step):
        return {axes[k]: lax.rem(me[k] + (counts[k] + step[k] - 1), counts[k])
                for k in range(3) if step[k] != 1}

    def inside(step):
        ok = None
        for k in range(3):
            if step[k] != 1:
                here = has[k][0] if step[k] == 0 else has[k][1]
                ok = here if ok is None else ok & here
        return ok

    def far_first(n):
        return sorted(range(1, n), key=lambda d: -min(d, n - d))

    columns = [(d, e) for d in range(3) for e in range(3)]
    reach = [(n, dz) for dz in far_first(nz) + [0] for n in range(9) if (n, dz) != (4, 0)]

    def column(n, dz):
        there = toward(columns[n] + (1,))
        if dz:
            there[axes[2]] = lax.rem(me[2] + dz, nz)
        return there

    barrier = pltpu.get_barrier_semaphore()
    total = 0
    for k in (2, 1, 0):
        for d in far_first(counts[k]):
            pl.semaphore_signal(
                barrier, inc=1, device_id={axes[k]: lax.rem(me[k] + d, counts[k])},
                device_id_type=MESH
            )
            total += 1
    around = [n for n in range(9) if n != 4]
    for n in around:
        if n % 2 == 0:
            pl.semaphore_signal(barrier, inc=1, device_id=column(n, 0), device_id_type=MESH)
            total += 1

    zero_plane = jnp.zeros((2, SY, SZ), f32)
    s_v[0:2, 8:8 + SY, :] = zero_plane
    s_v[SX + 2:SX + 4, 8:8 + SY, :] = zero_plane
    zero_rows = jnp.zeros((SX, 2, SZ), f32)
    s_v[2:SX + 2, 6:8, :] = zero_rows
    s_v[2:SX + 2, 8 + SY:10 + SY, :] = zero_rows

    row, col = iota((2 * SZ, 2 * SZ), 0) % SZ, iota((2 * SZ, 2 * SZ), 1)
    away = row - col
    slope = jnp.where(away == 1, 8.0, jnp.where(away == -1, -8.0, jnp.where(
        away == -2, 1.0, jnp.where(away == 2, -1.0, 0.0))))
    pick = jnp.where(row == (col % 4 + SZ - 2) % SZ, 1.0, 0.0)
    pz_v[...] = jnp.where(col < SZ, slope, pick).astype(bf16)
    lane = iota((SY, SZ), 1)
    half_x = SX // 2

    def split(value):
        high = value.astype(bf16)
        return high, (value - high.astype(f32)).astype(bf16)

    for c in range(cells):
        load_wait(c)
        wide = ([], [])
        for x in range(c * SPF, (c + 1) * SPF):
            w, f = w_v[x], f_v[x]
            s, d = w + f, w - f
            s_v[x + 2, 8:8 + SY, :] = s
            w_v[x] = d
            for side, part in ((0, slice(0, 2)), (1, slice(SY - 2, SY))):
                ysend[side, 2 * x:2 * x + 2, :] = s[part]
                yd[side, 2 * x:2 * x + 2, :] = d[part]
            for n, value in enumerate((s, d)):
                wide[n].append(jnp.concatenate(split(value), axis=1))
        out = jnp.dot(jnp.concatenate(wide[0], axis=0), pz_v[...], preferred_element_type=f32)
        gz_v[c] = out[:, 0:SZ]
        picked = (out[:, SZ:2 * SZ],
                  jnp.dot(jnp.concatenate(wide[1], axis=0), pz_v[:, SZ:2 * SZ], preferred_element_type=f32))
        tile = c * SPF // half_x
        for n in range(2):
            pack = None if c * SPF % half_x == 0 else zp_v[n, tile]
            for xx in range(SPF):
                value = picked[n][xx * SY:(xx + 1) * SY]
                here = lane // 4 == (c * SPF + xx) % half_x
                pack = value if pack is None else jnp.where(here, value, pack)
            zp_v[n, tile] = pack
    upper = lane % 4 >= 2
    for n, ref in enumerate((zsend, zd)):
        ref[0] = jnp.where(upper, zp_v[n, 0], pltpu.roll(zp_v[n, 1], SZ - 2, 1))
        ref[1] = jnp.where(upper, pltpu.roll(zp_v[n, 0], 2, 1), zp_v[n, 1])

    pl.semaphore_wait(barrier, total)
    for n in around:
        pl.semaphore_signal(ready, inc=1, device_id=column(n, 0), device_id_type=MESH)

    def neighbour_copy(k, side, src, dst, send, recv):
        step = [1, 1, 1]
        step[k] = 2 * side
        return pltpu.make_async_remote_copy(
            src_ref=src, dst_ref=dst, send_sem=send, recv_sem=recv,
            device_id=toward(step), device_id_type=MESH,
        )

    def halo(k, side):
        if k == 0:
            src = s_v.at[pl.ds(2 if side == 0 else SX, 2), pl.ds(8, SY), :]
        else:
            src = (ysend if k == 1 else zsend).at[side]
        return neighbour_copy(k, side, src, (xrecv, yrecv, zrecv)[k].at[1 - side],
                              hs_sem.at[k], hr_sem.at[k])

    def whole(k, ref, send, recv):
        return neighbour_copy(k, 0, ref, ref, send, recv)

    for k in (1, 2, 0):
        for side in range(2):
            halo(k, side).start()

    def split_store(ref, index, value):
        high = value.astype(bf16)
        ref[index + (0,)] = high
        ref[index + (1,)] = (value - high.astype(f32)).astype(bf16)

    def ext_q(q):
        return jnp.where(q < PY, q, jnp.where(q < PY + 2, q - PY - 2, q - 2))

    def outer(along_x, along_y):
        return jnp.concatenate([along_x[p:p + 1] * along_y for p in range(along_x.shape[0])], axis=0)

    col = iota((8, KC), 1)
    col2 = iota((QE, KC), 1)
    split_store(wf_v, (), outer(weight(col // SY, iota((8, KC), 0) - 2, SPF)[0:5],
                                weight(col2 % SY, ext_q(iota((QE, KC), 0)), SPF)))
    along_y = weight(col % SY, iota((8, KC), 0) - 2, SPC)
    for c in range(cells):
        split_store(wc_v, (c,), outer(
            weight(col // SY + c * SPF, iota((8, KC), 0) - 2, SPC)[0:CX], along_y))
    col, row = iota((QE, 4 * SX), 1), iota((QE, 4 * SX), 0)
    face_x, face_y = (col % (2 * SX)) // 2, col % 2 + (SY - 2) * (col // (2 * SX))
    along_x = weight(face_x, row - 2, SPF)[0:EX]
    along_y = weight(face_y, ext_q(row), SPF)
    split_store(wy_v, (), jnp.concatenate([
        outer(along_x, along_y[0:PY]), outer(along_x, along_y[PY:QE]),
        outer(weight(face_x, row - 2, SPC)[0:CX], weight(face_y, row - 2, SPC)[0:CQ])], axis=0))
    row, col = iota((4 * SX, 128), 0), iota((4 * SX, 128), 1)
    face_x = (row % (2 * SX)) // 4 + jnp.where(row % 4 < 2, SX // 2, 0)
    place = row % 2 + 2 - 2 * (row // (2 * SX))
    wxe_v[...] = jnp.where(col % 4 == place, jnp.where(
        col < 64, weight(face_x, col // 4 - 2, SPF), weight(face_x, col // 4 - 18, SPC)), 0.0)
    rows, cols = iota((SZ, 128), 0), iota((SZ, 128), 1)
    bzc_v[...] = weight(rows, cols % 8 - 2, SPC) * (SPC ** -1.5 / 24.0)
    accf[...] = jnp.zeros(accf.shape, f32)
    accc[...] = jnp.zeros(accc.shape, f32)

    def forces(i):
        T = 16
        tiles = {}
        for r in range(0, SY, T):
            at = 8 + r
            near = [s_v[i * SPF + n, at:at + T, :] for n in range(4)]
            for xx in range(SPF):
                x = i * SPF + xx
                near.append(s_v[x + 4, at:at + T, :])
                d = w_v[x, r:r + T, :]
                gx = near[0] - near[4] + 8.0 * (near[3] - near[1])
                near.pop(0)
                gy = (s_v[x + 2, at - 2:at - 2 + T, :] - s_v[x + 2, at + 2:at + 2 + T, :]
                      + 8.0 * (s_v[x + 2, at + 1:at + 1 + T, :] - s_v[x + 2, at - 1:at - 1 + T, :]))
                row = xx * SY + r
                gz = gz_v[i, row:row + T, :]
                tiles[row] = [split(g * d) for g in (gx, gy, gz)]
        return [jnp.concatenate([
            jnp.concatenate([tiles[row][a][n] for row in sorted(tiles)], axis=0)
            for a in range(3)], axis=1) for n in range(2)]

    def cell_weights(i):
        return jnp.concatenate([wf_v[0], wc_v[i, 0], wf_v[1], wc_v[i, 1]], axis=0)

    def project(weights, high, low):
        many = weights.shape[0] // 2
        both = jnp.dot(weights, high, preferred_element_type=f32)
        return both[:many] + both[many:] + jnp.dot(
            weights[:many], low, preferred_element_type=f32)

    def collect(i, out, part):
        fine = out[:5 * QE].reshape(5, 2, PY, out.shape[1])
        accf[0, i:i + 5, :, part] += fine[:, 0]
        accf[1, i:i + 5, :, part] += fine[:, 1]
        accc[:, part] += out[5 * QE:]

    for i in range(cells):
        collect(i, project(cell_weights(i), *forces(i)), slice(0, lanes))

    for k, got in enumerate((xrecv, yrecv, zrecv)):
        whole(k, got, hs_sem.at[k], hr_sem.at[k]).wait_recv()

    gate = [[jnp.where(h, 1.0, 0.0) for h in pair] for pair in has]

    def diff(x):
        return w_v[x]

    for side, i in ((0, 0), (1, cells - 1)):
        r0, r1 = xrecv[side, 0] * gate[0][side], xrecv[side, 1] * gate[0][side]
        if side == 0:
            face = jnp.concatenate([(r0 - 8.0 * r1) * diff(0), r1 * diff(1)], axis=0)
            part = slice(0, 2 * SY)
        else:
            face = jnp.concatenate([-r0 * diff(SX - 2), (8.0 * r0 - r1) * diff(SX - 1)], axis=0)
            part = slice(KC - 2 * SY, KC)
        collect(i, project(cell_weights(i)[:, part], *split(face)), slice(0, SZ))

    rows = iota((SX // 4, 8, SZ), 1) % 2 == 0
    r = (yrecv[0] * gate[1][0]).reshape(SX // 4, 8, SZ)
    low = jnp.where(rows, r - 8.0 * pltpu.roll(r, 7, 1), r).reshape(2 * SX, SZ) * yd[0]
    r = (yrecv[1] * gate[1][1]).reshape(SX // 4, 8, SZ)
    high = jnp.where(rows, -r, 8.0 * pltpu.roll(r, 1, 1) - r).reshape(2 * SX, SZ) * yd[1]
    out = project(jnp.concatenate([wy_v[0], wy_v[1]], axis=0),
                  *split(jnp.concatenate([low, high], axis=0)))
    for half in range(2):
        accf[half, :, :, SZ:2 * SZ] += out[half * EX * PY:(half + 1) * EX * PY].reshape(EX, PY, SZ)
    accc[:, SZ:2 * SZ] += out[2 * EX * PY:]

    even = lane % 2 == 0
    dl = zrecv[0] * gate[2][0]
    dh = zrecv[1] * gate[2][1]
    low = jnp.where(even, dl - 8.0 * pltpu.roll(dl, SZ - 1, 1), dl) * zd[0]
    high = jnp.where(even, -dh, 8.0 * pltpu.roll(dh, 1, 1) - dh) * zd[1]
    row, col = iota((QE + CQ, SY), 0), iota((QE + CQ, SY), 1)
    along_y = jnp.where(row < QE, weight(col, ext_q(row), SPF), weight(col, row - QE - 2, SPC))
    out = nn(nn(along_y, jnp.concatenate([low, high], axis=1)), wxe_v[...])
    at = iota((PY, SZ), 1)
    edge = (at < 2) | (at >= SZ - 2)

    def spread(half, shift):
        return jnp.where(edge, pltpu.roll(out[half * PY:(half + 1) * PY], shift % 128, 1), 0.0)

    for p in range(EX):
        for half in range(2):
            accf[half, p, :, 2 * SZ:3 * SZ] += spread(half, 254 - 4 * p)
    for p in range(CX):
        accc[p * CQ:(p + 1) * CQ, 2 * SZ:3 * SZ] += spread(2, 254 - 64 - 4 * p)

    stack = jnp.concatenate([accc[:, a * SZ:(a + 1) * SZ] for a in range(3)], axis=0)
    shares = nn(stack, bzc_v[...])
    rows, cols = iota((CR, 128), 0), iota((CR, 128), 1)
    keep = (cols // 32 == 2 * ((rows // CQ) % 2) + rows % 2) & (cols % 32 < 24)
    value = jnp.where(cols % 32 < 8, shares[0:CR],
                      jnp.where(cols % 32 < 16, shares[CR:2 * CR], shares[2 * CR:3 * CR]))
    value = jnp.where(keep, value, 0.0).reshape(3, 2, CQ, 128)
    value = value[:, 0] + value[:, 1]
    value = value + pltpu.roll(value, 7, 1)
    for n, (d, e) in enumerate(columns):
        cmsg[n] = value[d, 2 * e:2 * e + 1, :]
    mine = pl.ds(me[2], 1)
    crecv[4, mine, :] = value[1, 2:3, :]
    pl.semaphore_wait(ready, len(around))
    for n, dz in reach:
        pltpu.make_async_remote_copy(
            src_ref=cmsg.at[n], dst_ref=crecv.at[8 - n, mine, :],
            send_sem=n_sem.at[0], recv_sem=n_sem.at[1],
            device_id=column(n, dz), device_id_type=MESH,
        ).start()

    rows, cols = iota((RZ, SZ), 0), iota((RZ, SZ), 1)

    def ext_point(row):
        return jnp.where(row < PZ, row, jnp.where(row < PZ + 2, row - PZ - 2, row - 2))

    bz = weight(cols, ext_point(rows), SPF) * (SPF ** -1.5 / 24.0)
    for a in range(3):
        for half in range(2):
            block = accf[half, :, :, a * SZ:(a + 1) * SZ].reshape(EX * PY, SZ)
            tz_v[half, a] = nt(bz, block)

    for copy in small:
        copy.wait()
    shape = (PX * PY, EX * QE)
    rows, cols = iota(shape, 0), iota(shape, 1)
    ox, oy, oz = me[0] * PX, me[1] * PY, me[2] * PZ
    wide, inner = cols // (EX * PY), cols % (EX * PY)
    planes = bend_planes(inner // PY - 2 + ox, ext_q(inner % PY + PY * wide) + oy,
                         rows // PY + ox, rows % PY + oy, PX * nx, PY * ny)
    zr, zc = ext_point(iota((RZ, PZ), 0)) + oz, iota((RZ, PZ), 1) + oz
    along = jnp.concatenate([same(zr, zc), diff1(zr, zc), diff2(zr, zc, PZ * nz)], axis=0)
    turned = nt(along, fc_ref[...].reshape(3 * PX * PY, PZ))
    turned = jnp.concatenate([jnp.concatenate([
        turned[k * RZ:(k + 1) * RZ, a * PX * PY:(a + 1) * PX * PY] for k in range(3)], axis=1)
        for a in range(3)], axis=0)
    bent = nn(turned, jnp.concatenate(planes, axis=0))
    for a in range(3):
        for half in range(2):
            tz_v[half, a] += bent[a * RZ:(a + 1) * RZ, half * EX * PY:(half + 1) * EX * PY]
            for side in range(2):
                zmsg[side, half, 2 * a:2 * a + 2, :] = tz_v[
                    half, a, PZ + 2 * side:PZ + 2 * side + 2, :]

    def fine_start(k):
        for side in range(2):
            source = (b_v, a_v.at[1], zmsg.at[side])[k]
            neighbour_copy(k, side, source, (bgot, agot, zgot)[k].at[1 - side],
                           ms_sem.at[k], mr_sem.at[k]).start()

    def fine_whole(k):
        return whole(k, (bgot, agot, zgot)[k], ms_sem.at[k], mr_sem.at[k])

    def coarse_slot(k, n):
        if k == 0:
            return xrow.at[n]
        return xrow.at[me[0], :, pl.ds(n, 1), :]

    def coarse_start(k):
        for d in far_first(counts[k]):
            pltpu.make_async_remote_copy(
                src_ref=coarse_slot(k, me[k]), dst_ref=coarse_slot(k, me[k]),
                send_sem=cs_sem.at[k], recv_sem=cr_sem.at[k],
                device_id={axes[k]: lax.rem(me[k] + d, counts[k])}, device_id_type=MESH,
            ).start()

    def coarse_whole(k):
        part = pl.ds(0, counts[k] - 1)
        ref = (xrow.at[part], xrow.at[me[0], :, part, :])[k]
        return whole(k, ref, cs_sem.at[k], cr_sem.at[k])

    fine_start(2)

    q_at, r_at = iota((KX, KY, 128), 1), iota((KX, KY, 128), 2)

    def laplace(c):
        zero = jnp.zeros((1, KY, 128), f32)
        total = (jnp.concatenate([c[1:], zero], axis=0) + jnp.concatenate([zero, c[:-1]], axis=0)
                 + jnp.where(q_at < KY - 1, pltpu.roll(c, KY - 1, 1), 0.0)
                 + jnp.where(q_at > 0, pltpu.roll(c, 1, 1), 0.0)
                 + pltpu.roll(c, 127, 2) + pltpu.roll(c, 1, 2))
        return jnp.where(r_at < KZ, total - 6.0 * c, 0.0)

    clane[...] = jnp.zeros(clane.shape, f32)
    for a in range(3):
        clane[:, :, 0:KZ] = cc_ref[a]
        cbend[a] = BEND * laplace(laplace(clane[...]))

    all_shares = crest.at[pl.ds(0, len(reach))]
    whole(0, all_shares, n_sem.at[0], n_sem.at[1]).wait_recv()
    total = crecv[4]
    for n, (d, e) in enumerate(columns):
        if n != 4:
            total = total + jnp.where(inside((d, e, 1)), crecv[n], 0.0)
    sub, at = iota((nz, 128), 0), iota((nz, 128), 1) % 32
    keep = (at >= 4 * sub - 2) & (at < 4 * sub + 6) & (at < KZ)
    for a in range(3):
        value = None
        for n in range(nz):
            shift = (4 * n - 2 - 8 * a) % 128
            moved = pltpu.roll(total, shift, 1) if shift else total
            value = moved if n == 0 else jnp.where(sub == n, moved, value)
        xrow[me[0], a, pl.ds(me[1], 1), :] = jnp.sum(
            jnp.where(keep, value, 0.0), axis=0, keepdims=True)
    coarse_start(1)

    fine_whole(2).wait_recv()
    for half in range(2):
        for a in range(3):
            part = slice(2 * a, 2 * a + 2)
            tz_v[half, a, 0:2, :] = tz_v[half, a, 0:2, :] + zgot[0, half, part, :] * gate[2][0]
            tz_v[half, a, PZ - 2:PZ, :] = (
                tz_v[half, a, PZ - 2:PZ, :] + zgot[1, half, part, :] * gate[2][1])
            a_v[half, a * PZ:(a + 1) * PZ, :] = tz_v[half, a, 0:PZ, :]
    fine_start(1)

    coarse_whole(1).wait_recv()
    coarse_start(0)

    fine_whole(1).wait_recv()
    shape = (EX * PY, EX * PY)
    rows, cols = iota(shape, 0), iota(shape, 1)
    p_same = rows // PY == cols // PY
    q, r = rows % PY, cols % PY
    low = jnp.where(p_same & (q == r + 2) & (r < 2), 1.0, 0.0)
    high = jnp.where(p_same & (q == r - (PY - 2)) & (r >= PY - 2), 1.0, 0.0)
    b_v[...] = (a_v[0] + nn(agot[0] * gate[1][0], low) + nn(agot[1] * gate[1][1], high))
    fine_start(0)

    fine_whole(0).wait_recv()
    shape = (PX * PY, EX * PY)
    rows, cols = iota(shape, 0), iota(shape, 1)
    own = jnp.where(cols == rows + 2 * PY, 1.0, 0.0)
    low = jnp.where((cols == rows + (PX + 2) * PY) & (rows < 2 * PY), gate[0][0], 0.0)
    high = jnp.where((cols == rows - (PX - 2) * PY) & (rows >= (PX - 2) * PY), gate[0][1], 0.0)
    for a in range(3):
        part = slice(a * PZ, (a + 1) * PZ)
        out = nt(own, b_v[part]) + nt(low, bgot[0, part]) + nt(high, bgot[1, part])
        fo_ref[a] = out.reshape(PX, PY, PZ)

    for k, got in enumerate((xrecv, yrecv, zrecv)):
        whole(k, got, hs_sem.at[k], hr_sem.at[k]).wait_send()
        fine_whole(k).wait_send()
        if k < 2:
            coarse_whole(k).wait_send()
    whole(0, all_shares, n_sem.at[0], n_sem.at[1]).wait_send()

    coarse_whole(0).wait_recv()
    for i in range(nx):
        for a in range(3):
            block = xrow[i, a]
            for g in range(4):
                value = block if g == 0 else pltpu.roll(block, 128 - 32 * g, 1)
                p = 2 * i + g // 2
                part = pl.ds(g % 2, ny, stride=2)
                co_ref[a, p, part, :] = (value + cbend[a, p, part, :])[:, 0:KZ]


def solution(mesh):
    sizes = tuple(mesh.shape[a] for a in ("gx", "gy", "gz"))

    def step(warped, fixed, fine, coarse):
        SX, SY, SZ = warped.shape
        PX, PY, PZ = SX // SPF, SY // SPF, SZ // SPF
        KX, KY, KZ = coarse.shape[1:]
        EX, QE, RZ = PX + 4, 2 * PY, PZ + 8
        CR = 48
        KC = SPF * SY
        vmem = pl.BlockSpec(memory_space=pltpu.VMEM)
        hbm = pl.BlockSpec(memory_space=pltpu.HBM)
        V = pltpu.VMEM
        D = pltpu.SemaphoreType.DMA
        return pl.pallas_call(
            functools.partial(kernel, sizes),
            out_shape=(V(fine.shape, f32), V(coarse.shape, f32)),
            in_specs=[hbm] * 4,
            out_specs=(vmem, vmem),
            scratch_shapes=[
                V((SX, SY, SZ), f32), V((SX, SY, SZ), f32),
                V((3, PX, PY, PZ), f32), V(coarse.shape, f32),
                V((SX + 4, SY + 16, SZ), f32), V((2, 2, SY, SZ), f32),
                V((2, 2 * SX, SZ), f32), V((2, 2 * SX, SZ), f32), V((2, 2 * SX, SZ), f32),
                V((2, SY, SZ), f32), V((2, SY, SZ), f32), V((2, SY, SZ), f32),
                V((2, 5 * QE, KC), bf16), V((SX // SPF, 2, CR, KC), bf16),
                V((2, EX * QE + CR, 4 * SX), bf16), V((4 * SX, 128), f32), V((SZ, 128), f32),
                V((2 * SZ, 2 * SZ), bf16),
                V((SX // SPF, KC, SZ), f32), V((2, 2, SY, SZ), f32),
                V((2, EX, PY, 3 * SZ), f32), V((CR, 3 * SZ), f32),
                V((2, 3, RZ, EX * PY), f32),
                V((KX, KY, 128), f32), V((3, KX, KY, 128), f32),
                V((2, 2, 8, EX * PY), f32), V((2, 2, 8, EX * PY), f32),
                V((2, 3 * PZ, EX * PY), f32), V((2, 3 * PZ, EX * PY), f32),
                V((3 * PZ, EX * PY), f32), V((2, 3 * PZ, EX * PY), f32),
                V((9, 1, 128), f32), V((9, sizes[2], 128), f32),
                V((9 * sizes[2], 128), f32), V((sizes[0], 3, sizes[1], 128), f32),
                D((SX // SPF,)), D((2,)), D((3,)), D((3,)),
                D((3,)), D((3,)), D((2,)), D((2,)), D((2,)), pltpu.SemaphoreType.REGULAR,
            ],
            compiler_params=pltpu.CompilerParams(
                collective_id=0, has_side_effects=True, vmem_limit_bytes=66000000
            ),
        )(warped, fixed, fine, coarse)

    in_specs = (P("gx", "gy", "gz"), P("gx", "gy", "gz"), P(None, "gx", "gy", "gz"), P())
    out_specs = (P(None, "gx", "gy", "gz"), P())
    return jax.shard_map(
        step, mesh=mesh, in_specs=in_specs, out_specs=out_specs, check_vma=False
    )
```

```python
import functools

import jax
import jax.numpy as jnp
from jax import lax
from jax.experimental import pallas as pl
from jax.experimental.pallas import tpu as pltpu
from jax.sharding import PartitionSpec as P

SPF = 8
SPC = 32
BEND = 0.01
HI = lax.Precision.HIGHEST
MESH = pl.DeviceIdType.MESH
f32 = jnp.float32
bf16 = jnp.bfloat16


def nn(a, b):
    return lax.dot_general(
        a, b, (((1,), (0,)), ((), ())), precision=HI, preferred_element_type=f32
    )


def nt(a, b):
    return lax.dot_general(
        a, b, (((1,), (1,)), ((), ())), precision=HI, preferred_element_type=f32
    )


def spline(t):
    m = jnp.abs(t)
    inner = 2.0 / 3.0 - m * m + 0.5 * m * m * m
    r = 2.0 - m
    outer = r * r * r * (1.0 / 6.0)
    return jnp.where(m < 1.0, inner, jnp.where(m < 2.0, outer, 0.0))


def weight(voxel, point, spacing):
    scaled = (2 * voxel + 1 - spacing * (2 * point + 1)).astype(f32)
    return spline(scaled * (0.5 / spacing))


def iota(shape, axis):
    return lax.broadcasted_iota(jnp.int32, shape, axis)


def diff1(out, inp):
    d = jnp.abs(out - inp)
    return jnp.where(d == 0, -2.0, jnp.where(d == 1, 1.0, 0.0)).astype(f32)


def diff2(out, inp, count):
    d = jnp.abs(out - inp)
    edge = (inp == 0) | (inp == count - 1)
    centre = jnp.where(edge, 5.0, 6.0)
    return jnp.where(
        d == 0, centre, jnp.where(d == 1, -4.0, jnp.where(d == 2, 1.0, 0.0))
    ).astype(f32)


def same(out, inp):
    return jnp.where(out == inp, 1.0, 0.0).astype(f32)


def bend_planes(px, py, qx, qy, cx, cy):
    jx, jy = same(px, qx), same(py, qy)
    tx, ty = diff1(px, qx), diff1(py, qy)
    m0 = diff2(px, qx, cx) * jy + jx * diff2(py, qy, cy) + 2.0 * tx * ty
    m1 = 2.0 * (tx * jy + jx * ty)
    return m0 * BEND, m1 * BEND, jx * jy * BEND


def kernel(sizes, w_hbm, f_hbm, fc_hbm, cc_hbm, fo_ref, co_ref,
           w_v, f_v, fc_ref, cc_ref, s_v, xrecv, ysend, yrecv, yd, zsend, zrecv, zd,
           wf_v, wc_v, wy_v, wxe_v, bzc_v, pz_v, gz_v, zp_v,
           accf, accc, tz_v, clane, cbend, zmsg, zgot, a_v, agot, b_v, bgot,
           cmsg, crecv, crest, xrow, load_sem, small_sem, hs_sem, hr_sem,
           ms_sem, mr_sem, n_sem, cs_sem, cr_sem, ready):
    nx, ny, nz = sizes
    axes = ("gx", "gy", "gz")
    counts = sizes
    me = [lax.axis_index(a) for a in axes]
    SX, SY, SZ = w_v.shape
    PX, PY, PZ = SX // SPF, SY // SPF, SZ // SPF
    KX, KY, KZ = cc_ref.shape[1:]
    EX, QE = PX + 4, 2 * PY
    CR = accc.shape[0]
    CQ, CX = 8, CR // 8
    RZ = tz_v.shape[2]
    KC = SPF * SY
    cells = SX // SPF
    lanes = 3 * SZ

    for c in range(cells):
        part = pl.ds(c * SPF, SPF)
        pltpu.make_async_copy(w_hbm.at[part], w_v.at[part], load_sem.at[c]).start()
        pltpu.make_async_copy(f_hbm.at[part], f_v.at[part], load_sem.at[c]).start()
    small = (pltpu.make_async_copy(fc_hbm, fc_ref, small_sem.at[0]),
             pltpu.make_async_copy(cc_hbm, cc_ref, small_sem.at[1]))
    for copy in small:
        copy.start()

    def load_wait(c):
        both = pl.ds(0, 2 * SPF)
        pltpu.make_async_copy(w_hbm.at[both], w_v.at[both], load_sem.at[c]).wait()

    has = [(me[k] > 0, me[k] < counts[k] - 1) for k in range(3)]

    def toward(step):
        return {axes[k]: lax.rem(me[k] + (counts[k] + step[k] - 1), counts[k])
                for k in range(3) if step[k] != 1}

    def inside(step):
        ok = None
        for k in range(3):
            if step[k] != 1:
                here = has[k][0] if step[k] == 0 else has[k][1]
                ok = here if ok is None else ok & here
        return ok

    def far_first(n):
        return sorted(range(1, n), key=lambda d: -min(d, n - d))

    columns = [(d, e) for d in range(3) for e in range(3)]
    reach = [(n, dz) for dz in far_first(nz) + [0] for n in range(9) if (n, dz) != (4, 0)]

    def column(n, dz):
        there = toward(columns[n] + (1,))
        if dz:
            there[axes[2]] = lax.rem(me[2] + dz, nz)
        return there

    barrier = pltpu.get_barrier_semaphore()
    total = 0
    for k in (2, 1, 0):
        for d in far_first(counts[k]):
            pl.semaphore_signal(
                barrier, inc=1, device_id={axes[k]: lax.rem(me[k] + d, counts[k])},
                device_id_type=MESH
            )
            total += 1
    around = [n for n in range(9) if n != 4]
    for n in around:
        if n % 2 == 0:
            pl.semaphore_signal(barrier, inc=1, device_id=column(n, 0), device_id_type=MESH)
            total += 1

    zero_plane = jnp.zeros((2, SY, SZ), f32)
    s_v[0:2, 8:8 + SY, :] = zero_plane
    s_v[SX + 2:SX + 4, 8:8 + SY, :] = zero_plane
    zero_rows = jnp.zeros((SX, 2, SZ), f32)
    s_v[2:SX + 2, 6:8, :] = zero_rows
    s_v[2:SX + 2, 8 + SY:10 + SY, :] = zero_rows

    row, col = iota((2 * SZ, 2 * SZ), 0) % SZ, iota((2 * SZ, 2 * SZ), 1)
    away = row - col
    slope = jnp.where(away == 1, 8.0, jnp.where(away == -1, -8.0, jnp.where(
        away == -2, 1.0, jnp.where(away == 2, -1.0, 0.0))))
    pick = jnp.where(row == (col % 4 + SZ - 2) % SZ, 1.0, 0.0)
    pz_v[...] = jnp.where(col < SZ, slope, pick).astype(bf16)
    def split_store(ref, index, value):
        high = value.astype(bf16)
        ref[index + (0,)] = high
        ref[index + (1,)] = (value - high.astype(f32)).astype(bf16)

    def ext_q(q):
        return jnp.where(q < PY, q, jnp.where(q < PY + 2, q - PY - 2, q - 2))

    def outer(along_x, along_y):
        return jnp.concatenate([along_x[p:p + 1] * along_y for p in range(along_x.shape[0])], axis=0)

    col = iota((8, KC), 1)
    col2 = iota((QE, KC), 1)
    split_store(wf_v, (), outer(weight(col // SY, iota((8, KC), 0) - 2, SPF)[0:5],
                                weight(col2 % SY, ext_q(iota((QE, KC), 0)), SPF)))
    along_y = weight(col % SY, iota((8, KC), 0) - 2, SPC)
    for c in range(cells):
        split_store(wc_v, (c,), outer(
            weight(col // SY + c * SPF, iota((8, KC), 0) - 2, SPC)[0:CX], along_y))
    col, row = iota((QE, 4 * SX), 1), iota((QE, 4 * SX), 0)
    face_x, face_y = (col % (2 * SX)) // 2, col % 2 + (SY - 2) * (col // (2 * SX))
    along_x = weight(face_x, row - 2, SPF)[0:EX]
    along_y = weight(face_y, ext_q(row), SPF)
    split_store(wy_v, (), jnp.concatenate([
        outer(along_x, along_y[0:PY]), outer(along_x, along_y[PY:QE]),
        outer(weight(face_x, row - 2, SPC)[0:CX], weight(face_y, row - 2, SPC)[0:CQ])], axis=0))
    row, col = iota((4 * SX, 128), 0), iota((4 * SX, 128), 1)
    face_x = (row % (2 * SX)) // 4 + jnp.where(row % 4 < 2, SX // 2, 0)
    place = row % 2 + 2 - 2 * (row // (2 * SX))
    wxe_v[...] = jnp.where(col % 4 == place, jnp.where(
        col < 64, weight(face_x, col // 4 - 2, SPF), weight(face_x, col // 4 - 18, SPC)), 0.0)
    rows, cols = iota((SZ, 128), 0), iota((SZ, 128), 1)
    bzc_v[...] = weight(rows, cols % 8 - 2, SPC) * (SPC ** -1.5 / 24.0)
    accf[...] = jnp.zeros(accf.shape, f32)
    accc[...] = jnp.zeros(accc.shape, f32)

    lane = iota((SY, SZ), 1)
    half_x = SX // 2

    def split(value):
        high = value.astype(bf16)
        return high, (value - high.astype(f32)).astype(bf16)

    def face_rows(c):
        for x in range(c * SPF, (c + 1) * SPF):
            for side, part in ((0, slice(0, 8)), (1, slice(SY - 8, SY))):
                w, f = w_v[x, part, :], f_v[x, part, :]
                rows = slice(6 * side, 6 * side + 2)
                ysend[side, 2 * x:2 * x + 2, :] = (w + f)[rows]
                yd[side, 2 * x:2 * x + 2, :] = (w - f)[rows]

    outer_planes = (0, 1, SX - 2, SX - 1)

    def sums(c):
        wide = ([], [])
        for x in range(c * SPF, (c + 1) * SPF):
            w, f = w_v[x], f_v[x]
            s, d = w + f, w - f
            if x not in outer_planes:
                s_v[x + 2, 8:8 + SY, :] = s
            w_v[x] = d
            for n, value in enumerate((s, d)):
                wide[n].append(jnp.concatenate(split(value), axis=1))
        out = jnp.dot(jnp.concatenate(wide[0], axis=0), pz_v[...], preferred_element_type=f32)
        gz_v[c] = out[:, 0:SZ]
        picked = (out[:, SZ:2 * SZ],
                  jnp.dot(jnp.concatenate(wide[1], axis=0), pz_v[:, SZ:2 * SZ], preferred_element_type=f32))
        tile = c * SPF // half_x
        for n in range(2):
            pack = None if c * SPF % half_x == 0 else zp_v[n, tile]
            for xx in range(SPF):
                value = picked[n][xx * SY:(xx + 1) * SY]
                here = lane // 4 == (c * SPF + xx) % half_x
                pack = value if pack is None else jnp.where(here, value, pack)
            zp_v[n, tile] = pack
    half = cells // 2
    for c in range(cells):
        load_wait(c)
        face_rows(c)
        for x in outer_planes:
            if x // SPF == c:
                s_v[x + 2, 8:8 + SY, :] = w_v[x] + f_v[x]
        if c < half:
            sums(c)

    pl.semaphore_wait(barrier, total)
    for n in around:
        pl.semaphore_signal(ready, inc=1, device_id=column(n, 0), device_id_type=MESH)

    def neighbour_copy(k, side, src, dst, send, recv):
        step = [1, 1, 1]
        step[k] = 2 * side
        return pltpu.make_async_remote_copy(
            src_ref=src, dst_ref=dst, send_sem=send, recv_sem=recv,
            device_id=toward(step), device_id_type=MESH,
        )

    def halo(k, side):
        if k == 0:
            src = s_v.at[pl.ds(2 if side == 0 else SX, 2), pl.ds(8, SY), :]
        else:
            src = (ysend if k == 1 else zsend).at[side]
        return neighbour_copy(k, side, src, (xrecv, yrecv, zrecv)[k].at[1 - side],
                              hs_sem.at[k], hr_sem.at[k])

    def whole(k, ref, send, recv):
        return neighbour_copy(k, 0, ref, ref, send, recv)

    for k in (1, 0):
        for side in range(2):
            halo(k, side).start()

    for c in range(half, cells):
        sums(c)
    upper = lane % 4 >= 2
    for n, ref in enumerate((zsend, zd)):
        ref[0] = jnp.where(upper, zp_v[n, 0], pltpu.roll(zp_v[n, 1], SZ - 2, 1))
        ref[1] = jnp.where(upper, pltpu.roll(zp_v[n, 0], 2, 1), zp_v[n, 1])

    for side in range(2):
        halo(2, side).start()

    def forces(i):
        T = 16
        tiles = {}
        for r in range(0, SY, T):
            at = 8 + r
            near = [s_v[i * SPF + n, at:at + T, :] for n in range(4)]
            for xx in range(SPF):
                x = i * SPF + xx
                near.append(s_v[x + 4, at:at + T, :])
                d = w_v[x, r:r + T, :]
                gx = near[0] - near[4] + 8.0 * (near[3] - near[1])
                near.pop(0)
                gy = (s_v[x + 2, at - 2:at - 2 + T, :] - s_v[x + 2, at + 2:at + 2 + T, :]
                      + 8.0 * (s_v[x + 2, at + 1:at + 1 + T, :] - s_v[x + 2, at - 1:at - 1 + T, :]))
                row = xx * SY + r
                gz = gz_v[i, row:row + T, :]
                tiles[row] = [split(g * d) for g in (gx, gy, gz)]
        return [jnp.concatenate([
            jnp.concatenate([tiles[row][a][n] for row in sorted(tiles)], axis=0)
            for a in range(3)], axis=1) for n in range(2)]

    def cell_weights(i):
        return jnp.concatenate([wf_v[0], wc_v[i, 0], wf_v[1], wc_v[i, 1]], axis=0)

    def project(weights, high, low):
        many = weights.shape[0] // 2
        both = jnp.dot(weights, high, preferred_element_type=f32)
        return both[:many] + both[many:] + jnp.dot(
            weights[:many], low, preferred_element_type=f32)

    def collect(i, out, part):
        fine = out[:5 * QE].reshape(5, 2, PY, out.shape[1])
        accf[0, i:i + 5, :, part] += fine[:, 0]
        accf[1, i:i + 5, :, part] += fine[:, 1]
        accc[:, part] += out[5 * QE:]

    for i in range(cells):
        collect(i, project(cell_weights(i), *forces(i)), slice(0, lanes))

    for k, got in enumerate((xrecv, yrecv, zrecv)):
        whole(k, got, hs_sem.at[k], hr_sem.at[k]).wait_recv()

    gate = [[jnp.where(h, 1.0, 0.0) for h in pair] for pair in has]

    def diff(x):
        return w_v[x]

    for side, i in ((0, 0), (1, cells - 1)):
        r0, r1 = xrecv[side, 0] * gate[0][side], xrecv[side, 1] * gate[0][side]
        if side == 0:
            face = jnp.concatenate([(r0 - 8.0 * r1) * diff(0), r1 * diff(1)], axis=0)
            part = slice(0, 2 * SY)
        else:
            face = jnp.concatenate([-r0 * diff(SX - 2), (8.0 * r0 - r1) * diff(SX - 1)], axis=0)
            part = slice(KC - 2 * SY, KC)
        collect(i, project(cell_weights(i)[:, part], *split(face)), slice(0, SZ))

    rows = iota((SX // 4, 8, SZ), 1) % 2 == 0
    r = (yrecv[0] * gate[1][0]).reshape(SX // 4, 8, SZ)
    low = jnp.where(rows, r - 8.0 * pltpu.roll(r, 7, 1), r).reshape(2 * SX, SZ) * yd[0]
    r = (yrecv[1] * gate[1][1]).reshape(SX // 4, 8, SZ)
    high = jnp.where(rows, -r, 8.0 * pltpu.roll(r, 1, 1) - r).reshape(2 * SX, SZ) * yd[1]
    out = project(jnp.concatenate([wy_v[0], wy_v[1]], axis=0),
                  *split(jnp.concatenate([low, high], axis=0)))
    for half in range(2):
        accf[half, :, :, SZ:2 * SZ] += out[half * EX * PY:(half + 1) * EX * PY].reshape(EX, PY, SZ)
    accc[:, SZ:2 * SZ] += out[2 * EX * PY:]

    even = lane % 2 == 0
    dl = zrecv[0] * gate[2][0]
    dh = zrecv[1] * gate[2][1]
    low = jnp.where(even, dl - 8.0 * pltpu.roll(dl, SZ - 1, 1), dl) * zd[0]
    high = jnp.where(even, -dh, 8.0 * pltpu.roll(dh, 1, 1) - dh) * zd[1]
    row, col = iota((QE + CQ, SY), 0), iota((QE + CQ, SY), 1)
    along_y = jnp.where(row < QE, weight(col, ext_q(row), SPF), weight(col, row - QE - 2, SPC))
    out = nn(nn(along_y, jnp.concatenate([low, high], axis=1)), wxe_v[...])
    at = iota((PY, SZ), 1)
    edge = (at < 2) | (at >= SZ - 2)

    def spread(half, shift):
        return jnp.where(edge, pltpu.roll(out[half * PY:(half + 1) * PY], shift % 128, 1), 0.0)

    for p in range(EX):
        for half in range(2):
            accf[half, p, :, 2 * SZ:3 * SZ] += spread(half, 254 - 4 * p)
    for p in range(CX):
        accc[p * CQ:(p + 1) * CQ, 2 * SZ:3 * SZ] += spread(2, 254 - 64 - 4 * p)

    stack = jnp.concatenate([accc[:, a * SZ:(a + 1) * SZ] for a in range(3)], axis=0)
    shares = nn(stack, bzc_v[...])
    rows, cols = iota((CR, 128), 0), iota((CR, 128), 1)
    keep = (cols // 32 == 2 * ((rows // CQ) % 2) + rows % 2) & (cols % 32 < 24)
    value = jnp.where(cols % 32 < 8, shares[0:CR],
                      jnp.where(cols % 32 < 16, shares[CR:2 * CR], shares[2 * CR:3 * CR]))
    value = jnp.where(keep, value, 0.0).reshape(3, 2, CQ, 128)
    value = value[:, 0] + value[:, 1]
    value = value + pltpu.roll(value, 7, 1)
    for n, (d, e) in enumerate(columns):
        cmsg[n] = value[d, 2 * e:2 * e + 1, :]
    mine = pl.ds(me[2], 1)
    crecv[4, mine, :] = value[1, 2:3, :]
    pl.semaphore_wait(ready, len(around))
    for n, dz in reach:
        pltpu.make_async_remote_copy(
            src_ref=cmsg.at[n], dst_ref=crecv.at[8 - n, mine, :],
            send_sem=n_sem.at[0], recv_sem=n_sem.at[1],
            device_id=column(n, dz), device_id_type=MESH,
        ).start()

    rows, cols = iota((RZ, SZ), 0), iota((RZ, SZ), 1)

    def ext_point(row):
        return jnp.where(row < PZ, row, jnp.where(row < PZ + 2, row - PZ - 2, row - 2))

    bz = weight(cols, ext_point(rows), SPF) * (SPF ** -1.5 / 24.0)
    for a in range(3):
        for half in range(2):
            block = accf[half, :, :, a * SZ:(a + 1) * SZ].reshape(EX * PY, SZ)
            tz_v[half, a] = nt(bz, block)

    for copy in small:
        copy.wait()
    shape = (PX * PY, EX * QE)
    rows, cols = iota(shape, 0), iota(shape, 1)
    ox, oy, oz = me[0] * PX, me[1] * PY, me[2] * PZ
    wide, inner = cols // (EX * PY), cols % (EX * PY)
    planes = bend_planes(inner // PY - 2 + ox, ext_q(inner % PY + PY * wide) + oy,
                         rows // PY + ox, rows % PY + oy, PX * nx, PY * ny)
    zr, zc = ext_point(iota((RZ, PZ), 0)) + oz, iota((RZ, PZ), 1) + oz
    along = jnp.concatenate([same(zr, zc), diff1(zr, zc), diff2(zr, zc, PZ * nz)], axis=0)
    turned = nt(along, fc_ref[...].reshape(3 * PX * PY, PZ))
    turned = jnp.concatenate([jnp.concatenate([
        turned[k * RZ:(k + 1) * RZ, a * PX * PY:(a + 1) * PX * PY] for k in range(3)], axis=1)
        for a in range(3)], axis=0)
    bent = nn(turned, jnp.concatenate(planes, axis=0))
    for a in range(3):
        for half in range(2):
            tz_v[half, a] += bent[a * RZ:(a + 1) * RZ, half * EX * PY:(half + 1) * EX * PY]
            for side in range(2):
                zmsg[side, half, 2 * a:2 * a + 2, :] = tz_v[
                    half, a, PZ + 2 * side:PZ + 2 * side + 2, :]

    def fine_start(k):
        for side in range(2):
            source = (b_v, a_v.at[1], zmsg.at[side])[k]
            neighbour_copy(k, side, source, (bgot, agot, zgot)[k].at[1 - side],
                           ms_sem.at[k], mr_sem.at[k]).start()

    def fine_whole(k):
        return whole(k, (bgot, agot, zgot)[k], ms_sem.at[k], mr_sem.at[k])

    def coarse_slot(k, n):
        if k == 0:
            return xrow.at[n]
        return xrow.at[me[0], :, pl.ds(n, 1), :]

    def coarse_start(k):
        for d in far_first(counts[k]):
            pltpu.make_async_remote_copy(
                src_ref=coarse_slot(k, me[k]), dst_ref=coarse_slot(k, me[k]),
                send_sem=cs_sem.at[k], recv_sem=cr_sem.at[k],
                device_id={axes[k]: lax.rem(me[k] + d, counts[k])}, device_id_type=MESH,
            ).start()

    def coarse_whole(k):
        part = pl.ds(0, counts[k] - 1)
        ref = (xrow.at[part], xrow.at[me[0], :, part, :])[k]
        return whole(k, ref, cs_sem.at[k], cr_sem.at[k])

    fine_start(2)

    q_at, r_at = iota((KX, KY, 128), 1), iota((KX, KY, 128), 2)

    def laplace(c):
        zero = jnp.zeros((1, KY, 128), f32)
        total = (jnp.concatenate([c[1:], zero], axis=0) + jnp.concatenate([zero, c[:-1]], axis=0)
                 + jnp.where(q_at < KY - 1, pltpu.roll(c, KY - 1, 1), 0.0)
                 + jnp.where(q_at > 0, pltpu.roll(c, 1, 1), 0.0)
                 + pltpu.roll(c, 127, 2) + pltpu.roll(c, 1, 2))
        return jnp.where(r_at < KZ, total - 6.0 * c, 0.0)

    clane[...] = jnp.zeros(clane.shape, f32)
    for a in range(3):
        clane[:, :, 0:KZ] = cc_ref[a]
        cbend[a] = BEND * laplace(laplace(clane[...]))

    all_shares = crest.at[pl.ds(0, len(reach))]
    whole(0, all_shares, n_sem.at[0], n_sem.at[1]).wait_recv()
    total = crecv[4]
    for n, (d, e) in enumerate(columns):
        if n != 4:
            total = total + jnp.where(inside((d, e, 1)), crecv[n], 0.0)
    sub, at = iota((nz, 128), 0), iota((nz, 128), 1) % 32
    keep = (at >= 4 * sub - 2) & (at < 4 * sub + 6) & (at < KZ)
    for a in range(3):
        value = None
        for n in range(nz):
            shift = (4 * n - 2 - 8 * a) % 128
            moved = pltpu.roll(total, shift, 1) if shift else total
            value = moved if n == 0 else jnp.where(sub == n, moved, value)
        xrow[me[0], a, pl.ds(me[1], 1), :] = jnp.sum(
            jnp.where(keep, value, 0.0), axis=0, keepdims=True)
    coarse_start(1)

    fine_whole(2).wait_recv()
    for half in range(2):
        for a in range(3):
            part = slice(2 * a, 2 * a + 2)
            tz_v[half, a, 0:2, :] = tz_v[half, a, 0:2, :] + zgot[0, half, part, :] * gate[2][0]
            tz_v[half, a, PZ - 2:PZ, :] = (
                tz_v[half, a, PZ - 2:PZ, :] + zgot[1, half, part, :] * gate[2][1])
            a_v[half, a * PZ:(a + 1) * PZ, :] = tz_v[half, a, 0:PZ, :]
    fine_start(1)

    coarse_whole(1).wait_recv()
    coarse_start(0)

    fine_whole(1).wait_recv()
    shape = (EX * PY, EX * PY)
    rows, cols = iota(shape, 0), iota(shape, 1)
    p_same = rows // PY == cols // PY
    q, r = rows % PY, cols % PY
    low = jnp.where(p_same & (q == r + 2) & (r < 2), 1.0, 0.0)
    high = jnp.where(p_same & (q == r - (PY - 2)) & (r >= PY - 2), 1.0, 0.0)
    b_v[...] = (a_v[0] + nn(agot[0] * gate[1][0], low) + nn(agot[1] * gate[1][1], high))
    fine_start(0)

    fine_whole(0).wait_recv()
    shape = (PX * PY, EX * PY)
    rows, cols = iota(shape, 0), iota(shape, 1)
    own = jnp.where(cols == rows + 2 * PY, 1.0, 0.0)
    low = jnp.where((cols == rows + (PX + 2) * PY) & (rows < 2 * PY), gate[0][0], 0.0)
    high = jnp.where((cols == rows - (PX - 2) * PY) & (rows >= (PX - 2) * PY), gate[0][1], 0.0)
    for a in range(3):
        part = slice(a * PZ, (a + 1) * PZ)
        out = nt(own, b_v[part]) + nt(low, bgot[0, part]) + nt(high, bgot[1, part])
        fo_ref[a] = out.reshape(PX, PY, PZ)

    for k, got in enumerate((xrecv, yrecv, zrecv)):
        whole(k, got, hs_sem.at[k], hr_sem.at[k]).wait_send()
        fine_whole(k).wait_send()
        if k < 2:
            coarse_whole(k).wait_send()
    whole(0, all_shares, n_sem.at[0], n_sem.at[1]).wait_send()

    coarse_whole(0).wait_recv()
    for i in range(nx):
        for a in range(3):
            block = xrow[i, a]
            for g in range(4):
                value = block if g == 0 else pltpu.roll(block, 128 - 32 * g, 1)
                p = 2 * i + g // 2
                part = pl.ds(g % 2, ny, stride=2)
                co_ref[a, p, part, :] = (value + cbend[a, p, part, :])[:, 0:KZ]


def solution(mesh):
    sizes = tuple(mesh.shape[a] for a in ("gx", "gy", "gz"))

    def step(warped, fixed, fine, coarse):
        SX, SY, SZ = warped.shape
        PX, PY, PZ = SX // SPF, SY // SPF, SZ // SPF
        KX, KY, KZ = coarse.shape[1:]
        EX, QE, RZ = PX + 4, 2 * PY, PZ + 8
        CR = 48
        KC = SPF * SY
        vmem = pl.BlockSpec(memory_space=pltpu.VMEM)
        hbm = pl.BlockSpec(memory_space=pltpu.HBM)
        V = pltpu.VMEM
        D = pltpu.SemaphoreType.DMA
        return pl.pallas_call(
            functools.partial(kernel, sizes),
            out_shape=(V(fine.shape, f32), V(coarse.shape, f32)),
            in_specs=[hbm] * 4,
            out_specs=(vmem, vmem),
            scratch_shapes=[
                V((SX, SY, SZ), f32), V((SX, SY, SZ), f32),
                V((3, PX, PY, PZ), f32), V(coarse.shape, f32),
                V((SX + 4, SY + 16, SZ), f32), V((2, 2, SY, SZ), f32),
                V((2, 2 * SX, SZ), f32), V((2, 2 * SX, SZ), f32), V((2, 2 * SX, SZ), f32),
                V((2, SY, SZ), f32), V((2, SY, SZ), f32), V((2, SY, SZ), f32),
                V((2, 5 * QE, KC), bf16), V((SX // SPF, 2, CR, KC), bf16),
                V((2, EX * QE + CR, 4 * SX), bf16), V((4 * SX, 128), f32), V((SZ, 128), f32),
                V((2 * SZ, 2 * SZ), bf16),
                V((SX // SPF, KC, SZ), f32), V((2, 2, SY, SZ), f32),
                V((2, EX, PY, 3 * SZ), f32), V((CR, 3 * SZ), f32),
                V((2, 3, RZ, EX * PY), f32),
                V((KX, KY, 128), f32), V((3, KX, KY, 128), f32),
                V((2, 2, 8, EX * PY), f32), V((2, 2, 8, EX * PY), f32),
                V((2, 3 * PZ, EX * PY), f32), V((2, 3 * PZ, EX * PY), f32),
                V((3 * PZ, EX * PY), f32), V((2, 3 * PZ, EX * PY), f32),
                V((9, 1, 128), f32), V((9, sizes[2], 128), f32),
                V((9 * sizes[2], 128), f32), V((sizes[0], 3, sizes[1], 128), f32),
                D((SX // SPF,)), D((2,)), D((3,)), D((3,)),
                D((3,)), D((3,)), D((2,)), D((2,)), D((2,)), pltpu.SemaphoreType.REGULAR,
            ],
            compiler_params=pltpu.CompilerParams(
                collective_id=0, has_side_effects=True, vmem_limit_bytes=66000000
            ),
        )(warped, fixed, fine, coarse)

    in_specs = (P("gx", "gy", "gz"), P("gx", "gy", "gz"), P(None, "gx", "gy", "gz"), P())
    out_specs = (P(None, "gx", "gy", "gz"), P())
    return jax.shard_map(
        step, mesh=mesh, in_specs=in_specs, out_specs=out_specs, check_vma=False
    )
```

```python
import functools

import jax
import jax.numpy as jnp
from jax import lax
from jax.experimental import pallas as pl
from jax.experimental.pallas import tpu as pltpu
from jax.sharding import PartitionSpec as P

SPF = 8
SPC = 32
BEND = 0.01
HI = lax.Precision.HIGHEST
MESH = pl.DeviceIdType.MESH
f32 = jnp.float32
bf16 = jnp.bfloat16


def nn(a, b):
    return lax.dot_general(
        a, b, (((1,), (0,)), ((), ())), precision=HI, preferred_element_type=f32
    )


def nt(a, b):
    return lax.dot_general(
        a, b, (((1,), (1,)), ((), ())), precision=HI, preferred_element_type=f32
    )


def spline(t):
    m = jnp.abs(t)
    inner = 2.0 / 3.0 - m * m + 0.5 * m * m * m
    r = 2.0 - m
    outer = r * r * r * (1.0 / 6.0)
    return jnp.where(m < 1.0, inner, jnp.where(m < 2.0, outer, 0.0))


def weight(voxel, point, spacing):
    scaled = (2 * voxel + 1 - spacing * (2 * point + 1)).astype(f32)
    return spline(scaled * (0.5 / spacing))


def iota(shape, axis):
    return lax.broadcasted_iota(jnp.int32, shape, axis)


def diff1(out, inp):
    d = jnp.abs(out - inp)
    return jnp.where(d == 0, -2.0, jnp.where(d == 1, 1.0, 0.0)).astype(f32)


def diff2(out, inp, count):
    d = jnp.abs(out - inp)
    edge = (inp == 0) | (inp == count - 1)
    centre = jnp.where(edge, 5.0, 6.0)
    return jnp.where(
        d == 0, centre, jnp.where(d == 1, -4.0, jnp.where(d == 2, 1.0, 0.0))
    ).astype(f32)


def same(out, inp):
    return jnp.where(out == inp, 1.0, 0.0).astype(f32)


def bend_planes(px, py, qx, qy, cx, cy):
    jx, jy = same(px, qx), same(py, qy)
    tx, ty = diff1(px, qx), diff1(py, qy)
    m0 = diff2(px, qx, cx) * jy + jx * diff2(py, qy, cy) + 2.0 * tx * ty
    m1 = 2.0 * (tx * jy + jx * ty)
    return m0 * BEND, m1 * BEND, jx * jy * BEND


def kernel(sizes, w_hbm, f_hbm, fc_hbm, cc_hbm, fo_ref, co_ref,
           w_v, f_v, fc_ref, cc_ref, s_v, xrecv, ysend, yrecv, yd, zsend, zrecv, zd,
           wf_v, wc_v, wy_v, wxe_v, bzc_v, pz_v, gz_v, zp_v,
           accf, accc, tz_v, clane, cbend, zmsg, zgot, a_v, agot, b_v, bgot,
           cmsg, crecv, crest, xrow, load_sem, small_sem, hs_sem, hr_sem,
           ms_sem, mr_sem, n_sem, cs_sem, cr_sem, ready):
    nx, ny, nz = sizes
    axes = ("gx", "gy", "gz")
    counts = sizes
    me = [lax.axis_index(a) for a in axes]
    SX, SY, SZ = w_v.shape
    PX, PY, PZ = SX // SPF, SY // SPF, SZ // SPF
    KX, KY, KZ = cc_ref.shape[1:]
    EX, QE = PX + 4, 2 * PY
    CR = accc.shape[0]
    CQ, CX = 8, CR // 8
    RZ = tz_v.shape[2]
    KC = SPF * SY
    cells = SX // SPF
    lanes = 3 * SZ

    for c in range(cells):
        part = pl.ds(c * SPF, SPF)
        pltpu.make_async_copy(w_hbm.at[part], w_v.at[part], load_sem.at[c]).start()
        pltpu.make_async_copy(f_hbm.at[part], f_v.at[part], load_sem.at[c]).start()
    small = (pltpu.make_async_copy(fc_hbm, fc_ref, small_sem.at[0]),
             pltpu.make_async_copy(cc_hbm, cc_ref, small_sem.at[1]))
    for copy in small:
        copy.start()

    def load_wait(c):
        both = pl.ds(0, 2 * SPF)
        pltpu.make_async_copy(w_hbm.at[both], w_v.at[both], load_sem.at[c]).wait()

    has = [(me[k] > 0, me[k] < counts[k] - 1) for k in range(3)]

    def toward(step):
        return {axes[k]: lax.rem(me[k] + (counts[k] + step[k] - 1), counts[k])
                for k in range(3) if step[k] != 1}

    def inside(step):
        ok = None
        for k in range(3):
            if step[k] != 1:
                here = has[k][0] if step[k] == 0 else has[k][1]
                ok = here if ok is None else ok & here
        return ok

    def far_first(n):
        return sorted(range(1, n), key=lambda d: -min(d, n - d))

    columns = [(d, e) for d in range(3) for e in range(3)]
    reach = [(n, dz) for dz in far_first(nz) + [0] for n in range(9) if (n, dz) != (4, 0)]

    def column(n, dz):
        there = toward(columns[n] + (1,))
        if dz:
            there[axes[2]] = lax.rem(me[2] + dz, nz)
        return there

    barrier = pltpu.get_barrier_semaphore()
    total = 0
    for k in (2, 1, 0):
        for d in far_first(counts[k]):
            pl.semaphore_signal(
                barrier, inc=1, device_id={axes[k]: lax.rem(me[k] + d, counts[k])},
                device_id_type=MESH
            )
            total += 1
    around = [n for n in range(9) if n != 4]
    for n in around:
        if n % 2 == 0:
            pl.semaphore_signal(barrier, inc=1, device_id=column(n, 0), device_id_type=MESH)
            total += 1

    zero_plane = jnp.zeros((2, SY, SZ), f32)
    s_v[0:2, 8:8 + SY, :] = zero_plane
    s_v[SX + 2:SX + 4, 8:8 + SY, :] = zero_plane
    zero_rows = jnp.zeros((SX, 2, SZ), f32)
    s_v[2:SX + 2, 6:8, :] = zero_rows
    s_v[2:SX + 2, 8 + SY:10 + SY, :] = zero_rows

    row, col = iota((2 * SZ, 2 * SZ), 0) % SZ, iota((2 * SZ, 2 * SZ), 1)
    away = row - col
    slope = jnp.where(away == 1, 8.0, jnp.where(away == -1, -8.0, jnp.where(
        away == -2, 1.0, jnp.where(away == 2, -1.0, 0.0))))
    pick = jnp.where(row == (col % 4 + SZ - 2) % SZ, 1.0, 0.0)
    pz_v[...] = jnp.where(col < SZ, slope, pick).astype(bf16)
    def split_store(ref, index, value):
        high = value.astype(bf16)
        ref[index + (0,)] = high
        ref[index + (1,)] = (value - high.astype(f32)).astype(bf16)

    def ext_q(q):
        return jnp.where(q < PY, q, jnp.where(q < PY + 2, q - PY - 2, q - 2))

    def outer(along_x, along_y):
        return jnp.concatenate([along_x[p:p + 1] * along_y for p in range(along_x.shape[0])], axis=0)

    col = iota((8, KC), 1)
    col2 = iota((QE, KC), 1)
    split_store(wf_v, (), outer(weight(col // SY, iota((8, KC), 0) - 2, SPF)[0:5],
                                weight(col2 % SY, ext_q(iota((QE, KC), 0)), SPF)))
    along_y = weight(col % SY, iota((8, KC), 0) - 2, SPC)
    for c in range(cells):
        split_store(wc_v, (c,), outer(
            weight(col // SY + c * SPF, iota((8, KC), 0) - 2, SPC)[0:CX], along_y))
    col, row = iota((QE, 4 * SX), 1), iota((QE, 4 * SX), 0)
    face_x, face_y = (col % (2 * SX)) // 2, col % 2 + (SY - 2) * (col // (2 * SX))
    along_x = weight(face_x, row - 2, SPF)[0:EX]
    along_y = weight(face_y, ext_q(row), SPF)
    split_store(wy_v, (), jnp.concatenate([
        outer(along_x, along_y[0:PY]), outer(along_x, along_y[PY:QE]),
        outer(weight(face_x, row - 2, SPC)[0:CX], weight(face_y, row - 2, SPC)[0:CQ])], axis=0))
    row, col = iota((4 * SX, 128), 0), iota((4 * SX, 128), 1)
    face_x = (row % (2 * SX)) // 4 + jnp.where(row % 4 < 2, SX // 2, 0)
    place = row % 2 + 2 - 2 * (row // (2 * SX))
    wxe_v[...] = jnp.where(col % 4 == place, jnp.where(
        col < 64, weight(face_x, col // 4 - 2, SPF), weight(face_x, col // 4 - 18, SPC)), 0.0)
    rows, cols = iota((SZ, 128), 0), iota((SZ, 128), 1)
    bzc_v[...] = weight(rows, cols % 8 - 2, SPC) * (SPC ** -1.5 / 24.0)
    accf[...] = jnp.zeros(accf.shape, f32)
    accc[...] = jnp.zeros(accc.shape, f32)

    lane = iota((SY, SZ), 1)
    half_x = SX // 2

    def split(value):
        high = value.astype(bf16)
        return high, (value - high.astype(f32)).astype(bf16)

    def face_rows(c):
        for x in range(c * SPF, (c + 1) * SPF):
            for side, part in ((0, slice(0, 8)), (1, slice(SY - 8, SY))):
                w, f = w_v[x, part, :], f_v[x, part, :]
                rows = slice(6 * side, 6 * side + 2)
                ysend[side, 2 * x:2 * x + 2, :] = (w + f)[rows]
                yd[side, 2 * x:2 * x + 2, :] = (w - f)[rows]

    outer_planes = (0, 1, SX - 2, SX - 1)

    def sums(c):
        wide = ([], [])
        for x in range(c * SPF, (c + 1) * SPF):
            w, f = w_v[x], f_v[x]
            s, d = w + f, w - f
            if x not in outer_planes:
                s_v[x + 2, 8:8 + SY, :] = s
            w_v[x] = d
            for n, value in enumerate((s, d)):
                wide[n].append(jnp.concatenate(split(value), axis=1))
        out = jnp.dot(jnp.concatenate(wide[0], axis=0), pz_v[...], preferred_element_type=f32)
        gz_v[c] = out[:, 0:SZ]
        picked = (out[:, SZ:2 * SZ],
                  jnp.dot(jnp.concatenate(wide[1], axis=0), pz_v[:, SZ:2 * SZ], preferred_element_type=f32))
        tile = c * SPF // half_x
        for n in range(2):
            pack = None if c * SPF % half_x == 0 else zp_v[n, tile]
            for xx in range(SPF):
                value = picked[n][xx * SY:(xx + 1) * SY]
                here = lane // 4 == (c * SPF + xx) % half_x
                pack = value if pack is None else jnp.where(here, value, pack)
            zp_v[n, tile] = pack
    half = cells // 2
    for c in range(cells):
        load_wait(c)
        face_rows(c)
        for x in outer_planes:
            if x // SPF == c:
                s_v[x + 2, 8:8 + SY, :] = w_v[x] + f_v[x]
        if c < half:
            sums(c)

    pl.semaphore_wait(barrier, total)
    for n in around:
        pl.semaphore_signal(ready, inc=1, device_id=column(n, 0), device_id_type=MESH)

    def neighbour_copy(k, side, src, dst, send, recv):
        step = [1, 1, 1]
        step[k] = 2 * side
        return pltpu.make_async_remote_copy(
            src_ref=src, dst_ref=dst, send_sem=send, recv_sem=recv,
            device_id=toward(step), device_id_type=MESH,
        )

    def halo(k, side):
        if k == 0:
            src = s_v.at[pl.ds(2 if side == 0 else SX, 2), pl.ds(8, SY), :]
        else:
            src = (ysend if k == 1 else zsend).at[side]
        return neighbour_copy(k, side, src, (xrecv, yrecv, zrecv)[k].at[1 - side],
                              hs_sem.at[k], hr_sem.at[k])

    def whole(k, ref, send, recv):
        return neighbour_copy(k, 0, ref, ref, send, recv)

    for k in (1, 0):
        for side in range(2):
            halo(k, side).start()

    for c in range(half, cells):
        sums(c)
    upper = lane % 4 >= 2
    for n, ref in enumerate((zsend, zd)):
        ref[0] = jnp.where(upper, zp_v[n, 0], pltpu.roll(zp_v[n, 1], SZ - 2, 1))
        ref[1] = jnp.where(upper, pltpu.roll(zp_v[n, 0], 2, 1), zp_v[n, 1])

    for side in range(2):
        halo(2, side).start()

    def forces(i):
        T = 16
        tiles = {}
        for r in range(0, SY, T):
            at = 8 + r
            near = [s_v[i * SPF + n, at:at + T, :] for n in range(4)]
            for xx in range(SPF):
                x = i * SPF + xx
                near.append(s_v[x + 4, at:at + T, :])
                d = w_v[x, r:r + T, :]
                gx = near[0] - near[4] + 8.0 * (near[3] - near[1])
                near.pop(0)
                gy = (s_v[x + 2, at - 2:at - 2 + T, :] - s_v[x + 2, at + 2:at + 2 + T, :]
                      + 8.0 * (s_v[x + 2, at + 1:at + 1 + T, :] - s_v[x + 2, at - 1:at - 1 + T, :]))
                row = xx * SY + r
                gz = gz_v[i, row:row + T, :]
                tiles[row] = [split(g * d) for g in (gx, gy, gz)]
        return [jnp.concatenate([
            jnp.concatenate([tiles[row][a][n] for row in sorted(tiles)], axis=0)
            for a in range(3)], axis=1) for n in range(2)]

    def cell_weights(i):
        return jnp.concatenate([wf_v[0], wc_v[i, 0], wf_v[1], wc_v[i, 1]], axis=0)

    def project(weights, high, low):
        many = weights.shape[0] // 2
        both = jnp.dot(weights, high, preferred_element_type=f32)
        return both[:many] + both[many:] + jnp.dot(
            weights[:many], low, preferred_element_type=f32)

    def collect(i, out, part):
        fine = out[:5 * QE].reshape(5, 2, PY, out.shape[1])
        accf[0, i:i + 5, :, part] += fine[:, 0]
        accf[1, i:i + 5, :, part] += fine[:, 1]
        accc[:, part] += out[5 * QE:]

    for i in range(cells):
        collect(i, project(cell_weights(i), *forces(i)), slice(0, lanes))

    for k, got in enumerate((xrecv, yrecv, zrecv)):
        whole(k, got, hs_sem.at[k], hr_sem.at[k]).wait_recv()

    gate = [[jnp.where(h, 1.0, 0.0) for h in pair] for pair in has]

    def diff(x):
        return w_v[x]

    for side, i in ((0, 0), (1, cells - 1)):
        r0, r1 = xrecv[side, 0] * gate[0][side], xrecv[side, 1] * gate[0][side]
        if side == 0:
            face = jnp.concatenate([(r0 - 8.0 * r1) * diff(0), r1 * diff(1)], axis=0)
            part = slice(0, 2 * SY)
        else:
            face = jnp.concatenate([-r0 * diff(SX - 2), (8.0 * r0 - r1) * diff(SX - 1)], axis=0)
            part = slice(KC - 2 * SY, KC)
        collect(i, project(cell_weights(i)[:, part], *split(face)), slice(0, SZ))

    rows = iota((SX // 4, 8, SZ), 1) % 2 == 0
    r = (yrecv[0] * gate[1][0]).reshape(SX // 4, 8, SZ)
    low = jnp.where(rows, r - 8.0 * pltpu.roll(r, 7, 1), r).reshape(2 * SX, SZ) * yd[0]
    r = (yrecv[1] * gate[1][1]).reshape(SX // 4, 8, SZ)
    high = jnp.where(rows, -r, 8.0 * pltpu.roll(r, 1, 1) - r).reshape(2 * SX, SZ) * yd[1]
    out = project(jnp.concatenate([wy_v[0], wy_v[1]], axis=0),
                  *split(jnp.concatenate([low, high], axis=0)))
    for half in range(2):
        accf[half, :, :, SZ:2 * SZ] += out[half * EX * PY:(half + 1) * EX * PY].reshape(EX, PY, SZ)
    accc[:, SZ:2 * SZ] += out[2 * EX * PY:]

    even = lane % 2 == 0
    dl = zrecv[0] * gate[2][0]
    dh = zrecv[1] * gate[2][1]
    low = jnp.where(even, dl - 8.0 * pltpu.roll(dl, SZ - 1, 1), dl) * zd[0]
    high = jnp.where(even, -dh, 8.0 * pltpu.roll(dh, 1, 1) - dh) * zd[1]
    row, col = iota((QE + CQ, SY), 0), iota((QE + CQ, SY), 1)
    along_y = jnp.where(row < QE, weight(col, ext_q(row), SPF), weight(col, row - QE - 2, SPC))
    out = nn(nn(along_y, jnp.concatenate([low, high], axis=1)), wxe_v[...])
    at = iota((PY, SZ), 1)
    edge = (at < 2) | (at >= SZ - 2)

    def spread(half, shift):
        return jnp.where(edge, pltpu.roll(out[half * PY:(half + 1) * PY], shift % 128, 1), 0.0)

    for p in range(EX):
        for half in range(2):
            accf[half, p, :, 2 * SZ:3 * SZ] += spread(half, 254 - 4 * p)
    for p in range(CX):
        accc[p * CQ:(p + 1) * CQ, 2 * SZ:3 * SZ] += spread(2, 254 - 64 - 4 * p)

    stack = jnp.concatenate([accc[:, a * SZ:(a + 1) * SZ] for a in range(3)], axis=0)
    shares = nn(stack, bzc_v[...])
    rows, cols = iota((CR, 128), 0), iota((CR, 128), 1)
    keep = (cols // 32 == 2 * ((rows // CQ) % 2) + rows % 2) & (cols % 32 < 24)
    value = jnp.where(cols % 32 < 8, shares[0:CR],
                      jnp.where(cols % 32 < 16, shares[CR:2 * CR], shares[2 * CR:3 * CR]))
    value = jnp.where(keep, value, 0.0).reshape(3, 2, CQ, 128)
    value = value[:, 0] + value[:, 1]
    value = value + pltpu.roll(value, 7, 1)
    for n, (d, e) in enumerate(columns):
        cmsg[n] = value[d, 2 * e:2 * e + 1, :]
    mine = pl.ds(me[2], 1)
    crecv[4, mine, :] = value[1, 2:3, :]
    pl.semaphore_wait(ready, len(around))
    for n, dz in reach:
        pltpu.make_async_remote_copy(
            src_ref=cmsg.at[n], dst_ref=crecv.at[8 - n, mine, :],
            send_sem=n_sem.at[0], recv_sem=n_sem.at[1],
            device_id=column(n, dz), device_id_type=MESH,
        ).start()

    rows, cols = iota((RZ, SZ), 0), iota((RZ, SZ), 1)

    def ext_point(row):
        return jnp.where(row < PZ, row, jnp.where(row < PZ + 2, row - PZ - 2, row - 2))

    bz = weight(cols, ext_point(rows), SPF) * (SPF ** -1.5 / 24.0)
    for a in range(3):
        for half in range(2):
            block = accf[half, :, :, a * SZ:(a + 1) * SZ].reshape(EX * PY, SZ)
            tz_v[half, a] = nt(bz, block)

    for copy in small:
        copy.wait()
    shape = (PX * PY, EX * QE)
    rows, cols = iota(shape, 0), iota(shape, 1)
    ox, oy, oz = me[0] * PX, me[1] * PY, me[2] * PZ
    wide, inner = cols // (EX * PY), cols % (EX * PY)
    planes = bend_planes(inner // PY - 2 + ox, ext_q(inner % PY + PY * wide) + oy,
                         rows // PY + ox, rows % PY + oy, PX * nx, PY * ny)
    zr, zc = ext_point(iota((RZ, PZ), 0)) + oz, iota((RZ, PZ), 1) + oz
    along = jnp.concatenate([same(zr, zc), diff1(zr, zc), diff2(zr, zc, PZ * nz)], axis=0)
    turned = nt(along, fc_ref[...].reshape(3 * PX * PY, PZ))
    turned = jnp.concatenate([jnp.concatenate([
        turned[k * RZ:(k + 1) * RZ, a * PX * PY:(a + 1) * PX * PY] for k in range(3)], axis=1)
        for a in range(3)], axis=0)
    bent = nn(turned, jnp.concatenate(planes, axis=0))
    for a in range(3):
        for half in range(2):
            tz_v[half, a] += bent[a * RZ:(a + 1) * RZ, half * EX * PY:(half + 1) * EX * PY]
            for side in range(2):
                zmsg[side, half, 2 * a:2 * a + 2, :] = tz_v[
                    half, a, PZ + 2 * side:PZ + 2 * side + 2, :]

    def fine_start(k):
        for side in range(2):
            source = (b_v, a_v.at[1], zmsg.at[side])[k]
            neighbour_copy(k, side, source, (bgot, agot, zgot)[k].at[1 - side],
                           ms_sem.at[k], mr_sem.at[k]).start()

    def fine_whole(k):
        return whole(k, (bgot, agot, zgot)[k], ms_sem.at[k], mr_sem.at[k])

    def coarse_slot(k, n):
        if k == 0:
            return xrow.at[n]
        return xrow.at[me[0], :, pl.ds(n, 1), :]

    def coarse_start(k):
        for d in far_first(counts[k]):
            pltpu.make_async_remote_copy(
                src_ref=coarse_slot(k, me[k]), dst_ref=coarse_slot(k, me[k]),
                send_sem=cs_sem.at[k], recv_sem=cr_sem.at[k],
                device_id={axes[k]: lax.rem(me[k] + d, counts[k])}, device_id_type=MESH,
            ).start()

    def coarse_whole(k):
        part = pl.ds(0, counts[k] - 1)
        ref = (xrow.at[part], xrow.at[me[0], :, part, :])[k]
        return whole(k, ref, cs_sem.at[k], cr_sem.at[k])

    fine_start(2)

    q_at, r_at = iota((KX, KY, 128), 1), iota((KX, KY, 128), 2)

    def laplace(c):
        zero = jnp.zeros((1, KY, 128), f32)
        total = (jnp.concatenate([c[1:], zero], axis=0) + jnp.concatenate([zero, c[:-1]], axis=0)
                 + jnp.where(q_at < KY - 1, pltpu.roll(c, KY - 1, 1), 0.0)
                 + jnp.where(q_at > 0, pltpu.roll(c, 1, 1), 0.0)
                 + pltpu.roll(c, 127, 2) + pltpu.roll(c, 1, 2))
        return jnp.where(r_at < KZ, total - 6.0 * c, 0.0)

    clane[...] = jnp.zeros(clane.shape, f32)
    for a in range(3):
        clane[:, :, 0:KZ] = cc_ref[a]
        cbend[a] = BEND * laplace(laplace(clane[...]))

    all_shares = crest.at[pl.ds(0, len(reach))]
    whole(0, all_shares, n_sem.at[0], n_sem.at[1]).wait_recv()
    total = crecv[4]
    for n, (d, e) in enumerate(columns):
        if n != 4:
            total = total + jnp.where(inside((d, e, 1)), crecv[n], 0.0)
    sub, at = iota((nz, 128), 0), iota((nz, 128), 1) % 32
    keep = (at >= 4 * sub - 2) & (at < 4 * sub + 6) & (at < KZ)
    for a in range(3):
        value = None
        for n in range(nz):
            shift = (4 * n - 2 - 8 * a) % 128
            moved = pltpu.roll(total, shift, 1) if shift else total
            value = moved if n == 0 else jnp.where(sub == n, moved, value)
        xrow[me[0], a, pl.ds(me[1], 1), :] = jnp.sum(
            jnp.where(keep, value, 0.0), axis=0, keepdims=True)
    coarse_start(1)

    fine_whole(2).wait_recv()
    for half in range(2):
        for a in range(3):
            part = slice(2 * a, 2 * a + 2)
            tz_v[half, a, 0:2, :] = tz_v[half, a, 0:2, :] + zgot[0, half, part, :] * gate[2][0]
            tz_v[half, a, PZ - 2:PZ, :] = (
                tz_v[half, a, PZ - 2:PZ, :] + zgot[1, half, part, :] * gate[2][1])
            a_v[half, a * PZ:(a + 1) * PZ, :] = tz_v[half, a, 0:PZ, :]
    fine_start(1)

    fine_whole(1).wait_recv()
    shape = (EX * PY, EX * PY)
    rows, cols = iota(shape, 0), iota(shape, 1)
    p_same = rows // PY == cols // PY
    q, r = rows % PY, cols % PY
    low = jnp.where(p_same & (q == r + 2) & (r < 2), 1.0, 0.0)
    high = jnp.where(p_same & (q == r - (PY - 2)) & (r >= PY - 2), 1.0, 0.0)
    b_v[...] = (a_v[0] + nn(agot[0] * gate[1][0], low) + nn(agot[1] * gate[1][1], high))
    fine_start(0)

    coarse_whole(1).wait_recv()
    coarse_start(0)

    fine_whole(0).wait_recv()
    shape = (PX * PY, EX * PY)
    rows, cols = iota(shape, 0), iota(shape, 1)
    own = jnp.where(cols == rows + 2 * PY, 1.0, 0.0)
    low = jnp.where((cols == rows + (PX + 2) * PY) & (rows < 2 * PY), gate[0][0], 0.0)
    high = jnp.where((cols == rows - (PX - 2) * PY) & (rows >= (PX - 2) * PY), gate[0][1], 0.0)
    for a in range(3):
        part = slice(a * PZ, (a + 1) * PZ)
        out = nt(own, b_v[part]) + nt(low, bgot[0, part]) + nt(high, bgot[1, part])
        fo_ref[a] = out.reshape(PX, PY, PZ)

    for k, got in enumerate((xrecv, yrecv, zrecv)):
        whole(k, got, hs_sem.at[k], hr_sem.at[k]).wait_send()
        fine_whole(k).wait_send()
        if k < 2:
            coarse_whole(k).wait_send()
    whole(0, all_shares, n_sem.at[0], n_sem.at[1]).wait_send()

    coarse_whole(0).wait_recv()
    for i in range(nx):
        for a in range(3):
            block = xrow[i, a]
            for g in range(4):
                value = block if g == 0 else pltpu.roll(block, 128 - 32 * g, 1)
                p = 2 * i + g // 2
                part = pl.ds(g % 2, ny, stride=2)
                co_ref[a, p, part, :] = (value + cbend[a, p, part, :])[:, 0:KZ]


def solution(mesh):
    sizes = tuple(mesh.shape[a] for a in ("gx", "gy", "gz"))

    def step(warped, fixed, fine, coarse):
        SX, SY, SZ = warped.shape
        PX, PY, PZ = SX // SPF, SY // SPF, SZ // SPF
        KX, KY, KZ = coarse.shape[1:]
        EX, QE, RZ = PX + 4, 2 * PY, PZ + 8
        CR = 48
        KC = SPF * SY
        vmem = pl.BlockSpec(memory_space=pltpu.VMEM)
        hbm = pl.BlockSpec(memory_space=pltpu.HBM)
        V = pltpu.VMEM
        D = pltpu.SemaphoreType.DMA
        return pl.pallas_call(
            functools.partial(kernel, sizes),
            out_shape=(V(fine.shape, f32), V(coarse.shape, f32)),
            in_specs=[hbm] * 4,
            out_specs=(vmem, vmem),
            scratch_shapes=[
                V((SX, SY, SZ), f32), V((SX, SY, SZ), f32),
                V((3, PX, PY, PZ), f32), V(coarse.shape, f32),
                V((SX + 4, SY + 16, SZ), f32), V((2, 2, SY, SZ), f32),
                V((2, 2 * SX, SZ), f32), V((2, 2 * SX, SZ), f32), V((2, 2 * SX, SZ), f32),
                V((2, SY, SZ), f32), V((2, SY, SZ), f32), V((2, SY, SZ), f32),
                V((2, 5 * QE, KC), bf16), V((SX // SPF, 2, CR, KC), bf16),
                V((2, EX * QE + CR, 4 * SX), bf16), V((4 * SX, 128), f32), V((SZ, 128), f32),
                V((2 * SZ, 2 * SZ), bf16),
                V((SX // SPF, KC, SZ), f32), V((2, 2, SY, SZ), f32),
                V((2, EX, PY, 3 * SZ), f32), V((CR, 3 * SZ), f32),
                V((2, 3, RZ, EX * PY), f32),
                V((KX, KY, 128), f32), V((3, KX, KY, 128), f32),
                V((2, 2, 8, EX * PY), f32), V((2, 2, 8, EX * PY), f32),
                V((2, 3 * PZ, EX * PY), f32), V((2, 3 * PZ, EX * PY), f32),
                V((3 * PZ, EX * PY), f32), V((2, 3 * PZ, EX * PY), f32),
                V((9, 1, 128), f32), V((9, sizes[2], 128), f32),
                V((9 * sizes[2], 128), f32), V((sizes[0], 3, sizes[1], 128), f32),
                D((SX // SPF,)), D((2,)), D((3,)), D((3,)),
                D((3,)), D((3,)), D((2,)), D((2,)), D((2,)), pltpu.SemaphoreType.REGULAR,
            ],
            compiler_params=pltpu.CompilerParams(
                collective_id=0, has_side_effects=True, vmem_limit_bytes=66000000
            ),
        )(warped, fixed, fine, coarse)

    in_specs = (P("gx", "gy", "gz"), P("gx", "gy", "gz"), P(None, "gx", "gy", "gz"), P())
    out_specs = (P(None, "gx", "gy", "gz"), P())
    return jax.shard_map(
        step, mesh=mesh, in_specs=in_specs, out_specs=out_specs, check_vma=False
    )
```
